256 devices in a mesh: gx: 16 (over z_lo, x, core), gy: 4 (over y), gz: 4 (over z_hi).
Axes of the slice: x: 4, y: 4, z: 8 (z_hi: 4, z_lo: 2; z = z_hi * 2 + z_lo), core: 2. Of those that a mesh axis runs over, the one named last changes fastest.
Arguments:
- estimate: float32 [384, 128, 512], P('gx', 'gy', 'gz'), may hold values from 0.03 to 11, as said below
- view_images: float32 [4, 384, 128, 512], P(None, 'gx', 'gy', 'gz'), may hold values from 0.015 to 21, as said below
- psf_taps: int32 [4, 3, 31], replicated, may hold values from 1 to 64
- view_weights: int32 [4], replicated, may hold values from 1 to 4
Outputs:
- deconvolved: float32 [384, 128, 512], P('gx', 'gy', 'gz')
- misfit: float32 [2, 4], replicated
The draws below stay inside these ranges and needn't reach their ends.
Inputs may be any that keep to these rules, and one draw needn't show every extreme that they name: `estimate`: positive. `view_images`: positive.
All inputs are finite; a program needn't handle non-finite values.
Results may differ from the reference program's by a relative error of at most 0.0001.
Values sent between devices are 32-bit elements; how exact they have to be, the bound alone decides.
No kernel may reach another device: no remote copies, remote signals or barrier semaphores. Data moves between devices by JAX's collectives and lax.ppermute only.
A program may use at most 128 MiB of HBM per device.

```python
import jax
import jax.numpy as jnp
from jax import lax

VIEWS = 4
TAPS = 31
ITERS = 2
NX = 384
NY = 128
NZ = 512


def ramp_profile(rising):
    first = (jnp.arange(NX, dtype=jnp.float32) + 0.5) / NX
    second = (jnp.arange(NY, dtype=jnp.float32) + 0.5) / NY
    third = (jnp.arange(NZ, dtype=jnp.float32) + 0.5) / NZ
    if rising:
        return (0.5 + first)[:, None, None] * (0.5 + second)[None, :, None] * (0.5 + third)[None, None, :]
    return (1.5 - first)[:, None, None] * (1.5 - second)[None, :, None] * (1.5 - third)[None, None, :]


def draw_view_images(key, part):
    inner = jax.random.fold_in(key, 11)
    profile = ramp_profile(True)[None]
    rough = jax.random.uniform(inner, (VIEWS, NX, NY, NZ), jnp.float32, 0.5, 2.0)
    return (profile * rough).astype(jnp.float32)


def draw_estimate(key, part):
    inner = jax.random.fold_in(key, 23)
    profile = ramp_profile(False)
    rough = jax.random.uniform(inner, (NX, NY, NZ), jnp.float32, 0.5, 1.5)
    return (profile * rough).astype(jnp.float32)


def set_ends(entries, stream_key, low, largest):
    longest = entries.shape.index(max(entries.shape))
    spots = []
    for shift in (0, 1):
        where = [jax.random.randint(jax.random.fold_in(stream_key, axis), (), 0, length) for axis, length in enumerate(entries.shape)]
        where[longest] = (where[longest] + shift) % entries.shape[longest]
        spots.append(tuple(where))
    return entries.at[spots[0]].set(low).at[spots[1]].set(largest)


def setup_inputs(seed: int = 0) -> dict:
    arg_keys = jax.random.split(jax.random.key(seed), 5)
    return {
        "estimate": draw_estimate(jax.random.fold_in(arg_keys[4], 71), 0),
        "view_images": draw_view_images(jax.random.fold_in(arg_keys[4], 71), 0),
        "psf_taps": set_ends(jax.random.randint(arg_keys[2], (VIEWS, 3, TAPS), 1, 65), jax.random.fold_in(arg_keys[2], 1), 1, 64).astype(jnp.int32),
        "view_weights": set_ends(jax.random.randint(arg_keys[3], (VIEWS,), 1, 5), jax.random.fold_in(arg_keys[3], 1), 1, 4).astype(jnp.int32),
    }


def convolve_axis(volume, kernel, axis_dim):
    moved = jnp.moveaxis(volume, axis_dim, -1)
    saved_shape = moved.shape
    flattened = moved.reshape(-1, 1, saved_shape[-1])
    reach = (TAPS - 1) // 2
    convolved = lax.conv_general_dilated(flattened, kernel.reshape(1, 1, -1), (1,), [(reach, reach)], dimension_numbers=("NCH", "OIH", "NCH"), precision=lax.Precision.HIGHEST)
    return jnp.moveaxis(convolved.reshape(saved_shape), -1, axis_dim)


def reference(estimate, view_images, psf_taps, view_weights):
    kernels = psf_taps.astype(jnp.float32) / 256.0
    flipped = kernels[:, :, ::-1]
    tap_sums = jnp.sum(kernels, axis=2)
    weight_float = view_weights.astype(jnp.float32)
    normalizer = jnp.sum(weight_float * jnp.prod(tap_sums, axis=1))
    data_total = jnp.sum(view_images, axis=(1, 2, 3))
    data_square = jnp.sum(view_images * view_images, axis=(1, 2, 3))
    misfits = []
    for iteration in range(ITERS):
        correction = jnp.zeros_like(estimate)
        row = []
        for view_index in range(VIEWS):
            blurred = convolve_axis(estimate, kernels[view_index, 0], 0)
            blurred = convolve_axis(blurred, kernels[view_index, 1], 1)
            blurred = convolve_axis(blurred, kernels[view_index, 2], 2)
            flux_scale = data_total[view_index] / jnp.sum(blurred)
            scaled = flux_scale * blurred
            difference = view_images[view_index] - scaled
            row.append(jnp.sum(difference * difference) / data_square[view_index])
            quotient = view_images[view_index] / scaled
            backed = convolve_axis(quotient, flipped[view_index, 0], 0)
            backed = convolve_axis(backed, flipped[view_index, 1], 1)
            backed = convolve_axis(backed, flipped[view_index, 2], 2)
            correction = correction + weight_float[view_index] * backed
        estimate = estimate * (correction / normalizer)
        misfits.append(jnp.stack(row))
    return estimate, jnp.stack(misfits)
```

```python
import functools

import jax
import jax.numpy as jnp
from jax import lax
from jax.experimental import pallas as pl
from jax.experimental.pallas import tpu as pltpu
from jax.sharding import Mesh
from jax.sharding import PartitionSpec as P

TAPS = 31
REACH = 15
ITERS = 2
VIEWS = 4
X, Y, Z = 24, 32, 128
YE = 64
F32 = jnp.float32
BF16 = jnp.bfloat16
GX = ("gx_0", "gx_1", "gx_2")
AXES = {"gx": GX, "gy": "gy", "gz": "gz"}
SUM_STEPS = (("gx_2", 1), ("gx_1", 1), ("gx_1", 2), ("gy", 1), ("gy", 2), ("gx_0", 1), ("gz", 1), ("gz", 2))


def parity(name):
    if name == "gx":
        return lax.axis_index("gx_2")
    return lax.rem(lax.axis_index(name), 2)


def position(name):
    if name == "gx":
        return (lax.axis_index("gx_0") * 4 + lax.axis_index("gx_1")) * 2 + lax.axis_index("gx_2")
    return lax.axis_index(name)


def lanes(shape):
    return lax.broadcasted_iota(jnp.int32, shape, len(shape) - 1)


def split(value):
    high = value.astype(BF16)
    low = (value - high.astype(F32)).astype(BF16)
    return high, low


def left_exact(matrix, data):
    high, low = split(data)
    return jnp.dot(matrix, high, preferred_element_type=F32) + jnp.dot(matrix, low, preferred_element_type=F32)


def right_exact(data, matrix):
    rows = data.shape[0]
    both = jnp.dot(jnp.concatenate(split(data), axis=0), matrix, preferred_element_type=F32)
    return both[:rows] + both[rows:]


def extended_offset(index, size, width, odd):
    low_first = index < size + width
    local = jnp.where(low_first, index - size, index - size - width)
    upper = low_first == (odd == 0)
    outside = jnp.where(upper, size + local, local - width)
    return jnp.where(index < size, index, outside)


def taps_matrix(taps_ref, view, axis, source, target):
    tap = source - target + REACH
    out = jnp.zeros(tap.shape, F32)
    for t in range(TAPS):
        out = jnp.where(tap == t, taps_ref[view, axis, t].astype(F32) / 256.0, out)
    return out


def select_matrix(rows, columns, match):
    r = lax.broadcasted_iota(jnp.int32, (rows, columns), 0)
    c = lax.broadcasted_iota(jnp.int32, (rows, columns), 1)
    return match(r, c)


def one_hot(rows, columns, match):
    return jnp.where(select_matrix(rows, columns, match), 1.0, 0.0).astype(BF16)


def setup_kernel(taps_ref, fz, fy, fx, bz, by, bx, ax, ayz):
    odd_x, odd_y, odd_z = parity("gx"), parity("gy"), parity("gz")
    XE = X + 2 * REACH
    for v in range(VIEWS):
        src = extended_offset(lax.broadcasted_iota(jnp.int32, (256, Z), 0), Z, 16, odd_z)
        raw = lax.broadcasted_iota(jnp.int32, (256, Z), 0)
        tgt = lax.broadcasted_iota(jnp.int32, (256, Z), 1)
        src = jnp.where(raw < Z + 32, src, -1000)
        fz[:, v * Z : (v + 1) * Z] = taps_matrix(taps_ref, v, 2, src, tgt).astype(BF16)
        raw = lax.broadcasted_iota(jnp.int32, (Z, 256), 1)
        src = extended_offset(raw, Z, 16, odd_z)
        src = jnp.where(raw < Z + 32, src, -1000)
        tgt = lax.broadcasted_iota(jnp.int32, (Z, 256), 0)
        bz[v * Z : (v + 1) * Z, :] = taps_matrix(taps_ref, v, 2, src, tgt).astype(BF16)
        tgt = lax.broadcasted_iota(jnp.int32, (Y, YE), 0)
        src = extended_offset(lax.broadcasted_iota(jnp.int32, (Y, YE), 1), Y, 16, odd_y)
        base = taps_matrix(taps_ref, v, 1, src, tgt).astype(BF16)
        spread = jnp.dot(one_hot(4 * Y, Y, lambda r, c: lax.rem(r, Y) == c), base, preferred_element_type=F32).astype(BF16)
        spread = jnp.dot(spread, one_hot(YE, 4 * YE, lambda r, c: lax.rem(c, YE) == r), preferred_element_type=F32)
        mask = select_matrix(4 * Y, 4 * YE, lambda r, c: r // Y == c // YE)
        spread = jnp.where(mask, spread, 0.0)
        fy[v] = spread.astype(BF16)
        by[v] = spread.T.astype(BF16)
        tgt = lax.broadcasted_iota(jnp.int32, (X, XE), 0)
        src = extended_offset(lax.broadcasted_iota(jnp.int32, (X, XE), 1), X, REACH, odd_x)
        base = taps_matrix(taps_ref, v, 0, src, tgt).astype(BF16)
        spread = jnp.dot(one_hot(X * 8, X, lambda r, c: r // 8 == c), base, preferred_element_type=F32).astype(BF16)
        spread = jnp.dot(spread, one_hot(XE, XE * 8, lambda r, c: c // 8 == r), preferred_element_type=F32)
        mask = select_matrix(X * 8, XE * 8, lambda r, c: lax.rem(r, 8) == lax.rem(c, 8))
        spread = jnp.where(mask, spread, 0.0)
        fx[v] = spread.astype(BF16)
        by_t = jnp.concatenate([spread, jnp.zeros((X * 8, 512 - XE * 8), F32)], axis=1).T
        bx[v] = by_t[: XE * 8].astype(BF16)
        def reachable(axis, name, size, count, iota):
            where_global = position(name) * size + iota
            out = jnp.zeros(iota.shape, F32)
            for t in range(TAPS):
                at = where_global - t + REACH
                inside = (at >= 0) & (at < count * size)
                out = out + jnp.where(inside, taps_ref[v, axis, t].astype(F32) / 256.0, 0.0)
            return out
        ax[v] = reachable(0, "gx", X, 16, lax.broadcasted_iota(jnp.int32, (X, Z), 0))
        ayz[v] = reachable(1, "gy", Y, 4, lax.broadcasted_iota(jnp.int32, (Y, Z), 0)) * reachable(
            2, "gz", Z, 4, lax.broadcasted_iota(jnp.int32, (Y, Z), 1)
        )


def pack_z(load, z_a, z_b):
    group = lanes((3 * Y, Z)) // 16
    up = jnp.zeros((3 * Y, Z), F32)
    down = jnp.zeros((3 * Y, Z), F32)
    for g in range(8):
        part = load(g)
        up = jnp.where(group == g, pltpu.roll(part, (16 * g + 16) % Z, 1) if g != 7 else part, up)
        down = jnp.where(group == g, pltpu.roll(part, 16 * g, 1) if g else part, down)
    odd = parity("gz")
    z_a[...] = jnp.where(odd == 0, up, down)
    z_b[...] = jnp.where(odd == 0, down, up)


def blurred_totals(load, ax, ayz):
    lane = lanes((8, Z))
    row = lax.broadcasted_iota(jnp.int32, (8, Z), 0)
    out = jnp.zeros((8, Z), F32)
    for v in range(VIEWS):
        acc = jnp.zeros((Y, Z), F32)
        for i in range(X):
            acc = acc + load(i) * ax[v, i : i + 1, :]
        total = jnp.sum(acc * ayz[v])
        out = jnp.where((lane == 8 + v) & (row == 0), total, out)
    return out


def first_kernel(est, z_a, z_b):
    pack_z(lambda g: est[3 * g : 3 * g + 3].reshape(3 * Y, Z), z_a, z_b)


def sums_kernel(est, views, ax, ayz, row_ref):
    lane = lanes((8, Z))
    row = lax.broadcasted_iota(jnp.int32, (8, Z), 0)
    out = blurred_totals(lambda i: est[i], ax, ayz)
    for v in range(VIEWS):
        total = jnp.zeros((Y, Z), F32)
        square = jnp.zeros((Y, Z), F32)
        for i in range(X):
            image = views[v, i]
            total = total + image
            square = square + image * image
        out = jnp.where((lane == v) & (row == 0), jnp.sum(total), out)
        out = jnp.where((lane == 4 + v) & (row == 0), jnp.sum(square), out)
    row_ref[...] = out


def pack_y_kernel(est, z_a, z_b, y_a, y_b):
    odd = parity("gy")
    start_a = pl.multiple_of((1 - odd) * 16, 16)
    start_b = pl.multiple_of(odd * 16, 16)
    for start, out in ((start_a, y_a), (start_b, y_b)):
        out[0:X] = est[:, pl.ds(start, 16), :]
        out[X : X + 3] = z_a[:, pl.ds(start, 16), :]
        out[X + 3 : X + 6] = z_b[:, pl.ds(start, 16), :]


def pack_x_kernel(est, z_a, z_b, y_a, y_b, own, x_a, x_b):
    own[0:X, 0:Y] = est[...]
    own[X : X + 3, 0:Y] = z_a[...]
    own[X + 3 : X + 6, 0:Y] = z_b[...]
    own[:, Y : Y + 16] = y_a[...]
    own[:, Y + 16 : YE] = y_b[...]
    odd = parity("gx")
    for flag, out in ((odd, x_a), (1 - odd, x_b)):
        out[0:REACH] = own[pl.ds((1 - flag) * 9, REACH)]
        for i in range(6):
            full = own[X + i]
            out[REACH + i] = jnp.where(flag == 0, pltpu.roll(full, Z - 48, 1), full)


def forward_group(src, first_z, plane, fz, fy, store):
    mains, sides = [], []
    lane = lanes((YE, Z))
    for k in range(4):
        p = plane + k
        g = p // 3
        i = p - 3 * g
        mains.append(src[p])
        a = pltpu.roll(src[first_z + i], lax.rem(Z - 16 * g, Z), 1)
        b = pltpu.roll(src[first_z + 3 + i], lax.rem(Z + 16 - 16 * g, Z), 1)
        sides.append(jnp.where(lane < 16, a, b))
    data = jnp.concatenate([jnp.concatenate(mains, 0), jnp.concatenate(sides, 0)], axis=1)
    wide = right_exact(data, fz[...])
    for v in range(VIEWS):
        out = left_exact(fy[v], wide[:, v * Z : (v + 1) * Z])
        store(v, out.reshape(4, Y, Z))


def forward_own_kernel(own, fz, fy, out):
    def step(j, carry):
        plane = j * 4

        def store(v, value):
            out[v, pl.ds(plane, 4)] = value

        forward_group(own, X, plane, fz, fy, store)
        return carry

    lax.fori_loop(0, 6, step, 0)


def forward_kernel(x_a, x_b, mid, fz, fy, fx, out, halo):
    for base, src in ((0, x_a), (REACH, x_b)):
        def step(j, carry, base=base, src=src):
            plane = jnp.minimum(j * 4, REACH - 4)

            def store(v, value):
                halo[v, pl.ds(base + plane, 4)] = value

            forward_group(src, REACH, plane, fz, fy, store)
            return carry

        lax.fori_loop(0, 4, step, 0)
    for v in range(VIEWS):
        for pair in range(2):
            columns = []
            for tile in (2 * pair, 2 * pair + 1):
                rows = pl.ds(tile * 8, 8)
                columns.append(
                    jnp.concatenate(
                        [mid[v, :, rows].reshape(X * 8, Z), halo[v, :, rows].reshape(2 * REACH * 8, Z)], axis=0
                    )
                )
            got = left_exact(fx[v], jnp.concatenate(columns, axis=1))
            for k, tile in enumerate((2 * pair, 2 * pair + 1)):
                out[v, :, tile * 8 : tile * 8 + 8] = got[:, k * Z : (k + 1) * Z].reshape(X, 8, Z)


def pick(row, lane, index):
    return jnp.sum(jnp.where(lane == index, row, 0.0), axis=1, keepdims=True)


def backward_group(load, plane, bz, by, store):
    parts = [left_exact(by[v], load(v, plane).reshape(4 * Y, Z)) for v in range(VIEWS)]
    wide = right_exact(jnp.concatenate(parts, axis=1), bz[...])
    store(wide)


def store_extended(dst, first_z, plane, wide):
    group = lanes((YE, Z)) // 16
    for k in range(4):
        p = plane + k
        g = p // 3
        i = p - 3 * g
        rows = wide[k * YE : (k + 1) * YE]
        dst[p] = rows[:, :Z]
        side = rows[:, Z:]
        a = pltpu.roll(side, lax.rem(16 * g + Z, Z), 1)
        b = pltpu.roll(side, lax.rem(16 * g + Z - 16, Z), 1)
        dst[first_z + i] = jnp.where(group == g, a, dst[first_z + i])
        dst[first_z + 3 + i] = jnp.where(group == g, b, dst[first_z + 3 + i])


def backward_kernel(sums, weights, norm, blurred, views, bz, by, bx, x_a, x_b, mid, misfit, halo):
    lane = lanes((1, Z))
    row = sums[0:1, :]
    out_lane = lanes((8, Z))
    out_row = lax.broadcasted_iota(jnp.int32, (8, Z), 0)
    misfits = jnp.zeros((8, Z), F32)
    for v in range(VIEWS):
        flux = pick(row, lane, v) / pick(row, lane, 8 + v)
        scale = weights[v].astype(F32) / norm[0]
        missed = jnp.zeros((X * 8, 2 * Z), F32)
        for pair in range(2):
            tiles = (2 * pair, 2 * pair + 1)
            b = jnp.concatenate([blurred[v, :, t * 8 : t * 8 + 8].reshape(X * 8, Z) for t in tiles], axis=1)
            image = jnp.concatenate([views[v, :, t * 8 : t * 8 + 8].reshape(X * 8, Z) for t in tiles], axis=1)
            scaled = flux * b
            gap = image - scaled
            missed = missed + gap * gap
            got = left_exact(bx[v], (image / scaled) * scale)
            for k, t in enumerate(tiles):
                piece = got[:, k * Z : (k + 1) * Z]
                mid[v, :, t * 8 : t * 8 + 8] = piece[: X * 8].reshape(X, 8, Z)
                halo[v, :, t * 8 : t * 8 + 8] = piece[X * 8 :].reshape(2 * REACH, 8, Z)
        misfits = jnp.where((out_lane == 12 + v) & (out_row == 0), jnp.sum(missed), misfits)
    misfit[...] = misfits
    for base, dst in ((0, x_a), (REACH, x_b)):
        dst[REACH : REACH + 6] = jnp.zeros((6, YE, Z), F32)

        def step(j, carry, base=base, dst=dst):
            plane = jnp.minimum(j * 4, REACH - 4)
            backward_group(
                lambda v, p: halo[v, pl.ds(base + p, 4)],
                plane, bz, by, lambda wide: store_extended(dst, REACH, plane, wide),
            )
            return carry

        lax.fori_loop(0, 4, step, 0)


def backward_own_kernel(mid, bz, by, own):
    own[X : X + 6] = jnp.zeros((6, YE, Z), F32)

    def step(j, carry):
        plane = j * 4
        backward_group(
            lambda v, p: mid[v, pl.ds(p, 4)], plane, bz, by, lambda wide: store_extended(own, X, plane, wide)
        )
        return carry

    lax.fori_loop(0, 6, step, 0)


def add_x_kernel(own, x_a, x_b, kept, y_a, y_b, total):
    total[...] = own[...]
    odd = parity("gx")
    valid = lanes((YE, Z)) < 80
    for flag, src in ((odd, x_a), (1 - odd, x_b)):
        spot = pl.ds((1 - flag) * 9, REACH)
        total[spot] = total[spot] + src[0:REACH]
        for i in range(6):
            side = jnp.where(valid, src[REACH + i], 0.0)
            total[X + i] = total[X + i] + jnp.where(flag == 0, pltpu.roll(side, 48, 1), side)
    kept[...] = total[:, 0:Y]
    y_a[...] = total[:, Y : Y + 16]
    y_b[...] = total[:, Y + 16 : YE]


def add_y_kernel(kept, y_a, y_b, main, z_a, z_b, total):
    total[...] = kept[...]
    odd = parity("gy")
    for start, src in (((1 - odd) * 16, y_a), (odd * 16, y_b)):
        spot = pl.ds(pl.multiple_of(start, 16), 16)
        total[:, spot] = total[:, spot] + src[...]
    main[...] = total[0:X]
    z_a[...] = total[X : X + 3]
    z_b[...] = total[X + 3 : X + 6]


def corrected(main, z_a, z_b, est, g):
    odd = parity("gz")
    lane = lanes((3 * Y, Z))
    a = z_a[...].reshape(3 * Y, Z)
    b = z_b[...].reshape(3 * Y, Z)
    up = jnp.where(odd == 0, a, b)
    down = jnp.where(odd == 0, b, a)
    up = pltpu.roll(up, (112 - 16 * g) % Z, 1) if g != 7 else up
    down = pltpu.roll(down, (Z - 16 * g) % Z, 1) if g else down
    total = main[3 * g : 3 * g + 3].reshape(3 * Y, Z)
    total = total + jnp.where(lane >= 112, up, 0.0) + jnp.where(lane < 16, down, 0.0)
    return est[3 * g : 3 * g + 3].reshape(3 * Y, Z) * total


def update_kernel(main, z_a, z_b, est, ax, ayz, carry, out, out_a, out_b, row_ref):
    for g in range(8):
        out[3 * g : 3 * g + 3] = corrected(main, z_a, z_b, est, g).reshape(3, Y, Z)
    pack_z(lambda g: out[3 * g : 3 * g + 3].reshape(3 * Y, Z), out_a, out_b)
    row_ref[...] = blurred_totals(lambda i: out[i], ax, ayz) + carry[...]


def finish_kernel(main, z_a, z_b, est, out):
    for g in range(8):
        out[3 * g : 3 * g + 3] = corrected(main, z_a, z_b, est, g).reshape(3, Y, Z)


VM = pl.BlockSpec(memory_space=pltpu.VMEM)
SM = pl.BlockSpec(memory_space=pltpu.SMEM)


def call(kernel, outs, operands, specs=None, scratch=(), limit=16, flops=0):
    shapes = [jax.ShapeDtypeStruct(shape, dtype) for shape, dtype in outs]
    return pl.pallas_call(
        kernel,
        out_shape=shapes,
        in_specs=specs or [VM] * len(operands),
        out_specs=[VM] * len(shapes),
        scratch_shapes=[pltpu.VMEM(shape, dtype) for shape, dtype in scratch],
        compiler_params=pltpu.CompilerParams(vmem_limit_bytes=limit << 20),
        cost_estimate=pl.CostEstimate(flops=max(flops, 1000), bytes_accessed=1000, transcendentals=0),
        name=kernel.__name__,
    )(*operands)


def swap(a, b, axis):
    names = AXES[axis]
    count = lax.axis_size(names)
    first = [(i, i ^ 1) for i in range(count)]
    second = [(i, i + 1) for i in range(1, count - 1, 2)] + [(i + 1, i) for i in range(1, count - 1, 2)]
    return lax.ppermute(a, names, first), lax.ppermute(b, names, second)


def all_sum(row):
    for axis, bit in SUM_STEPS:
        count = lax.axis_size(axis)
        row = row + lax.ppermute(row, axis, [(i, i ^ bit) for i in range(count)])
    return row


ZS = ((3 * Y, Z), F32)
Z3 = ((3, Y, Z), F32)
YS = ((X + 6, 16, Z), F32)
XS = ((REACH + 6, YE, Z), F32)
OWN = ((X + 6, YE, Z), F32)
CUBE = ((X, Y, Z), F32)
FOUR = ((VIEWS, X, Y, Z), F32)
ROW = ((8, Z), F32)
GF = 1 << 30


def local(estimate, view_images, psf_taps, view_weights):
    XE8 = (X + 2 * REACH) * 8
    kernels = psf_taps.astype(F32) / 256.0
    tap_sums = jnp.sum(kernels, axis=2)
    norm = jnp.sum(view_weights.astype(F32) * jnp.prod(tap_sums, axis=1)).reshape(1)
    z_a, z_b = call(first_kernel, [ZS, ZS], [estimate])
    fz, fy, fx, bz, by, bx, ax, ayz = call(
        setup_kernel,
        [
            ((256, VIEWS * Z), BF16), ((VIEWS, 4 * Y, 4 * YE), BF16), ((VIEWS, X * 8, XE8), BF16),
            ((VIEWS * Z, 256), BF16), ((VIEWS, 4 * YE, 4 * Y), BF16), ((VIEWS, XE8, X * 8), BF16),
            ((VIEWS, X, Z), F32), ((VIEWS, Y, Z), F32),
        ],
        [psf_taps], specs=[SM], limit=24, flops=4 * GF,
    )
    (row,) = call(sums_kernel, [ROW], [estimate, view_images, ax, ayz], flops=GF)
    data = None
    misfits = []
    for iteration in range(ITERS):
        z_a, z_b = swap(z_a, z_b, "gz")
        z_a, z_b = z_a.reshape(3, Y, Z), z_b.reshape(3, Y, Z)
        sums = all_sum(row)
        y_a, y_b = call(pack_y_kernel, [YS, YS], [estimate, z_a, z_b])
        y_a, y_b = swap(y_a, y_b, "gy")
        own, x_a, x_b = call(pack_x_kernel, [OWN, XS, XS], [estimate, z_a, z_b, y_a, y_b])
        x_a, x_b = swap(x_a, x_b, "gx")
        (mid,) = call(forward_own_kernel, [FOUR], [own, fz, fy], flops=3 * GF)
        (blurred,) = call(
            forward_kernel, [FOUR], [x_a, x_b, mid, fz, fy, fx],
            scratch=[((VIEWS, 2 * REACH, Y, Z), F32)], limit=24, flops=4 * GF,
        )
        if iteration == 0:
            data = sums
        else:
            lane = lax.broadcasted_iota(jnp.int32, (8, Z), 1)
            data = jnp.where(lane < 8, data, sums)
        x_a, x_b, mid, missed = call(
            backward_kernel, [XS, XS, FOUR, ROW], [data, view_weights, norm, blurred, view_images, bz, by, bx],
            specs=[VM, SM, SM] + [VM] * 5,
            scratch=[((VIEWS, 2 * REACH, Y, Z), F32)], limit=24, flops=4 * GF,
        )
        x_a, x_b = swap(x_a, x_b, "gx")
        (own,) = call(backward_own_kernel, [OWN], [mid, bz, by], flops=3 * GF)
        kept, y_a, y_b = call(
            add_x_kernel, [((X + 6, Y, Z), F32), YS, YS], [own, x_a, x_b], scratch=[OWN],
        )
        y_a, y_b = swap(y_a, y_b, "gy")
        main, z_a, z_b = call(add_y_kernel, [CUBE, Z3, Z3], [kept, y_a, y_b], scratch=[((X + 6, Y, Z), F32)])
        z_a, z_b = swap(z_a, z_b, "gz")
        if iteration + 1 < ITERS:
            estimate, z_a, z_b, row = call(
                update_kernel, [CUBE, ZS, ZS, ROW], [main, z_a, z_b, estimate, ax, ayz, missed]
            )
        else:
            last = all_sum(missed)
            (estimate,) = call(finish_kernel, [CUBE], [main, z_a, z_b, estimate])
            misfits = [data[0, 12:16] / data[0, 4:8], last[0, 12:16] / data[0, 4:8]]
    return (estimate, jnp.stack(misfits))


def solution(mesh):
    torus = Mesh(
        mesh.devices.reshape(2, 4, 2, mesh.shape["gy"], mesh.shape["gz"]),
        ("gx_0", "gx_1", "gx_2", "gy", "gz"),
    )
    in_specs = (P(GX, "gy", "gz"), P(None, GX, "gy", "gz"), P(), P())
    out_specs = (P(GX, "gy", "gz"), P())
    return jax.shard_map(local, mesh=torus, in_specs=in_specs, out_specs=out_specs, check_vma=False)
```

```python
import jax
import jax.numpy as jnp
from jax import lax
from jax.experimental import pallas as pl
from jax.experimental.pallas import tpu as pltpu
from jax.sharding import Mesh
from jax.sharding import PartitionSpec as P


TAPS = 31
REACH = 15
ITERS = 2
VIEWS = 4
X, Y, Z = 24, 32, 128
YE = 64
F32 = jnp.float32
BF16 = jnp.bfloat16
GX = ("gx_0", "gx_1", "gx_2")
AXES = {"gx": GX, "gy": "gy", "gz": "gz"}


def parity(name):
    if name == "gx":
        return lax.axis_index("gx_2")
    return lax.rem(lax.axis_index(name), 2)


def position(name):
    if name == "gx":
        return (lax.axis_index("gx_0") * 4 + lax.axis_index("gx_1")) * 2 + lax.axis_index("gx_2")
    return lax.axis_index(name)


def lanes(shape):
    return lax.broadcasted_iota(jnp.int32, shape, len(shape) - 1)


def split(value):
    high = value.astype(BF16)
    low = (value - high.astype(F32)).astype(BF16)
    return high, low


def left_exact(matrix, data):
    high, low = split(data)
    return jnp.dot(matrix, high, preferred_element_type=F32) + jnp.dot(matrix, low, preferred_element_type=F32)


def right_exact(data, matrix):
    rows = data.shape[0]
    both = jnp.dot(jnp.concatenate(split(data), axis=0), matrix, preferred_element_type=F32)
    return both[:rows] + both[rows:]


def extended_offset(index, size, width, odd):
    low_first = index < size + width
    local = jnp.where(low_first, index - size, index - size - width)
    upper = low_first == (odd == 0)
    outside = jnp.where(upper, size + local, local - width)
    return jnp.where(index < size, index, outside)


def taps_matrix(taps_ref, view, axis, source, target):
    tap = source - target + REACH
    out = jnp.zeros(tap.shape, F32)
    for t in range(TAPS):
        out = jnp.where(tap == t, taps_ref[view, axis, t].astype(F32) / 256.0, out)
    return out


def select_matrix(rows, columns, match):
    r = lax.broadcasted_iota(jnp.int32, (rows, columns), 0)
    c = lax.broadcasted_iota(jnp.int32, (rows, columns), 1)
    return match(r, c)


def one_hot(rows, columns, match):
    return jnp.where(select_matrix(rows, columns, match), 1.0, 0.0).astype(BF16)


def setup_kernel(taps_ref, fz, fy, fx, bz, by, bx):
    odd_x, odd_y, odd_z = parity("gx"), parity("gy"), parity("gz")
    XE = X + 2 * REACH

    def one_view(v, carry):
        lane0 = pl.multiple_of(v * Z, Z)
        raw = lax.broadcasted_iota(jnp.int32, (256, Z), 0)
        tgt = lax.broadcasted_iota(jnp.int32, (256, Z), 1)
        src = jnp.where(raw < Z + 32, extended_offset(raw, Z, 16, odd_z), -1000)
        band = taps_matrix(taps_ref, v, 2, src, tgt)
        fz[:, pl.ds(lane0, Z)] = band.astype(BF16)
        bz[pl.ds(lane0, Z), :] = band.T.astype(BF16)
        tgt = lax.broadcasted_iota(jnp.int32, (Y, YE), 0)
        src = extended_offset(lax.broadcasted_iota(jnp.int32, (Y, YE), 1), Y, 16, odd_y)
        base = taps_matrix(taps_ref, v, 1, src, tgt).astype(BF16)
        spread = jnp.dot(one_hot(4 * Y, Y, lambda r, c: lax.rem(r, Y) == c), base, preferred_element_type=F32).astype(BF16)
        spread = jnp.dot(spread, one_hot(YE, 4 * YE, lambda r, c: lax.rem(c, YE) == r), preferred_element_type=F32)
        spread = jnp.where(select_matrix(4 * Y, 4 * YE, lambda r, c: r // Y == c // YE), spread, 0.0)
        fy[v] = spread.astype(BF16)
        by[v] = spread.T.astype(BF16)
        tgt = lax.broadcasted_iota(jnp.int32, (X, XE), 0)
        src = extended_offset(lax.broadcasted_iota(jnp.int32, (X, XE), 1), X, REACH, odd_x)
        base = taps_matrix(taps_ref, v, 0, src, tgt).astype(BF16)
        spread = jnp.dot(one_hot(X * 8, X, lambda r, c: r // 8 == c), base, preferred_element_type=F32).astype(BF16)
        spread = jnp.dot(spread, one_hot(XE, XE * 8, lambda r, c: c // 8 == r), preferred_element_type=F32)
        spread = jnp.where(select_matrix(X * 8, XE * 8, lambda r, c: lax.rem(r, 8) == lax.rem(c, 8)), spread, 0.0)
        fx[v] = spread.astype(BF16)
        wide = jnp.concatenate([spread, jnp.zeros((X * 8, 512 - XE * 8), F32)], axis=1).T
        bx[v] = wide[: XE * 8].astype(BF16)
        return carry

    lax.fori_loop(0, VIEWS, one_view, 0)


def reach_kernel(taps_ref, weights, ax, ayz, share):
    def reachable(v, axis, name, size, count, iota):
        where_global = position(name) * size + iota
        out = jnp.zeros(iota.shape, F32)
        for t in range(TAPS):
            at = where_global - t + REACH
            inside = (at >= 0) & (at < count * size)
            out = out + jnp.where(inside, taps_ref[v, axis, t].astype(F32) / 256.0, 0.0)
        return out

    lane = lanes((8, Z))

    def one_view(v, carry):
        shares, norm = carry
        ax[v] = reachable(v, 0, "gx", X, 16, lax.broadcasted_iota(jnp.int32, (X, Z), 0))
        along_y = reachable(v, 1, "gy", Y, 4, lax.broadcasted_iota(jnp.int32, (Y, Z), 0))
        along_z = reachable(v, 2, "gz", Z, 4, lax.broadcasted_iota(jnp.int32, (8, Z), 1))
        ayz[v] = along_y * along_z[0:1]
        weight = weights[v].astype(F32)
        whole = jnp.full((8, Z), 1.0, F32)
        for axis in range(3):
            taps = jnp.zeros((), jnp.int32)
            for t in range(TAPS):
                taps = taps + taps_ref[v, axis, t]
            whole = whole * (taps.astype(F32) / 256.0)
        return jnp.where(lane == v, weight, shares), norm + weight * whole

    shares, norm = lax.fori_loop(0, VIEWS, one_view, (jnp.zeros((8, Z), F32), jnp.zeros((8, Z), F32)))
    share[...] = shares / norm


def pack_sides(side_a, side_b, store, store_rest):
    lane = lanes((YE, Z))
    quarter = lanes((16, Z)) // 32
    for i in range(3):
        a, b = side_a(i), side_b(i)
        store(i, jnp.where(lane < 80, a, pltpu.roll(b, 80, 1)))
        rest = pltpu.roll(b, Z - 48, 1)
        packed = rest[0:16]
        for q in range(1, 4):
            packed = jnp.where(quarter == q, pltpu.roll(rest[16 * q : 16 * q + 16], 32 * q, 1), packed)
        store_rest(i, packed)


def unpack_sides(tile, packed):
    lane = lanes((YE, Z))
    parts = [packed] + [pltpu.roll(packed, Z - 32 * q, 1) for q in range(1, 4)]
    rest = jnp.concatenate(parts, axis=0)
    a = jnp.where(lane < 80, tile, 0.0)
    b = jnp.where(lane < 48, pltpu.roll(tile, Z - 80, 1), pltpu.roll(rest, 48, 1))
    return a, jnp.where(lane < 80, b, 0.0)


def pack_z(load, z_a, z_b, row=None):
    group = lanes((3 * Y, Z)) // 16
    up = jnp.zeros((3 * Y, Z), F32)
    down = jnp.zeros((3 * Y, Z), F32)
    for g in range(8):
        part = load(g)
        up = jnp.where(group == g, pltpu.roll(part, (16 * g + 16) % Z, 1) if g != 7 else part, up)
        down = jnp.where(group == g, pltpu.roll(part, 16 * g, 1) if g else part, down)
    odd = parity("gz")
    z_a[0 : 3 * Y] = jnp.where(odd == 0, up, down)
    z_b[0 : 3 * Y] = jnp.where(odd == 0, down, up)
    if row is not None:
        z_a[3 * Y :] = row


def blurred_totals(load, ax, ayz):
    lane = lanes((8, Z))
    row = lax.broadcasted_iota(jnp.int32, (8, Z), 0)
    out = jnp.zeros((8, Z), F32)
    for v in range(VIEWS):
        acc = jnp.zeros((Y, Z), F32)
        for i in range(X):
            acc = acc + load(i) * ax[v, i : i + 1, :]
        total = jnp.sum(acc * ayz[v])
        out = jnp.where((lane == 8 + v) & (row == 0), total, out)
    return out


def first_kernel(est, z_a, z_b):
    pack_z(lambda g: est[3 * g : 3 * g + 3].reshape(3 * Y, Z), z_a, z_b)


def sums_kernel(est, views, ax, ayz, row_ref):
    lane = lanes((8, Z))
    row = lax.broadcasted_iota(jnp.int32, (8, Z), 0)
    out = blurred_totals(lambda i: est[i], ax, ayz)
    for v in range(VIEWS):
        total = jnp.zeros((Y, Z), F32)
        square = jnp.zeros((Y, Z), F32)
        for i in range(X):
            image = views[v, i]
            total = total + image
            square = square + image * image
        out = jnp.where((lane == v) & (row == 0), jnp.sum(total), out)
        out = jnp.where((lane == 4 + v) & (row == 0), jnp.sum(square), out)
    row_ref[...] = out


def pack_y_kernel(est, z_a, z_b, row, y_a, y_b, row_out):
    odd = parity("gy")
    start_a = pl.multiple_of((1 - odd) * 16, 16)
    start_b = pl.multiple_of(odd * 16, 16)
    for start, out in ((start_a, y_a), (start_b, y_b)):
        out[0:X] = est[:, pl.ds(start, 16), :]
        for i in range(3):
            out[X + i] = z_a[pl.ds(start + i * Y, 16)]
            out[X + 3 + i] = z_b[pl.ds(start + i * Y, 16)]
    total = row[...]
    if z_a.shape[0] > 3 * Y:
        total = total + z_a[3 * Y :]
    row_out[...] = total
    y_a[X + 6, 0:8] = total
    y_a[X + 6, 8:16] = total


def pack_x_kernel(est, z_a, z_b, y_a, y_b, row, own, x_a, x_b, row_out):
    own[0:X, 0:Y] = est[...]
    for i in range(3):
        own[X + i, 0:Y] = z_a[i * Y : i * Y + Y]
        own[X + 3 + i, 0:Y] = z_b[i * Y : i * Y + Y]
    own[:, Y : Y + 16] = y_a[0 : X + 6]
    own[:, Y + 16 : YE] = y_b[...]
    total = row[...] + y_a[X + 6, 0:8]
    row_out[...] = total
    odd = parity("gx")
    for flag, out in ((odd, x_a), (1 - odd, x_b)):
        out[0:REACH] = own[pl.ds((1 - flag) * 9, REACH)]

        def side(first):
            def get(i, flag=flag):
                full = own[first + i]
                return jnp.where(flag == 0, pltpu.roll(full, Z - 48, 1), full)

            return get

        def store(i, value, out=out):
            out[REACH + i] = value

        def store_rest(i, value, out=out):
            out[REACH + 3, 16 * i : 16 * i + 16] = value

        pack_sides(side(X), side(X + 3), store, store_rest)
        out[REACH + 3, 48:56] = total
        out[REACH + 3, 56:64] = total


def forward_group(src, sides_ref, first_z, plane, fz, fy, store):
    mains, sides = [], []
    lane = lanes((YE, Z))
    for k in range(4):
        p = plane + k
        g = p // 3
        i = p - 3 * g
        mains.append(src[p])
        a = pltpu.roll(sides_ref[first_z + i], lax.rem(Z - 16 * g, Z), 1)
        b = pltpu.roll(sides_ref[first_z + 3 + i], lax.rem(Z + 16 - 16 * g, Z), 1)
        sides.append(jnp.where(lane < 16, a, b))
    data = jnp.concatenate([jnp.concatenate(mains, 0), jnp.concatenate(sides, 0)], axis=1)
    wide = right_exact(data, fz[...])
    for v in range(VIEWS):
        out = left_exact(fy[v], wide[:, v * Z : (v + 1) * Z])
        store(v, out.reshape(4, Y, Z))


def forward_own_kernel(own, fz, fy, out):
    def step(j, carry):
        plane = j * 4

        def store(v, value):
            out[v, pl.ds(plane, 4)] = value

        forward_group(own, own, X, plane, fz, fy, store)
        return carry

    lax.fori_loop(0, 6, step, 0, unroll=UNROLL)


def forward_halo_kernel(src, fz, fy, out, sides):
    for i in range(3):
        sides[i], sides[3 + i] = unpack_sides(src[REACH + i], src[REACH + 3, 16 * i : 16 * i + 16])

    def step(j, carry):
        plane = jnp.minimum(j * 4, REACH - 4)

        def store(v, value):
            out[v, pl.ds(plane, 4)] = value

        forward_group(src, sides, 0, plane, fz, fy, store)
        return carry

    lax.fori_loop(0, 4, step, 0, unroll=UNROLL)


def forward_last_kernel(mid, halo_a, halo_b, fx, out):
    def one_view(v, carry):
        for pair in range(2):
            columns = []
            for tile in (2 * pair, 2 * pair + 1):
                rows = pl.ds(tile * 8, 8)
                columns.append(
                    jnp.concatenate(
                        [
                            mid[v, :, rows].reshape(X * 8, Z),
                            halo_a[v, :, rows].reshape(REACH * 8, Z),
                            halo_b[v, :, rows].reshape(REACH * 8, Z),
                        ],
                        axis=0,
                    )
                )
            got = left_exact(fx[v], jnp.concatenate(columns, axis=1))
            for k, tile in enumerate((2 * pair, 2 * pair + 1)):
                out[v, :, tile * 8 : tile * 8 + 8] = got[:, k * Z : (k + 1) * Z].reshape(X, 8, Z)
        return carry

    lax.fori_loop(0, VIEWS, one_view, 0, unroll=2)


def pick(row, lane, index):
    return jnp.sum(jnp.where(lane == index, row, 0.0), axis=1, keepdims=True)


def view_scales(sums, share):
    lane = lanes((1, Z))
    row = sums[0:1, :]
    return [pick(share[0:1, :], lane, v) * (pick(row, lane, 8 + v) / pick(row, lane, v)) for v in range(VIEWS)]


def backward_group(load, plane, scales, bz, by, store):
    parts = [left_exact(by[v], load(v, plane).reshape(4 * Y, Z) * scales[v]) for v in range(VIEWS)]
    wide = right_exact(jnp.concatenate(parts, axis=1), bz[...])
    store(wide)


def store_extended(dst, sides_ref, first_z, plane, wide):
    group = lanes((YE, Z)) // 16
    for k in range(4):
        p = plane + k
        g = p // 3
        i = p - 3 * g
        rows = wide[k * YE : (k + 1) * YE]
        dst[p] = rows[:, :Z]
        side = rows[:, Z:]
        a = pltpu.roll(side, lax.rem(16 * g + Z, Z), 1)
        b = pltpu.roll(side, lax.rem(16 * g + Z - 16, Z), 1)
        sides_ref[first_z + i] = jnp.where(group == g, a, sides_ref[first_z + i])
        sides_ref[first_z + 3 + i] = jnp.where(group == g, b, sides_ref[first_z + 3 + i])


def backward_kernel(blurred, views, bx, mid, halo_a, halo_b):
    def one_view(v, carry):
        for pair in range(2):
            tiles = (2 * pair, 2 * pair + 1)
            b = jnp.concatenate([blurred[v, :, t * 8 : t * 8 + 8].reshape(X * 8, Z) for t in tiles], axis=1)
            image = jnp.concatenate([views[v, :, t * 8 : t * 8 + 8].reshape(X * 8, Z) for t in tiles], axis=1)
            got = left_exact(bx[v], image / b)
            for k, t in enumerate(tiles):
                piece = got[:, k * Z : (k + 1) * Z]
                rows = slice(t * 8, t * 8 + 8)
                mid[v, :, rows] = piece[: X * 8].reshape(X, 8, Z)
                halo_a[v, :, rows] = piece[X * 8 : (X + REACH) * 8].reshape(REACH, 8, Z)
                halo_b[v, :, rows] = piece[(X + REACH) * 8 :].reshape(REACH, 8, Z)
        return carry

    lax.fori_loop(0, VIEWS, one_view, 0, unroll=2)


def misfit_kernel(sums, blurred, views, misfit):
    lane = lanes((1, Z))
    row = sums[0:1, :]
    out_lane = lanes((8, Z))
    out_row = lax.broadcasted_iota(jnp.int32, (8, Z), 0)
    misfits = jnp.zeros((8, Z), F32)
    for v in range(VIEWS):
        flux = pick(row, lane, v) / pick(row, lane, 8 + v)

        def plane(i, total, v=v, flux=flux):
            gap = views[v, i] - flux * blurred[v, i]
            return total + gap * gap

        missed = lax.fori_loop(0, X, plane, jnp.zeros((Y, Z), F32), unroll=4)
        misfits = jnp.where((out_lane == 12 + v) & (out_row == 0), jnp.sum(missed), misfits)
    misfit[...] = misfits


def backward_halo_kernel(halo, sums, share, row, bz, by, dst, sides):
    sides[...] = jnp.zeros((6, YE, Z), F32)
    scales = view_scales(sums, share)

    def step(j, carry):
        plane = jnp.minimum(j * 4, REACH - 4)
        backward_group(
            lambda v, p: halo[v, pl.ds(p, 4)], plane, scales, bz, by,
            lambda wide: store_extended(dst, sides, 0, plane, wide),
        )
        return carry

    lax.fori_loop(0, 4, step, 0, unroll=UNROLL)

    def store(i, value):
        dst[REACH + i] = value

    def store_rest(i, value):
        dst[REACH + 3, 16 * i : 16 * i + 16] = value

    pack_sides(lambda i: sides[i], lambda i: sides[3 + i], store, store_rest)
    dst[REACH + 3, 48:56] = row[...]
    dst[REACH + 3, 56:64] = row[...]


def backward_own_kernel(mid, sums, share, bz, by, own):
    own[X : X + 6] = jnp.zeros((6, YE, Z), F32)
    scales = view_scales(sums, share)

    def step(j, carry):
        plane = j * 4
        backward_group(
            lambda v, p: mid[v, pl.ds(p, 4)], plane, scales, bz, by,
            lambda wide: store_extended(own, own, X, plane, wide),
        )
        return carry

    lax.fori_loop(0, 6, step, 0, unroll=UNROLL)


def add_x_kernel(own, x_a, x_b, kept, y_a, y_b, total):
    total[...] = own[...]
    odd = parity("gx")
    for flag, src in ((odd, x_a), (1 - odd, x_b)):
        spot = pl.ds((1 - flag) * 9, REACH)
        total[spot] = total[spot] + src[0:REACH]
        for i in range(3):
            sides = unpack_sides(src[REACH + i], src[REACH + 3, 16 * i : 16 * i + 16])
            for k, side in enumerate(sides):
                at = X + 3 * k + i
                total[at] = total[at] + jnp.where(flag == 0, pltpu.roll(side, 48, 1), side)
    kept[...] = total[:, 0:Y]
    y_a[...] = total[:, Y : Y + 16]
    y_b[...] = total[:, Y + 16 : YE]


def add_y_kernel(kept, y_a, y_b, main, z_a, z_b, total):
    total[...] = kept[...]
    odd = parity("gy")
    for start, src in (((1 - odd) * 16, y_a), (odd * 16, y_b)):
        spot = pl.ds(pl.multiple_of(start, 16), 16)
        total[:, spot] = total[:, spot] + src[...]
    main[...] = total[0:X]
    z_a[...] = total[X : X + 3]
    z_b[...] = total[X + 3 : X + 6]


def corrected(main, z_a, z_b, est, g):
    odd = parity("gz")
    lane = lanes((3 * Y, Z))
    a = z_a[...].reshape(3 * Y, Z)
    b = z_b[...].reshape(3 * Y, Z)
    up = jnp.where(odd == 0, a, b)
    down = jnp.where(odd == 0, b, a)
    up = pltpu.roll(up, (112 - 16 * g) % Z, 1) if g != 7 else up
    down = pltpu.roll(down, (Z - 16 * g) % Z, 1) if g else down
    total = main[3 * g : 3 * g + 3].reshape(3 * Y, Z)
    total = total + jnp.where(lane >= 112, up, 0.0) + jnp.where(lane < 16, down, 0.0)
    return est[3 * g : 3 * g + 3].reshape(3 * Y, Z) * total


def update_kernel(main, z_a, z_b, est, ax, ayz, carry, out, out_a, out_b, row_ref):
    for g in range(8):
        out[3 * g : 3 * g + 3] = corrected(main, z_a, z_b, est, g).reshape(3, Y, Z)
    row = blurred_totals(lambda i: out[i], ax, ayz) + carry[...]
    pack_z(lambda g: out[3 * g : 3 * g + 3].reshape(3 * Y, Z), out_a, out_b, row)
    row_ref[...] = row


def finish_kernel(main, z_a, z_b, est, out):
    for g in range(8):
        out[3 * g : 3 * g + 3] = corrected(main, z_a, z_b, est, g).reshape(3, Y, Z)


VM = pl.BlockSpec(memory_space=pltpu.VMEM)
SM = pl.BlockSpec(memory_space=pltpu.SMEM)


def call(kernel, outs, operands, specs=None, scratch=(), limit=16, flops=0):
    shapes = [jax.ShapeDtypeStruct(shape, dtype) for shape, dtype in outs]
    return pl.pallas_call(
        kernel,
        out_shape=shapes,
        in_specs=specs or [VM] * len(operands),
        out_specs=[VM] * len(shapes),
        scratch_shapes=[pltpu.VMEM(shape, dtype) for shape, dtype in scratch],
        compiler_params=pltpu.CompilerParams(vmem_limit_bytes=limit << 20),
        cost_estimate=pl.CostEstimate(flops=max(flops, 1000), bytes_accessed=1000, transcendentals=0),
    )(*operands)


def swap(a, b, axis):
    names = AXES[axis]
    count = lax.axis_size(names)
    first = [(i, i ^ 1) for i in range(count)]
    second = [(i, i + 1) for i in range(1, count - 1, 2)] + [(i + 1, i) for i in range(1, count - 1, 2)]
    b = lax.ppermute(b, names, second)
    a = lax.ppermute(a, names, first)
    return a, b


def sum_step(row, axis, bit):
    count = lax.axis_size(axis)
    other = lax.ppermute(row, axis, [(i, i ^ bit) for i in range(count)])
    return row + other


UNROLL = 1
ZS = ((3 * Y, Z), F32)
ZR = ((3 * Y + 8, Z), F32)
Z3 = ((3, Y, Z), F32)
YS = ((X + 6, 16, Z), F32)
YR = ((X + 7, 16, Z), F32)
XS = ((REACH + 4, YE, Z), F32)
OWN = ((X + 6, YE, Z), F32)
SIDES = ((6, YE, Z), F32)
CUBE = ((X, Y, Z), F32)
FOUR = ((VIEWS, X, Y, Z), F32)
ROW = ((8, Z), F32)
GF = 1 << 30
HALO = ((VIEWS, REACH, Y, Z), F32)


def local(estimate, view_images, psf_taps, view_weights):
    XE8 = (X + 2 * REACH) * 8
    z_a, z_b = call(first_kernel, [ZS, ZS], [estimate], limit=2)
    ax, ayz, share = call(
        reach_kernel, [((VIEWS, X, Z), F32), ((VIEWS, Y, Z), F32), ROW], [psf_taps, view_weights],
        specs=[SM, SM], limit=2,
    )
    (row,) = call(sums_kernel, [ROW], [estimate, view_images, ax, ayz], limit=2, flops=GF // 4)
    fz, fy, fx, bz, by, bx = call(
        setup_kernel,
        [
            ((256, VIEWS * Z), BF16), ((VIEWS, 4 * Y, 4 * YE), BF16), ((VIEWS, X * 8, XE8), BF16),
            ((VIEWS * Z, 256), BF16), ((VIEWS, 4 * YE, 4 * Y), BF16), ((VIEWS, XE8, X * 8), BF16),
        ],
        [psf_taps], specs=[SM], limit=4, flops=4 * GF,
    )
    row = sum_step(row, "gz", 1)
    data = None
    misfits = []
    for iteration in range(ITERS):
        final = iteration + 1 == ITERS
        z_a, z_b = swap(z_a, z_b, "gz")
        y_a, y_b, row = call(pack_y_kernel, [YR, YS, ROW], [estimate, z_a, z_b, row], limit=2)
        y_a, y_b = swap(y_a, y_b, "gy")
        own, x_a, x_b, row = call(
            pack_x_kernel, [OWN, XS, XS, ROW], [estimate, z_a, z_b, y_a, y_b, row], limit=2
        )
        x_a, x_b = swap(x_a, x_b, "gx")
        row = row + x_a[REACH + 3, 48:56]
        for axis, bit in (("gx_1", 1), ("gx_1", 2), ("gy", 2), ("gx_0", 1), ("gz", 2)):
            row = sum_step(row, axis, bit)
        (mid,) = call(forward_own_kernel, [FOUR], [own, fz, fy], limit=4, flops=3 * GF)
        (halo_a,) = call(forward_halo_kernel, [HALO], [x_a, fz, fy], scratch=[SIDES], limit=4, flops=2 * GF)
        (halo_b,) = call(forward_halo_kernel, [HALO], [x_b, fz, fy], scratch=[SIDES], limit=4, flops=2 * GF)
        (blurred,) = call(forward_last_kernel, [FOUR], [mid, halo_a, halo_b, fx], limit=4, flops=2 * GF)
        mid, halo_a, halo_b = call(
            backward_kernel, [FOUR, HALO, HALO], [blurred, view_images, bx], limit=4, flops=2 * GF
        )
        if iteration == 0:
            data = row
        else:
            lane = lax.broadcasted_iota(jnp.int32, (8, Z), 1)
            data = jnp.where(lane < 8, data, row)
        (missed,) = call(misfit_kernel, [ROW], [data, blurred, view_images], limit=2, flops=GF // 4)
        sent = missed if final else data
        (x_b,) = call(
            backward_halo_kernel, [XS], [halo_b, data, share, data, bz, by],
            scratch=[SIDES], limit=4, flops=2 * GF,
        )
        (x_a,) = call(
            backward_halo_kernel, [XS], [halo_a, data, share, sent, bz, by],
            scratch=[SIDES], limit=4, flops=2 * GF,
        )
        x_a, x_b = swap(x_a, x_b, "gx")
        (own,) = call(backward_own_kernel, [OWN], [mid, data, share, bz, by], limit=4, flops=3 * GF)
        if final:
            last = missed + x_a[REACH + 3, 48:56]
            for axis, bit in (("gx_1", 1), ("gx_1", 2), ("gx_0", 1), ("gy", 1), ("gy", 2)):
                last = sum_step(last, axis, bit)
            others = []
            for bit in (1, 2, 3):
                others.append(lax.ppermute(last, "gz", [(i, i ^ bit) for i in range(lax.axis_size("gz"))]))
            last = (last + others[0]) + (others[1] + others[2])
        kept, y_a, y_b = call(
            add_x_kernel, [((X + 6, Y, Z), F32), YS, YS], [own, x_a, x_b], scratch=[OWN], limit=4
        )
        y_a, y_b = swap(y_a, y_b, "gy")
        main, z_a, z_b = call(add_y_kernel, [CUBE, Z3, Z3], [kept, y_a, y_b], scratch=[((X + 6, Y, Z), F32)], limit=2)
        z_a, z_b = swap(z_a, z_b, "gz")
        if not final:
            estimate, z_a, z_b, row = call(
                update_kernel, [CUBE, ZR, ZS, ROW], [main, z_a, z_b, estimate, ax, ayz, missed], limit=2
            )
        else:
            (estimate,) = call(finish_kernel, [CUBE], [main, z_a, z_b, estimate], limit=2)
            misfits = [data[0, 12:16] / data[0, 4:8], last[0, 12:16] / data[0, 4:8]]
    return (estimate, jnp.stack(misfits))


def solution(mesh):
    torus = Mesh(
        mesh.devices.reshape(2, 4, 2, mesh.shape["gy"], mesh.shape["gz"]),
        ("gx_0", "gx_1", "gx_2", "gy", "gz"),
    )
    in_specs = (P(GX, "gy", "gz"), P(None, GX, "gy", "gz"), P(), P())
    out_specs = (P(GX, "gy", "gz"), P())
    return jax.shard_map(local, mesh=torus, in_specs=in_specs, out_specs=out_specs, check_vma=False)
```

```python
import jax
import jax.numpy as jnp
from jax import lax
from jax.experimental import pallas as pl
from jax.experimental.pallas import tpu as pltpu
from jax.sharding import Mesh
from jax.sharding import PartitionSpec as P


TAPS = 31
REACH = 15
ITERS = 2
VIEWS = 4
X, Y, Z = 24, 32, 128
YE = 64
F32 = jnp.float32
BF16 = jnp.bfloat16
GX = ("gx_0", "gx_1", "gx_2")
AXES = {"gx": GX, "gy": "gy", "gz": "gz"}


def parity(name):
    if name == "gx":
        return lax.axis_index("gx_2")
    return lax.rem(lax.axis_index(name), 2)


def position(name):
    if name == "gx":
        return (lax.axis_index("gx_0") * 4 + lax.axis_index("gx_1")) * 2 + lax.axis_index("gx_2")
    return lax.axis_index(name)


def lanes(shape):
    return lax.broadcasted_iota(jnp.int32, shape, len(shape) - 1)


def split(value):
    high = value.astype(BF16)
    low = (value - high.astype(F32)).astype(BF16)
    return high, low


def left_exact(matrix, data):
    high, low = split(data)
    return jnp.dot(matrix, high, preferred_element_type=F32) + jnp.dot(matrix, low, preferred_element_type=F32)


def right_exact(data, matrix):
    rows = data.shape[0]
    both = jnp.dot(jnp.concatenate(split(data), axis=0), matrix, preferred_element_type=F32)
    return both[:rows] + both[rows:]


def extended_offset(index, size, width, odd):
    low_first = index < size + width
    local = jnp.where(low_first, index - size, index - size - width)
    upper = low_first == (odd == 0)
    outside = jnp.where(upper, size + local, local - width)
    return jnp.where(index < size, index, outside)


def taps_matrix(taps_ref, view, axis, source, target):
    tap = source - target + REACH
    out = jnp.zeros(tap.shape, F32)
    for t in range(TAPS):
        out = jnp.where(tap == t, taps_ref[view, axis, t].astype(F32) / 256.0, out)
    return out


def select_matrix(rows, columns, match):
    r = lax.broadcasted_iota(jnp.int32, (rows, columns), 0)
    c = lax.broadcasted_iota(jnp.int32, (rows, columns), 1)
    return match(r, c)


def one_hot(rows, columns, match):
    return jnp.where(select_matrix(rows, columns, match), 1.0, 0.0).astype(BF16)


def setup_kernel(taps_ref, fz, fy, fx, bz, by, bx):
    odd_x, odd_y, odd_z = parity("gx"), parity("gy"), parity("gz")
    XE = X + 2 * REACH

    def one_view(v, carry):
        lane0 = pl.multiple_of(v * Z, Z)
        raw = lax.broadcasted_iota(jnp.int32, (Z + 32, Z), 0)
        tgt = lax.broadcasted_iota(jnp.int32, (Z + 32, Z), 1)
        band = taps_matrix(taps_ref, v, 2, extended_offset(raw, Z, 16, odd_z), tgt)
        band = jnp.concatenate([band, jnp.zeros((Z - 32, Z), F32)], axis=0)
        fz[:, pl.ds(lane0, Z)] = band.astype(BF16)
        bz[pl.ds(lane0, Z), :] = band.T.astype(BF16)
        tgt = lax.broadcasted_iota(jnp.int32, (Y, YE), 0)
        src = extended_offset(lax.broadcasted_iota(jnp.int32, (Y, YE), 1), Y, 16, odd_y)
        base = taps_matrix(taps_ref, v, 1, src, tgt).astype(BF16)
        spread = jnp.dot(one_hot(4 * Y, Y, lambda r, c: lax.rem(r, Y) == c), base, preferred_element_type=F32).astype(BF16)
        spread = jnp.dot(spread, one_hot(YE, 4 * YE, lambda r, c: lax.rem(c, YE) == r), preferred_element_type=F32)
        spread = jnp.where(select_matrix(4 * Y, 4 * YE, lambda r, c: r // Y == c // YE), spread, 0.0)
        fy[v] = spread.astype(BF16)
        by[v] = spread.T.astype(BF16)
        tgt = lax.broadcasted_iota(jnp.int32, (X, XE), 0)
        src = extended_offset(lax.broadcasted_iota(jnp.int32, (X, XE), 1), X, REACH, odd_x)
        base = taps_matrix(taps_ref, v, 0, src, tgt).astype(BF16)
        spread = jnp.dot(one_hot(X * 8, X, lambda r, c: r // 8 == c), base, preferred_element_type=F32).astype(BF16)
        spread = jnp.dot(spread, one_hot(XE, XE * 8, lambda r, c: c // 8 == r), preferred_element_type=F32)
        spread = jnp.where(select_matrix(X * 8, XE * 8, lambda r, c: lax.rem(r, 8) == lax.rem(c, 8)), spread, 0.0)
        fx[v] = spread.astype(BF16)
        wide = jnp.concatenate([spread, jnp.zeros((X * 8, 512 - XE * 8), F32)], axis=1).T
        bx[v] = wide[: XE * 8].astype(BF16)
        return carry

    lax.fori_loop(0, VIEWS, one_view, 0)


def reach_kernel(taps_ref, weights, along_x, along_y, along_z, sides, sent_a, sent_b, share):
    odd_x, odd_y, odd_z = parity("gx"), parity("gy"), parity("gz")
    lane = lanes((8, Z))
    row = lax.broadcasted_iota(jnp.int32, (8, Z), 0)
    base_x = 3 * (lane // 16)
    near_at = extended_offset(jnp.where(row < 3, base_x + row, X + base_x + row - 3), X, REACH, odd_x)
    far_at = jnp.where(row < 3, X + REACH + base_x + row, lane)
    far_at = extended_offset(far_at, X, REACH, odd_x)
    y_at = extended_offset(lane, Y, 16, odd_y)
    z_at = jnp.where(row == 0, lane, Z + lax.rem(lane, 16) + jnp.where(row == 2, 16, 0))
    z_at = extended_offset(z_at, Z, 16, odd_z)

    def down(values):
        return jnp.broadcast_to(values, (Z, Z)).T

    def one_view(v, carry):
        shares, norm = carry

        def reach(axis, name, size, count, *indices):
            outs = [jnp.zeros((8, Z), F32) for _ in indices]
            ats = [position(name) * size + index + REACH for index in indices]
            taps = jnp.zeros((), jnp.int32)
            for t in range(TAPS):
                tap = taps_ref[v, axis, t]
                taps = taps + tap
                value = tap.astype(F32) / 256.0
                outs = [
                    out + jnp.where((at >= t) & (at < count * size + t), value, 0.0) for out, at in zip(outs, ats)
                ]
            return outs, taps.astype(F32) / 256.0

        (near, far), whole_x = reach(0, "gx", X, 16, near_at, far_at)
        (rows_y,), whole_y = reach(1, "gy", Y, 4, y_at)
        (rows_z,), whole_z = reach(2, "gz", Z, 4, z_at)
        weight = weights[v].astype(F32)
        along_x[v] = down(far[3:4])[0:56]
        spread_y = down(rows_y[0:1])[0:YE]
        along_y[v] = spread_y
        along_z[v] = rows_z
        z_side = (rows_z[1:2], rows_z[2:3])
        for k in range(2):
            sides[v, 8 * k : 8 * k + 8] = near * z_side[k]
        for source, first, dst in ((near, 3, sent_a), (far, 0, sent_b)):
            def tile(k, source=source, first=first):
                return lambda i: spread_y * (source[first + i : first + i + 1] * z_side[k])

            def store(i, value, dst=dst):
                dst[v, i] = value

            def store_rest(i, value, dst=dst):
                dst[v, 3, 16 * i : 16 * i + 16] = value

            pack_sides(tile(0), tile(1), store, store_rest)
            dst[v, 3, 48:64] = jnp.zeros((16, Z), F32)
        whole = jnp.full((8, Z), whole_x * whole_y * whole_z, F32)
        return jnp.where(lane == v, weight, shares), norm + weight * whole

    shares, norm = lax.fori_loop(0, VIEWS, one_view, (jnp.zeros((8, Z), F32), jnp.zeros((8, Z), F32)))
    share[...] = shares / norm


def pack_sides(side_a, side_b, store, store_rest):
    lane = lanes((YE, Z))
    quarter = lanes((16, Z)) // 32
    for i in range(3):
        a, b = side_a(i), side_b(i)
        store(i, jnp.where(lane < 80, a, pltpu.roll(b, 80, 1)))
        rest = pltpu.roll(b, Z - 48, 1)
        packed = rest[0:16]
        for q in range(1, 4):
            packed = jnp.where(quarter == q, pltpu.roll(rest[16 * q : 16 * q + 16], 32 * q, 1), packed)
        store_rest(i, packed)


def unpack_sides(tile, packed):
    lane = lanes((YE, Z))
    parts = [packed] + [pltpu.roll(packed, Z - 32 * q, 1) for q in range(1, 4)]
    rest = jnp.concatenate(parts, axis=0)
    a = jnp.where(lane < 80, tile, 0.0)
    b = jnp.where(lane < 48, pltpu.roll(tile, Z - 80, 1), pltpu.roll(rest, 48, 1))
    return a, jnp.where(lane < 80, b, 0.0)


def pack_z(load, z_a, z_b):
    group = lanes((3 * Y, Z)) // 16
    up = jnp.zeros((3 * Y, Z), F32)
    down = jnp.zeros((3 * Y, Z), F32)
    for g in range(8):
        part = load(g)
        up = jnp.where(group == g, pltpu.roll(part, (16 * g + 16) % Z, 1) if g != 7 else part, up)
        down = jnp.where(group == g, pltpu.roll(part, 16 * g, 1) if g else part, down)
    odd = parity("gz")
    z_a[...] = jnp.where(odd == 0, up, down)
    z_b[...] = jnp.where(odd == 0, down, up)


def blurred_totals(load, along_x, along_y, along_z):
    lane = lanes((8, Z))
    row = lax.broadcasted_iota(jnp.int32, (8, Z), 0)
    out = jnp.zeros((8, Z), F32)
    for v in range(VIEWS):
        acc = jnp.zeros((Y, Z), F32)
        for i in range(X):
            acc = acc + load(i) * along_x[v, i : i + 1, :]
        total = jnp.sum(acc * along_y[v, 0:Y] * along_z[v, 0:1])
        out = jnp.where((lane == 8 + v) & (row == 0), total, out)
    return out


def first_kernel(est, z_a, z_b, kept):
    kept[...] = est[...]
    pack_z(lambda g: est[3 * g : 3 * g + 3].reshape(3 * Y, Z), z_a, z_b)


def sums_kernel(est, views, along_x, along_y, along_z, row_ref):
    lane = lanes((8, Z))
    row = lax.broadcasted_iota(jnp.int32, (8, Z), 0)
    out = blurred_totals(lambda i: est[i], along_x, along_y, along_z)
    for v in range(VIEWS):
        total = jnp.zeros((Y, Z), F32)
        square = jnp.zeros((Y, Z), F32)
        for i in range(X):
            image = views[v, i]
            total = total + image
            square = square + image * image
        out = jnp.where((lane == v) & (row == 0), jnp.sum(total), out)
        out = jnp.where((lane == 4 + v) & (row == 0), jnp.sum(square), out)
    row_ref[...] = out


def pack_y_kernel(est, z_a, z_b, *refs):
    row, y_a, y_b = refs if len(refs) == 3 else (None, *refs)
    odd = parity("gy")
    start_a = pl.multiple_of((1 - odd) * 16, 16)
    start_b = pl.multiple_of(odd * 16, 16)
    for start, out in ((start_a, y_a), (start_b, y_b)):
        out[0:X] = est[:, pl.ds(start, 16), :]
        for i in range(3):
            out[X + i] = z_a[pl.ds(start + i * Y, 16)]
            out[X + 3 + i] = z_b[pl.ds(start + i * Y, 16)]
    if row is not None:
        y_a[X + 6, 0:8] = row[...]
        y_a[X + 6, 8:16] = row[...]


def pack_x_kernel(est, z_a, z_b, y_a, y_b, row, own, x_a, x_b, row_out):
    own[0:X, 0:Y] = est[...]
    for i in range(3):
        own[X + i, 0:Y] = z_a[i * Y : i * Y + Y]
        own[X + 3 + i, 0:Y] = z_b[i * Y : i * Y + Y]
    own[:, Y : Y + 16] = y_a[0 : X + 6]
    own[:, Y + 16 : YE] = y_b[...]
    total = row[...] + y_a[X + 6, 0:8] if y_a.shape[0] > X + 6 else row[...]
    row_out[...] = total
    odd = parity("gx")
    for flag, out in ((odd, x_a), (1 - odd, x_b)):
        out[0:REACH] = own[pl.ds((1 - flag) * 9, REACH)]

        def side(first):
            def get(i, flag=flag):
                full = own[first + i]
                return jnp.where(flag == 0, pltpu.roll(full, Z - 48, 1), full)

            return get

        def store(i, value, out=out):
            out[REACH + i] = value

        def store_rest(i, value, out=out):
            out[REACH + 3, 16 * i : 16 * i + 16] = value

        pack_sides(side(X), side(X + 3), store, store_rest)
        out[REACH + 3, 48:56] = total
        out[REACH + 3, 56:64] = total


def forward_group(src, sides_ref, plane, fz, fy, store):
    mains, sides = [], []
    lane = lanes((YE, Z))
    for k in range(4):
        p = plane + k
        g, spot = side_spot(p)
        mains.append(src[p])
        a = pltpu.roll(sides_ref[spot], lax.rem(Z - 16 * g, Z), 1)
        b = pltpu.roll(sides_ref[spot + 3], lax.rem(Z + 16 - 16 * g, Z), 1)
        sides.append(jnp.where(lane < 16, a, b))
    data = jnp.concatenate([jnp.concatenate(mains, 0), jnp.concatenate(sides, 0)], axis=1)
    wide = right_exact(data, fz[...])
    for v in range(VIEWS):
        out = left_exact(fy[v], wide[:, v * Z : (v + 1) * Z])
        store(v, out.reshape(4, Y, Z))


def side_spot(p):
    beyond = (p >= X).astype(jnp.int32)
    local_plane = p - X * beyond
    g = local_plane // 3
    return g, local_plane - 3 * g + 6 * beyond


def forward_most_kernel(own, x_a, fz, fy, out, src, sides):
    src[0:X] = own[0:X]
    src[X:] = x_a[0:REACH]
    sides[0:6] = own[X:]
    for i in range(3):
        sides[6 + i], sides[9 + i] = unpack_sides(x_a[REACH + i], x_a[REACH + 3, 16 * i : 16 * i + 16])

    def step(j, carry):
        plane = jnp.minimum(j * 4, X + REACH - 4)

        def store(v, value):
            out[v, pl.ds(plane, 4)] = value

        forward_group(src, sides, plane, fz, fy, store)
        return carry

    lax.fori_loop(0, 10, step, 0, unroll=MOST_UNROLL)


def forward_halo_kernel(src, fz, fy, out, sides):
    for i in range(3):
        sides[i], sides[3 + i] = unpack_sides(src[REACH + i], src[REACH + 3, 16 * i : 16 * i + 16])

    def step(j, carry):
        plane = jnp.minimum(j * 4, REACH - 4)

        def store(v, value):
            out[v, pl.ds(plane, 4)] = value

        forward_group(src, sides, plane, fz, fy, store)
        return carry

    lax.fori_loop(0, 4, step, 0, unroll=HALO_UNROLL)


def forward_last_kernel(mid, halo_b, fx, out):
    def one_view(v, carry):
        for pair in range(2):
            columns = []
            for tile in (2 * pair, 2 * pair + 1):
                rows = pl.ds(tile * 8, 8)
                columns.append(
                    jnp.concatenate(
                        [
                            mid[v, :, rows].reshape((X + REACH) * 8, Z),
                            halo_b[v, :, rows].reshape(REACH * 8, Z),
                        ],
                        axis=0,
                    )
                )
            got = left_exact(fx[v], jnp.concatenate(columns, axis=1))
            for k, tile in enumerate((2 * pair, 2 * pair + 1)):
                out[v, :, tile * 8 : tile * 8 + 8] = got[:, k * Z : (k + 1) * Z].reshape(X, 8, Z)
        return carry

    lax.fori_loop(0, VIEWS, one_view, 0, unroll=2)


def pick(row, lane, index):
    return jnp.sum(jnp.where(lane == index, row, 0.0), axis=1, keepdims=True)


def view_scales(sums, share):
    lane = lanes((1, Z))
    row = sums[0:1, :]
    return [pick(share[0:1, :], lane, v) * (pick(row, lane, 8 + v) / pick(row, lane, v)) for v in range(VIEWS)]


def backward_group(load, plane, scales, bz, by, store):
    parts = [left_exact(by[v], load(v, plane).reshape(4 * Y, Z) * scales[v]) for v in range(VIEWS)]
    wide = right_exact(jnp.concatenate(parts, axis=1), bz[...])
    store(wide)


def store_extended(dst, sides_ref, plane, wide):
    group = lanes((YE, Z)) // 16
    for k in range(4):
        p = plane + k
        g, spot = side_spot(p)
        rows = wide[k * YE : (k + 1) * YE]
        dst[p] = rows[:, :Z]
        side = rows[:, Z:]
        a = pltpu.roll(side, lax.rem(16 * g + Z, Z), 1)
        b = pltpu.roll(side, lax.rem(16 * g + Z - 16, Z), 1)
        sides_ref[spot] = jnp.where(group == g, a, sides_ref[spot])
        sides_ref[spot + 3] = jnp.where(group == g, b, sides_ref[spot + 3])


def backward_kernel(blurred, views, bx, mid, halo_b):
    def one_view(v, carry):
        for pair in range(2):
            tiles = (2 * pair, 2 * pair + 1)
            b = jnp.concatenate([blurred[v, :, t * 8 : t * 8 + 8].reshape(X * 8, Z) for t in tiles], axis=1)
            image = jnp.concatenate([views[v, :, t * 8 : t * 8 + 8].reshape(X * 8, Z) for t in tiles], axis=1)
            got = left_exact(bx[v], image / b)
            for k, t in enumerate(tiles):
                piece = got[:, k * Z : (k + 1) * Z]
                rows = slice(t * 8, t * 8 + 8)
                mid[v, :, rows] = piece[: (X + REACH) * 8].reshape(X + REACH, 8, Z)
                halo_b[v, :, rows] = piece[(X + REACH) * 8 :].reshape(REACH, 8, Z)
        return carry

    lax.fori_loop(0, VIEWS, one_view, 0, unroll=2)


def misfit_kernel(sums, blurred, views, misfit):
    lane = lanes((1, Z))
    row = sums[0:1, :]
    out_lane = lanes((8, Z))
    out_row = lax.broadcasted_iota(jnp.int32, (8, Z), 0)
    misfits = jnp.zeros((8, Z), F32)
    for v in range(VIEWS):
        flux = pick(row, lane, v) / pick(row, lane, 8 + v)

        def plane(i, total, v=v, flux=flux):
            gap = views[v, i] - flux * blurred[v, i]
            return total + gap * gap

        missed = lax.fori_loop(0, X, plane, jnp.zeros((Y, Z), F32), unroll=4)
        misfits = jnp.where((out_lane == 12 + v) & (out_row == 0), jnp.sum(missed), misfits)
    misfit[...] = misfits


def centred_kernel(sums, blurred, views, out):
    lane = lanes((1, Z))
    row = sums[0:1, :]
    out_lane = lanes((8, Z))
    out_row = lax.broadcasted_iota(jnp.int32, (8, Z), 0)
    total = jnp.zeros((8, Z), F32)
    for v in range(VIEWS):
        centre = pick(row, lane, v) / pick(row, lane, 8 + v)

        def plane(i, carry, v=v, centre=centre):
            value = blurred[v, i]
            gap = views[v, i] - centre * value
            return carry[0] + gap * gap, carry[1] + gap * value, carry[2] + value * value

        zero = jnp.zeros((Y, Z), F32)
        for k, part in enumerate(lax.fori_loop(0, X, plane, (zero, zero, zero), unroll=4)):
            total = jnp.where((out_lane == 12 + 4 * k + v) & (out_row == 0), jnp.sum(part), total)
    out[...] = total


def report_kernel(first, sums, last, out):
    def at(row, start):
        return pltpu.roll(row, Z - start, 1) if start else row

    before, now, end = first[...], sums[...], last[...]
    square = at(now, 4)
    shift = now / at(now, 8) - before / at(before, 8)
    missed = at(end, 12) - 2.0 * shift * at(end, 16) + shift * shift * at(end, 20)
    out[0:1] = (at(now, 12) / square)[0:1, 0:VIEWS]
    out[1:2] = (missed / square)[0:1, 0:VIEWS]


def backward_halo_kernel(halo, sums, share, bz, by, dst, sides):
    sides[...] = jnp.zeros((6, YE, Z), F32)
    scales = view_scales(sums, share)

    def step(j, carry):
        plane = jnp.minimum(j * 4, REACH - 4)
        backward_group(
            lambda v, p: halo[v, pl.ds(p, 4)], plane, scales, bz, by,
            lambda wide: store_extended(dst, sides, plane, wide),
        )
        return carry

    lax.fori_loop(0, 4, step, 0, unroll=HALO_UNROLL)
    send_sides(dst, sides, 0, None)


def send_sides(dst, sides, first, row):
    def store(i, value):
        dst[REACH + i] = value

    def store_rest(i, value):
        dst[REACH + 3, 16 * i : 16 * i + 16] = value

    pack_sides(lambda i: sides[first + i], lambda i: sides[first + 3 + i], store, store_rest)
    for start in (48, 56):
        dst[REACH + 3, start : start + 8] = jnp.zeros((8, Z), F32) if row is None else row[...]


def backward_most_kernel(mid, sums, share, row, bz, by, own, x_a, sides):
    sides[...] = jnp.zeros((12, YE, Z), F32)
    scales = view_scales(sums, share)

    def step(j, carry):
        plane = jnp.minimum(j * 4, X + REACH - 4)
        backward_group(
            lambda v, p: mid[v, pl.ds(p, 4)], plane, scales, bz, by,
            lambda wide: store_extended(own, sides, plane, wide),
        )
        return carry

    lax.fori_loop(0, 10, step, 0, unroll=MOST_UNROLL)
    own[X + REACH :] = sides[0:6]
    x_a[0:REACH] = own[X : X + REACH]
    send_sides(x_a, sides, 6, row)


def totals_kernel(missed, own_f, xa_f, xb_f, own_b, xa_b, xb_b, along_x, along_y, along_z, sides, sent_a, sent_b, out):
    def planes(left, right, count, first, accs):
        def one(p, accs):
            product = left[p] * right[p]
            return tuple(acc + product * along_x[v, pl.ds(first + p, 1), :] for v, acc in enumerate(accs))

        return lax.fori_loop(0, count, one, accs, unroll=3)

    accs = tuple(jnp.zeros((YE, Z), F32) for _ in range(VIEWS))
    accs = planes(own_f, own_b, X, 0, accs)
    accs = planes(xa_f, xa_b, REACH, X, accs)
    accs = planes(xb_f, xb_b, REACH, X + REACH, accs)
    lane = lanes((8, Z))
    row = lax.broadcasted_iota(jnp.int32, (8, Z), 0)
    result = missed[...]
    for v in range(VIEWS):
        acc = accs[v] * along_z[v, 0:1]
        for k in range(2):
            for i in range(3):
                product = own_f[X + 3 * k + i] * own_b[X + REACH + 3 * k + i]
                acc = acc + product * sides[v, 8 * k + i : 8 * k + i + 1]
        acc = acc * along_y[v]
        for left, right, weight in ((xa_f, xa_b, sent_a), (xb_f, xb_b, sent_b)):
            for i in range(4):
                acc = acc + left[REACH + i] * right[REACH + i] * weight[v, i]
        result = jnp.where((lane == 8 + v) & (row == 0), jnp.sum(acc), result)
    out[...] = result


def add_x_kernel(own, x_a, x_b, kept, y_a, y_b, total):
    total[0:X] = own[0:X]
    total[X:] = own[X + REACH :]
    odd = parity("gx")
    for flag, src in ((odd, x_a), (1 - odd, x_b)):
        spot = pl.ds((1 - flag) * 9, REACH)
        total[spot] = total[spot] + src[0:REACH]
        for i in range(3):
            sides = unpack_sides(src[REACH + i], src[REACH + 3, 16 * i : 16 * i + 16])
            for k, side in enumerate(sides):
                at = X + 3 * k + i
                total[at] = total[at] + jnp.where(flag == 0, pltpu.roll(side, 48, 1), side)
    kept[...] = total[:, 0:Y]
    y_a[...] = total[:, Y : Y + 16]
    y_b[...] = total[:, Y + 16 : YE]


def add_y_kernel(kept, y_a, y_b, row, main, z_a, z_b, total):
    total[...] = kept[...]
    odd = parity("gy")
    for start, src in (((1 - odd) * 16, y_a), (odd * 16, y_b)):
        spot = pl.ds(pl.multiple_of(start, 16), 16)
        total[:, spot] = total[:, spot] + src[...]
    main[...] = total[0:X]
    for i in range(3):
        z_a[Y * i : Y * i + Y] = total[X + i]
        z_b[Y * i : Y * i + Y] = total[X + 3 + i]
    z_a[3 * Y :] = row[...]


def corrected(main, z_a, z_b, est, g):
    odd = parity("gz")
    lane = lanes((3 * Y, Z))
    a = z_a[0 : 3 * Y]
    b = z_b[...]
    up = jnp.where(odd == 0, a, b)
    down = jnp.where(odd == 0, b, a)
    up = pltpu.roll(up, (112 - 16 * g) % Z, 1) if g != 7 else up
    down = pltpu.roll(down, (Z - 16 * g) % Z, 1) if g else down
    total = main[3 * g : 3 * g + 3].reshape(3 * Y, Z)
    total = total + jnp.where(lane >= 112, up, 0.0) + jnp.where(lane < 16, down, 0.0)
    return est[3 * g : 3 * g + 3].reshape(3 * Y, Z) * total


def update_kernel(main, z_a, z_b, est, row, out, out_a, out_b, row_out):
    for g in range(8):
        out[3 * g : 3 * g + 3] = corrected(main, z_a, z_b, est, g).reshape(3, Y, Z)
    pack_z(lambda g: out[3 * g : 3 * g + 3].reshape(3 * Y, Z), out_a, out_b)
    row_out[...] = row[...] + z_a[3 * Y :]


def finish_kernel(main, z_a, z_b, est, out):
    for g in range(8):
        out[3 * g : 3 * g + 3] = corrected(main, z_a, z_b, est, g).reshape(3, Y, Z)


VM = pl.BlockSpec(memory_space=pltpu.VMEM)
SM = pl.BlockSpec(memory_space=pltpu.SMEM)


def call(kernel, outs, operands, specs=None, scratch=(), limit=16, flops=0):
    shapes = [jax.ShapeDtypeStruct(shape, dtype) for shape, dtype in outs]
    return pl.pallas_call(
        kernel,
        out_shape=shapes,
        in_specs=specs or [VM] * len(operands),
        out_specs=[VM] * len(shapes),
        scratch_shapes=[pltpu.VMEM(shape, dtype) for shape, dtype in scratch],
        compiler_params=pltpu.CompilerParams(vmem_limit_bytes=limit << 20),
        cost_estimate=pl.CostEstimate(flops=max(flops, 1000), bytes_accessed=1000, transcendentals=0),
    )(*operands)


def swap(a, b, axis):
    names = AXES[axis]
    count = lax.axis_size(names)
    first = [(i, i ^ 1) for i in range(count)]
    second = [(i, i + 1) for i in range(1, count - 1, 2)] + [(i + 1, i) for i in range(1, count - 1, 2)]
    b = lax.ppermute(b, names, second)
    a = lax.ppermute(a, names, first)
    return a, b


def sum_step(row, axis, bit):
    count = lax.axis_size(axis)
    other = lax.ppermute(row, axis, [(i, i ^ bit) for i in range(count)])
    return row + other


MOST_UNROLL = 2
HALO_UNROLL = 4
ZS = ((3 * Y, Z), F32)
ZR = ((3 * Y + 8, Z), F32)
YS = ((X + 6, 16, Z), F32)
YR = ((X + 7, 16, Z), F32)
MOST = ((VIEWS, X + REACH, Y, Z), F32)
OWNB = ((X + REACH + 6, YE, Z), F32)
SIDES2 = ((12, YE, Z), F32)
XS = ((REACH + 4, YE, Z), F32)
OWN = ((X + 6, YE, Z), F32)
SIDES = ((6, YE, Z), F32)
CUBE = ((X, Y, Z), F32)
FOUR = ((VIEWS, X, Y, Z), F32)
ROW = ((8, Z), F32)
GF = 1 << 30
HALO = ((VIEWS, REACH, Y, Z), F32)


def local(estimate, view_images, psf_taps, view_weights):
    XE8 = (X + 2 * REACH) * 8
    z_a, z_b, estimate = call(first_kernel, [ZS, ZS, CUBE], [estimate], limit=2)
    *weights, share = call(
        reach_kernel,
        [
            ((VIEWS, 56, Z), F32), ((VIEWS, YE, Z), F32), ((VIEWS, 8, Z), F32), ((VIEWS, 16, Z), F32),
            ((VIEWS, 4, YE, Z), F32), ((VIEWS, 4, YE, Z), F32), ROW,
        ],
        [psf_taps, view_weights], specs=[SM, SM], limit=2,
    )
    (row,) = call(sums_kernel, [ROW], [estimate, view_images, *weights[:3]], limit=2, flops=GF // 4)
    fz, fy, fx, bz, by, bx = call(
        setup_kernel,
        [
            ((256, VIEWS * Z), BF16), ((VIEWS, 4 * Y, 4 * YE), BF16), ((VIEWS, X * 8, XE8), BF16),
            ((VIEWS * Z, 256), BF16), ((VIEWS, 4 * YE, 4 * Y), BF16), ((VIEWS, XE8, X * 8), BF16),
        ],
        [psf_taps], specs=[SM], limit=4, flops=4 * GF,
    )
    for iteration in range(ITERS):
        final = iteration + 1 == ITERS
        z_a, z_b = swap(z_a, z_b, "gz")
        for axis, bit in EARLY_STEPS if iteration == 0 else NEXT_STEPS:
            row = sum_step(row, axis, bit)
        rides = [] if iteration == 0 else [row]
        y_a, y_b = call(pack_y_kernel, [YR if rides else YS, YS], [estimate, z_a, z_b, *rides], limit=2)
        y_a, y_b = swap(y_a, y_b, "gy")
        own_f, xa_f, xb_f, row = call(pack_x_kernel, [OWN, XS, XS, ROW], [estimate, z_a, z_b, y_a, y_b, row], limit=2)
        xa_f, xb_f = swap(xa_f, xb_f, "gx")
        row = row + xa_f[REACH + 3, 48:56]
        for axis, bit in FIRST_STEPS if iteration == 0 else FINAL_STEPS:
            row = sum_step(row, axis, bit)
        (mid,) = call(
            forward_most_kernel, [MOST], [own_f, xa_f, fz, fy],
            scratch=[((X + REACH, YE, Z), F32), SIDES2], limit=6, flops=5 * GF,
        )
        (halo_b,) = call(forward_halo_kernel, [HALO], [xb_f, fz, fy], scratch=[SIDES], limit=4, flops=2 * GF)
        (blurred,) = call(forward_last_kernel, [FOUR], [mid, halo_b, fx], limit=4, flops=2 * GF)
        mid, halo_b = call(
            backward_kernel, [MOST, HALO], [blurred, view_images, bx], limit=4, flops=2 * GF
        )
        if iteration == 0:
            data = sent = first = row
            (missed,) = call(misfit_kernel, [ROW], [data, blurred, view_images], limit=2, flops=GF // 4)
        else:
            (missed,) = call(centred_kernel, [ROW], [first, blurred, view_images], limit=2, flops=GF // 4)
            sent = last = sum_step(missed, "gz", 3)
            data = jnp.where(lax.broadcasted_iota(jnp.int32, (8, Z), 1) < 8, first, row)
        (xb_b,) = call(
            backward_halo_kernel, [XS], [halo_b, data, share, bz, by],
            scratch=[SIDES], limit=4, flops=2 * GF,
        )
        own_b, xa_b = call(
            backward_most_kernel, [OWNB, XS], [mid, data, share, sent, bz, by],
            scratch=[SIDES2], limit=4, flops=5 * GF,
        )
        x_a, x_b = swap(xa_b, xb_b, "gx")
        if final:
            last = last + x_a[REACH + 3, 48:56]
            for axis, bit in LAST_STEPS:
                last = sum_step(last, axis, bit)
        else:
            (row,) = call(
                totals_kernel, [ROW], [missed, own_f, xa_f, xb_f, own_b, xa_b, xb_b, *weights], limit=2, flops=GF
            )
            for axis, bit in BETWEEN_STEPS:
                row = sum_step(row, axis, bit)
        kept, y_a, y_b = call(add_x_kernel, [((X + 6, Y, Z), F32), YS, YS], [own_b, x_a, x_b], scratch=[OWN], limit=4)
        y_a, y_b = swap(y_a, y_b, "gy")
        main, z_a, z_b = call(
            add_y_kernel, [CUBE, ZR, ZS], [kept, y_a, y_b, last if final else row], scratch=[((X + 6, Y, Z), F32)], limit=2
        )
        z_a, z_b = swap(z_a, z_b, "gz")
        if not final:
            estimate, z_a, z_b, row = call(update_kernel, [CUBE, ZS, ZS, ROW], [main, z_a, z_b, estimate, row], limit=2)
        else:
            last = last + z_a[3 * Y :]
            for axis, bit in TAIL_STEPS:
                last = sum_step(last, axis, bit)
            (estimate,) = call(finish_kernel, [CUBE], [main, z_a, z_b, estimate], limit=2)
            (misfits,) = call(report_kernel, [((ITERS, VIEWS), F32)], [first, data, last], limit=2)
    return (estimate, misfits)


EARLY_STEPS = (("gz", 1), ("gx_1", 1))
FIRST_STEPS = (("gz", 3), ("gy", 1), ("gy", 3), ("gx_0", 1), ("gx_1", 3))
BETWEEN_STEPS = (("gy", 3), ("gx_1", 1), ("gx_1", 3))
NEXT_STEPS = (("gx_0", 1),)
FINAL_STEPS = (("gz", 3),)
LAST_STEPS = (("gy", 1), ("gx_1", 1), ("gx_1", 3))
TAIL_STEPS = (("gy", 3), ("gx_0", 1))


def solution(mesh):
    torus = Mesh(
        mesh.devices.reshape(2, 4, 2, mesh.shape["gy"], mesh.shape["gz"]),
        ("gx_0", "gx_1", "gx_2", "gy", "gz"),
    )
    in_specs = (P(GX, "gy", "gz"), P(None, GX, "gy", "gz"), P(), P())
    out_specs = (P(GX, "gy", "gz"), P())
    return jax.shard_map(local, mesh=torus, in_specs=in_specs, out_specs=out_specs, check_vma=False)
```

```python
import jax
import jax.numpy as jnp
from jax import lax
from jax.experimental import pallas as pl
from jax.experimental.pallas import tpu as pltpu
from jax.sharding import Mesh
from jax.sharding import PartitionSpec as P


TAPS = 31
REACH = 15
ITERS = 2
VIEWS = 4
X, Y, Z = 24, 32, 128
YE = 64
F32 = jnp.float32
BF16 = jnp.bfloat16
GX = ("gx_0", "gx_1", "gx_2")
AXES = {"gx": GX, "gy": "gy", "gz": "gz"}


def parity(name):
    if name == "gx":
        return lax.axis_index("gx_2")
    return lax.rem(lax.axis_index(name), 2)


def position(name):
    if name == "gx":
        return (lax.axis_index("gx_0") * 4 + lax.axis_index("gx_1")) * 2 + lax.axis_index("gx_2")
    return lax.axis_index(name)


def lanes(shape):
    return lax.broadcasted_iota(jnp.int32, shape, len(shape) - 1)


def split(value):
    high = value.astype(BF16)
    low = (value - high.astype(F32)).astype(BF16)
    return high, low


def left_exact(matrix, data):
    high, low = split(data)
    return jnp.dot(matrix, high, preferred_element_type=F32) + jnp.dot(matrix, low, preferred_element_type=F32)


def right_exact(data, matrix):
    rows = data.shape[0]
    both = jnp.dot(jnp.concatenate(split(data), axis=0), matrix, preferred_element_type=F32)
    return both[:rows] + both[rows:]


def extended_offset(index, size, width, odd):
    low_first = index < size + width
    local = jnp.where(low_first, index - size, index - size - width)
    upper = low_first == (odd == 0)
    outside = jnp.where(upper, size + local, local - width)
    return jnp.where(index < size, index, outside)


def taps_matrix(taps_ref, view, axis, source, target):
    tap = source - target + REACH
    out = jnp.zeros(tap.shape, F32)
    for t in range(TAPS):
        out = jnp.where(tap == t, taps_ref[view, axis, t].astype(F32) / 256.0, out)
    return out


def select_matrix(rows, columns, match):
    r = lax.broadcasted_iota(jnp.int32, (rows, columns), 0)
    c = lax.broadcasted_iota(jnp.int32, (rows, columns), 1)
    return match(r, c)


def one_hot(rows, columns, match):
    return jnp.where(select_matrix(rows, columns, match), 1.0, 0.0).astype(BF16)


def setup_kernel(taps_ref, fz, fy, fx):
    odd_x, odd_y, odd_z = parity("gx"), parity("gy"), parity("gz")
    XE = X + 2 * REACH

    def one_view(v, carry):
        lane0 = pl.multiple_of(v * Z, Z)
        raw = lax.broadcasted_iota(jnp.int32, (Z + 32, Z), 0)
        tgt = lax.broadcasted_iota(jnp.int32, (Z + 32, Z), 1)
        band = taps_matrix(taps_ref, v, 2, extended_offset(raw, Z, 16, odd_z), tgt)
        band = jnp.concatenate([band, jnp.zeros((Z - 32, Z), F32)], axis=0)
        fz[:, pl.ds(lane0, Z)] = band.astype(BF16)
        tgt = lax.broadcasted_iota(jnp.int32, (Y, YE), 0)
        src = extended_offset(lax.broadcasted_iota(jnp.int32, (Y, YE), 1), Y, 16, odd_y)
        base = taps_matrix(taps_ref, v, 1, src, tgt).astype(BF16)
        spread = jnp.dot(one_hot(4 * Y, Y, lambda r, c: lax.rem(r, Y) == c), base, preferred_element_type=F32).astype(BF16)
        spread = jnp.dot(spread, one_hot(YE, 4 * YE, lambda r, c: lax.rem(c, YE) == r), preferred_element_type=F32)
        spread = jnp.where(select_matrix(4 * Y, 4 * YE, lambda r, c: r // Y == c // YE), spread, 0.0)
        fy[v] = spread.astype(BF16)
        tgt = lax.broadcasted_iota(jnp.int32, (X, XE), 0)
        src = extended_offset(lax.broadcasted_iota(jnp.int32, (X, XE), 1), X, REACH, odd_x)
        base = taps_matrix(taps_ref, v, 0, src, tgt).astype(BF16)
        spread = jnp.dot(one_hot(X * 8, X, lambda r, c: r // 8 == c), base, preferred_element_type=F32).astype(BF16)
        spread = jnp.dot(spread, one_hot(XE, XE * 8, lambda r, c: c // 8 == r), preferred_element_type=F32)
        spread = jnp.where(select_matrix(X * 8, XE * 8, lambda r, c: lax.rem(r, 8) == lax.rem(c, 8)), spread, 0.0)
        fx[v] = spread.astype(BF16)
        return carry

    lax.fori_loop(0, VIEWS, one_view, 0, unroll=2)


def transpose_kernel(fz, fy, fx, bz, by, bx):
    XE = X + 2 * REACH

    def one_view(v, carry):
        lane0 = pl.multiple_of(v * Z, Z)
        bz[pl.ds(lane0, Z), :] = fz[:, pl.ds(lane0, Z)].astype(F32).T.astype(BF16)
        by[v] = fy[v].astype(F32).T.astype(BF16)
        wide = jnp.concatenate([fx[v].astype(F32), jnp.zeros((X * 8, 512 - XE * 8), F32)], axis=1).T
        bx[v] = wide[: XE * 8].astype(BF16)
        return carry

    lax.fori_loop(0, VIEWS, one_view, 0)


def reach_kernel(taps_ref, weights, along_x, along_y, along_z, sides, sent_a, sent_b, share):
    odd_x, odd_y, odd_z = parity("gx"), parity("gy"), parity("gz")
    lane = lanes((8, Z))
    row = lax.broadcasted_iota(jnp.int32, (8, Z), 0)
    base_x = 3 * (lane // 16)
    near_at = extended_offset(jnp.where(row < 3, base_x + row, X + base_x + row - 3), X, REACH, odd_x)
    far_at = jnp.where(row < 3, X + REACH + base_x + row, lane)
    far_at = extended_offset(far_at, X, REACH, odd_x)
    y_at = extended_offset(lane, Y, 16, odd_y)
    z_at = jnp.where(row == 0, lane, Z + lax.rem(lane, 16) + jnp.where(row == 2, 16, 0))
    z_at = extended_offset(z_at, Z, 16, odd_z)

    def down(values):
        return jnp.broadcast_to(values, (Z, Z)).T

    def one_view(v, carry):
        shares, norm = carry

        def reach(axis, name, size, count, *indices):
            outs = [jnp.zeros((8, Z), F32) for _ in indices]
            ats = [position(name) * size + index + REACH for index in indices]
            taps = jnp.zeros((), jnp.int32)
            for t in range(TAPS):
                tap = taps_ref[v, axis, t]
                taps = taps + tap
                value = tap.astype(F32) / 256.0
                outs = [
                    out + jnp.where((at >= t) & (at < count * size + t), value, 0.0) for out, at in zip(outs, ats)
                ]
            return outs, taps.astype(F32) / 256.0

        (near, far), whole_x = reach(0, "gx", X, 16, near_at, far_at)
        (rows_y,), whole_y = reach(1, "gy", Y, 4, y_at)
        (rows_z,), whole_z = reach(2, "gz", Z, 4, z_at)
        weight = weights[v].astype(F32)
        along_x[v] = down(far[3:4])[0:56]
        spread_y = down(rows_y[0:1])[0:YE]
        along_y[v] = spread_y
        along_z[v] = rows_z
        z_side = (rows_z[1:2], rows_z[2:3])
        for k in range(2):
            sides[v, 8 * k : 8 * k + 8] = near * z_side[k]
        for source, first, dst in ((near, 3, sent_a), (far, 0, sent_b)):
            def tile(k, source=source, first=first):
                return lambda i: spread_y * (source[first + i : first + i + 1] * z_side[k])

            def store(i, value, dst=dst):
                dst[v, i] = value

            def store_rest(i, value, dst=dst):
                dst[v, 3, 16 * i : 16 * i + 16] = value

            pack_sides(tile(0), tile(1), store, store_rest)
            dst[v, 3, 48:64] = jnp.zeros((16, Z), F32)
        whole = jnp.full((8, Z), whole_x * whole_y * whole_z, F32)
        return jnp.where(lane == v, weight, shares), norm + weight * whole

    shares, norm = lax.fori_loop(0, VIEWS, one_view, (jnp.zeros((8, Z), F32), jnp.zeros((8, Z), F32)))
    share[...] = shares / norm


def pack_sides(side_a, side_b, store, store_rest):
    lane = lanes((YE, Z))
    quarter = lanes((16, Z)) // 32
    for i in range(3):
        a, b = side_a(i), side_b(i)
        store(i, jnp.where(lane < 80, a, pltpu.roll(b, 80, 1)))
        rest = pltpu.roll(b, Z - 48, 1)
        packed = rest[0:16]
        for q in range(1, 4):
            packed = jnp.where(quarter == q, pltpu.roll(rest[16 * q : 16 * q + 16], 32 * q, 1), packed)
        store_rest(i, packed)


def unpack_sides(tile, packed):
    lane = lanes((YE, Z))
    parts = [packed] + [pltpu.roll(packed, Z - 32 * q, 1) for q in range(1, 4)]
    rest = jnp.concatenate(parts, axis=0)
    a = jnp.where(lane < 80, tile, 0.0)
    b = jnp.where(lane < 48, pltpu.roll(tile, Z - 80, 1), pltpu.roll(rest, 48, 1))
    return a, jnp.where(lane < 80, b, 0.0)


def pack_z(load, z_a, z_b):
    group = lanes((3 * Y, Z)) // 16
    up = jnp.zeros((3 * Y, Z), F32)
    down = jnp.zeros((3 * Y, Z), F32)
    for g in range(8):
        part = load(g)
        up = jnp.where(group == g, pltpu.roll(part, (16 * g + 16) % Z, 1) if g != 7 else part, up)
        down = jnp.where(group == g, pltpu.roll(part, 16 * g, 1) if g else part, down)
    odd = parity("gz")
    z_a[...] = jnp.where(odd == 0, up, down)
    z_b[...] = jnp.where(odd == 0, down, up)


def blurred_totals(load, along_x, along_y, along_z):
    lane = lanes((8, Z))
    row = lax.broadcasted_iota(jnp.int32, (8, Z), 0)
    out = jnp.zeros((8, Z), F32)
    for v in range(VIEWS):
        acc = jnp.zeros((Y, Z), F32)
        for i in range(X):
            acc = acc + load(i) * along_x[v, i : i + 1, :]
        total = jnp.sum(acc * along_y[v, 0:Y] * along_z[v, 0:1])
        out = jnp.where((lane == 8 + v) & (row == 0), total, out)
    return out


def first_kernel(est, z_a, z_b, kept):
    kept[...] = est[...]
    pack_z(lambda g: est[3 * g : 3 * g + 3].reshape(3 * Y, Z), z_a, z_b)


def sums_kernel(est, views, along_x, along_y, along_z, row_ref):
    lane = lanes((8, Z))
    row = lax.broadcasted_iota(jnp.int32, (8, Z), 0)
    out = blurred_totals(lambda i: est[i], along_x, along_y, along_z)
    for v in range(VIEWS):
        total = jnp.zeros((Y, Z), F32)
        square = jnp.zeros((Y, Z), F32)
        for i in range(X):
            image = views[v, i]
            total = total + image
            square = square + image * image
        out = jnp.where((lane == v) & (row == 0), jnp.sum(total), out)
        out = jnp.where((lane == 4 + v) & (row == 0), jnp.sum(square), out)
    row_ref[...] = out


def pack_y_kernel(est, z_a, z_b, *refs):
    row, y_a, y_b = refs if len(refs) == 3 else (None, *refs)
    odd = parity("gy")
    start_a = pl.multiple_of((1 - odd) * 16, 16)
    start_b = pl.multiple_of(odd * 16, 16)
    for start, out in ((start_a, y_a), (start_b, y_b)):
        out[0:X] = est[:, pl.ds(start, 16), :]
        for i in range(3):
            out[X + i] = z_a[pl.ds(start + i * Y, 16)]
            out[X + 3 + i] = z_b[pl.ds(start + i * Y, 16)]
    if row is not None:
        y_a[X + 6, 0:8] = row[...]
        y_a[X + 6, 8:16] = row[...]


def pack_x_kernel(est, z_a, z_b, y_a, y_b, row, own, x_a, x_b, row_out):
    def copy(i, carry):
        own[i, 0:Y] = est[i]
        return carry

    def beside(i, carry):
        own[i, Y : Y + 16] = y_a[i]
        own[i, Y + 16 : YE] = y_b[i]
        return carry

    lax.fori_loop(0, X, copy, 0, unroll=12)
    lax.fori_loop(0, X + 6, beside, 0, unroll=10)
    for i in range(3):
        own[X + i, 0:Y] = z_a[i * Y : i * Y + Y]
        own[X + 3 + i, 0:Y] = z_b[i * Y : i * Y + Y]
    total = row[...] + y_a[X + 6, 0:8] if y_a.shape[0] > X + 6 else row[...]
    row_out[...] = total
    odd = parity("gx")
    for flag, out in ((odd, x_a), (1 - odd, x_b)):
        out[0:REACH] = own[pl.ds((1 - flag) * 9, REACH)]

        def side(first):
            def get(i, flag=flag):
                full = own[first + i]
                return jnp.where(flag == 0, pltpu.roll(full, Z - 48, 1), full)

            return get

        def store(i, value, out=out):
            out[REACH + i] = value

        def store_rest(i, value, out=out):
            out[REACH + 3, 16 * i : 16 * i + 16] = value

        pack_sides(side(X), side(X + 3), store, store_rest)
        out[REACH + 3, 48:56] = total
        out[REACH + 3, 56:64] = total


def forward_group(src, sides_ref, plane, fz, fy, store):
    mains, sides = [], []
    lane = lanes((YE, Z))
    for k in range(4):
        p = plane + k
        g, spot = side_spot(p)
        mains.append(src[p])
        a = pltpu.roll(sides_ref[spot], lax.rem(Z - 16 * g, Z), 1)
        b = pltpu.roll(sides_ref[spot + 3], lax.rem(Z + 16 - 16 * g, Z), 1)
        sides.append(jnp.where(lane < 16, a, b))
    data = jnp.concatenate([jnp.concatenate(mains, 0), jnp.concatenate(sides, 0)], axis=1)
    wide = right_exact(data, fz[...])
    for v in range(VIEWS):
        out = left_exact(fy[v], wide[:, v * Z : (v + 1) * Z])
        store(v, out.reshape(4, Y, Z))


def side_spot(p):
    beyond = (p >= X).astype(jnp.int32)
    local_plane = p - X * beyond
    g = local_plane // 3
    return g, local_plane - 3 * g + 6 * beyond


def forward_most_kernel(own, x_a, fz, fy, out, src, sides):
    src[0:X] = own[0:X]
    src[X:] = x_a[0:REACH]
    sides[0:6] = own[X:]
    for i in range(3):
        sides[6 + i], sides[9 + i] = unpack_sides(x_a[REACH + i], x_a[REACH + 3, 16 * i : 16 * i + 16])

    def step(j, carry):
        plane = jnp.minimum(j * 4, X + REACH - 4)

        def store(v, value):
            out[v, pl.ds(plane, 4)] = value

        forward_group(src, sides, plane, fz, fy, store)
        return carry

    lax.fori_loop(0, 10, step, 0, unroll=MOST_UNROLL)


def forward_halo_kernel(src, fz, fy, out, sides):
    for i in range(3):
        sides[i], sides[3 + i] = unpack_sides(src[REACH + i], src[REACH + 3, 16 * i : 16 * i + 16])

    def step(j, carry):
        plane = jnp.minimum(j * 4, REACH - 4)

        def store(v, value):
            out[v, pl.ds(plane, 4)] = value

        forward_group(src, sides, plane, fz, fy, store)
        return carry

    lax.fori_loop(0, 4, step, 0, unroll=2)


def forward_last_kernel(mid, halo_b, fx, out):
    def one_view(v, carry):
        for pair in range(2):
            columns = []
            for tile in (2 * pair, 2 * pair + 1):
                rows = pl.ds(tile * 8, 8)
                columns.append(
                    jnp.concatenate(
                        [
                            mid[v, :, rows].reshape((X + REACH) * 8, Z),
                            halo_b[v, :, rows].reshape(REACH * 8, Z),
                        ],
                        axis=0,
                    )
                )
            got = left_exact(fx[v], jnp.concatenate(columns, axis=1))
            for k, tile in enumerate((2 * pair, 2 * pair + 1)):
                out[v, :, tile * 8 : tile * 8 + 8] = got[:, k * Z : (k + 1) * Z].reshape(X, 8, Z)
        return carry

    lax.fori_loop(0, VIEWS, one_view, 0, unroll=2)


def pick(row, lane, index):
    return jnp.sum(jnp.where(lane == index, row, 0.0), axis=1, keepdims=True)


def view_scales(sums, share):
    lane = lanes((1, Z))
    row = sums[0:1, :]
    return [pick(share[0:1, :], lane, v) * (pick(row, lane, 8 + v) / pick(row, lane, v)) for v in range(VIEWS)]


def backward_group(load, plane, scales, bz, by, store):
    parts = [left_exact(by[v], load(v, plane).reshape(4 * Y, Z) * scales[v]) for v in range(VIEWS)]
    wide = right_exact(jnp.concatenate(parts, axis=1), bz[...])
    store(wide)


def store_extended(dst, sides_ref, plane, wide):
    group = lanes((YE, Z)) // 16
    for k in range(4):
        p = plane + k
        g, spot = side_spot(p)
        rows = wide[k * YE : (k + 1) * YE]
        dst[p] = rows[:, :Z]
        side = rows[:, Z:]
        a = pltpu.roll(side, lax.rem(16 * g + Z, Z), 1)
        b = pltpu.roll(side, lax.rem(16 * g + Z - 16, Z), 1)
        sides_ref[spot] = jnp.where(group == g, a, sides_ref[spot])
        sides_ref[spot + 3] = jnp.where(group == g, b, sides_ref[spot + 3])


def backward_kernel(blurred, views, bx, mid, halo_b):
    def one_view(v, carry):
        for pair in range(2):
            tiles = (2 * pair, 2 * pair + 1)
            b = jnp.concatenate([blurred[v, :, t * 8 : t * 8 + 8].reshape(X * 8, Z) for t in tiles], axis=1)
            image = jnp.concatenate([views[v, :, t * 8 : t * 8 + 8].reshape(X * 8, Z) for t in tiles], axis=1)
            got = left_exact(bx[v], image / b)
            for k, t in enumerate(tiles):
                piece = got[:, k * Z : (k + 1) * Z]
                rows = slice(t * 8, t * 8 + 8)
                mid[v, :, rows] = piece[: (X + REACH) * 8].reshape(X + REACH, 8, Z)
                halo_b[v, :, rows] = piece[(X + REACH) * 8 :].reshape(REACH, 8, Z)
        return carry

    lax.fori_loop(0, VIEWS, one_view, 0, unroll=2)


def misfit_kernel(sums, blurred, views, misfit):
    lane = lanes((1, Z))
    row = sums[0:1, :]
    out_lane = lanes((8, Z))
    out_row = lax.broadcasted_iota(jnp.int32, (8, Z), 0)
    misfits = jnp.zeros((8, Z), F32)
    for v in range(VIEWS):
        flux = pick(row, lane, v) / pick(row, lane, 8 + v)

        def plane(i, total, v=v, flux=flux):
            gap = views[v, i] - flux * blurred[v, i]
            return total + gap * gap

        missed = lax.fori_loop(0, X, plane, jnp.zeros((Y, Z), F32), unroll=4)
        misfits = jnp.where((out_lane == 24 + v) & (out_row == 0), jnp.sum(missed), misfits)
    misfit[...] = misfits


def centred_kernel(sums, earlier, blurred, views, out):
    lane = lanes((1, Z))
    row = sums[0:1, :]
    out_lane = lanes((8, Z))
    out_row = lax.broadcasted_iota(jnp.int32, (8, Z), 0)
    total = earlier[...]
    for v in range(VIEWS):
        centre = pick(row, lane, v) / pick(row, lane, 8 + v)

        def plane(i, carry, v=v, centre=centre):
            value = blurred[v, i]
            gap = views[v, i] - centre * value
            return carry[0] + gap * gap, carry[1] + gap * value, carry[2] + value * value

        zero = jnp.zeros((Y, Z), F32)
        for k, part in enumerate(lax.fori_loop(0, X, plane, (zero, zero, zero), unroll=4)):
            total = jnp.where((out_lane == 12 + 4 * k + v) & (out_row == 0), jnp.sum(part), total)
    out[...] = total


def report_kernel(first, sums, last, out):
    def at(row, start):
        return pltpu.roll(row, Z - start, 1) if start else row

    before, now, end = first[...], sums[...], last[...]
    square = at(now, 4)
    shift = now / at(now, 8) - before / at(before, 8)
    missed = at(end, 12) - 2.0 * shift * at(end, 16) + shift * shift * at(end, 20)
    out[0:1] = (at(end, 24) / square)[0:1, 0:VIEWS]
    out[1:2] = (missed / square)[0:1, 0:VIEWS]


def backward_halo_kernel(halo, sums, share, bz, by, dst, sides):
    sides[...] = jnp.zeros((6, YE, Z), F32)
    scales = view_scales(sums, share)

    def step(j, carry):
        plane = jnp.minimum(j * 4, REACH - 4)
        backward_group(
            lambda v, p: halo[v, pl.ds(p, 4)], plane, scales, bz, by,
            lambda wide: store_extended(dst, sides, plane, wide),
        )
        return carry

    lax.fori_loop(0, 4, step, 0, unroll=HALO_UNROLL)
    send_sides(dst, sides, 0)


def send_sides(dst, sides, first):
    def store(i, value):
        dst[REACH + i] = value

    def store_rest(i, value):
        dst[REACH + 3, 16 * i : 16 * i + 16] = value

    pack_sides(lambda i: sides[first + i], lambda i: sides[first + 3 + i], store, store_rest)
    dst[REACH + 3, 48:64] = jnp.zeros((16, Z), F32)


def backward_most_kernel(mid, sums, share, bz, by, own, x_a, sides):
    sides[...] = jnp.zeros((12, YE, Z), F32)
    scales = view_scales(sums, share)

    def step(j, carry):
        plane = jnp.minimum(j * 4, X + REACH - 4)
        backward_group(
            lambda v, p: mid[v, pl.ds(p, 4)], plane, scales, bz, by,
            lambda wide: store_extended(own, sides, plane, wide),
        )
        return carry

    lax.fori_loop(0, 10, step, 0, unroll=MOST_UNROLL)
    own[X + REACH :] = sides[0:6]
    x_a[0:REACH] = own[X : X + REACH]
    send_sides(x_a, sides, 6)


def totals_kernel(own_f, xa_f, xb_f, own_b, xa_b, xb_b, along_x, along_y, along_z, sides, sent_a, sent_b, out):
    def planes(left, right, count, first, accs):
        def one(p, accs):
            product = left[p] * right[p]
            return tuple(acc + product * along_x[v, pl.ds(first + p, 1), :] for v, acc in enumerate(accs))

        return lax.fori_loop(0, count, one, accs, unroll=3)

    accs = tuple(jnp.zeros((YE, Z), F32) for _ in range(VIEWS))
    accs = planes(own_f, own_b, X, 0, accs)
    accs = planes(xa_f, xa_b, REACH, X, accs)
    accs = planes(xb_f, xb_b, REACH, X + REACH, accs)
    lane = lanes((8, Z))
    row = lax.broadcasted_iota(jnp.int32, (8, Z), 0)
    result = jnp.zeros((8, Z), F32)
    for v in range(VIEWS):
        acc = accs[v] * along_z[v, 0:1]
        for k in range(2):
            for i in range(3):
                product = own_f[X + 3 * k + i] * own_b[X + REACH + 3 * k + i]
                acc = acc + product * sides[v, 8 * k + i : 8 * k + i + 1]
        acc = acc * along_y[v]
        for left, right, weight in ((xa_f, xa_b, sent_a), (xb_f, xb_b, sent_b)):
            for i in range(4):
                acc = acc + left[REACH + i] * right[REACH + i] * weight[v, i]
        result = jnp.where((lane == 8 + v) & (row == 0), jnp.sum(acc), result)
    out[...] = result


def add_x_kernel(own, x_a, x_b, kept, y_a, y_b, total):
    odd = parity("gx")
    start_a = (1 - odd) * 9
    start_b = odd * 9

    def copy(i, carry):
        total[i] = own[i]
        return carry

    def add(m, carry):
        total[start_a + m] = total[start_a + m] + x_a[m]
        return carry

    def add_far(m, carry):
        total[start_b + m] = total[start_b + m] + x_b[m]
        return carry

    def share_out(i, carry):
        kept[i] = total[i, 0:Y]
        y_a[i] = total[i, Y : Y + 16]
        y_b[i] = total[i, Y + 16 : YE]
        return carry

    lax.fori_loop(0, X, copy, 0, unroll=8)
    lax.fori_loop(0, REACH, add, 0, unroll=5)
    lax.fori_loop(0, REACH, add_far, 0, unroll=5)
    total[X:] = own[X + REACH :]
    for flag, src in ((odd, x_a), (1 - odd, x_b)):
        for i in range(3):
            sides = unpack_sides(src[REACH + i], src[REACH + 3, 16 * i : 16 * i + 16])
            for k, side in enumerate(sides):
                at = X + 3 * k + i
                total[at] = total[at] + jnp.where(flag == 0, pltpu.roll(side, 48, 1), side)
    lax.fori_loop(0, X + 6, share_out, 0, unroll=10)


def add_y_kernel(kept, y_a, y_b, row, main, z_a, z_b, total):
    total[...] = kept[...]
    odd = parity("gy")
    for start, src in (((1 - odd) * 16, y_a), (odd * 16, y_b)):
        spot = pl.ds(pl.multiple_of(start, 16), 16)
        total[:, spot] = total[:, spot] + src[...]
    main[...] = total[0:X]
    for i in range(3):
        z_a[Y * i : Y * i + Y] = total[X + i]
        z_b[Y * i : Y * i + Y] = total[X + 3 + i]
    z_a[3 * Y :] = row[...]


def corrected(main, z_a, z_b, est, g):
    odd = parity("gz")
    lane = lanes((3 * Y, Z))
    a = z_a[0 : 3 * Y]
    b = z_b[...]
    up = jnp.where(odd == 0, a, b)
    down = jnp.where(odd == 0, b, a)
    up = pltpu.roll(up, (112 - 16 * g) % Z, 1) if g != 7 else up
    down = pltpu.roll(down, (Z - 16 * g) % Z, 1) if g else down
    total = main[3 * g : 3 * g + 3].reshape(3 * Y, Z)
    total = total + jnp.where(lane >= 112, up, 0.0) + jnp.where(lane < 16, down, 0.0)
    return est[3 * g : 3 * g + 3].reshape(3 * Y, Z) * total


def update_kernel(main, z_a, z_b, est, row, out, out_a, out_b, row_out):
    for g in range(8):
        out[3 * g : 3 * g + 3] = corrected(main, z_a, z_b, est, g).reshape(3, Y, Z)
    pack_z(lambda g: out[3 * g : 3 * g + 3].reshape(3 * Y, Z), out_a, out_b)
    row_out[...] = row[...] + z_a[3 * Y :]


def finish_kernel(main, z_a, z_b, est, out):
    for g in range(8):
        out[3 * g : 3 * g + 3] = corrected(main, z_a, z_b, est, g).reshape(3, Y, Z)


VM = pl.BlockSpec(memory_space=pltpu.VMEM)
SM = pl.BlockSpec(memory_space=pltpu.SMEM)


def call(kernel, outs, operands, specs=None, scratch=(), limit=16, flops=0):
    shapes = [jax.ShapeDtypeStruct(shape, dtype) for shape, dtype in outs]
    return pl.pallas_call(
        kernel,
        out_shape=shapes,
        in_specs=specs or [VM] * len(operands),
        out_specs=[VM] * len(shapes),
        scratch_shapes=[pltpu.VMEM(shape, dtype) for shape, dtype in scratch],
        compiler_params=pltpu.CompilerParams(vmem_limit_bytes=limit << 20),
        cost_estimate=pl.CostEstimate(flops=max(flops, 1000), bytes_accessed=1000, transcendentals=0),
    )(*operands)


def swap(a, b, axis):
    names = AXES[axis]
    count = lax.axis_size(names)
    first = [(i, i ^ 1) for i in range(count)]
    second = [(i, i + 1) for i in range(1, count - 1, 2)] + [(i + 1, i) for i in range(1, count - 1, 2)]
    b = lax.ppermute(b, names, second)
    a = lax.ppermute(a, names, first)
    return a, b


def sum_step(row, axis, bit):
    count = lax.axis_size(axis)
    other = lax.ppermute(row, axis, [(i, i ^ bit) for i in range(count)])
    return row + other


MOST_UNROLL = 2
HALO_UNROLL = 4
ZS = ((3 * Y, Z), F32)
ZR = ((3 * Y + 8, Z), F32)
YS = ((X + 6, 16, Z), F32)
YR = ((X + 7, 16, Z), F32)
MOST = ((VIEWS, X + REACH, Y, Z), F32)
OWNB = ((X + REACH + 6, YE, Z), F32)
SIDES2 = ((12, YE, Z), F32)
XS = ((REACH + 4, YE, Z), F32)
OWN = ((X + 6, YE, Z), F32)
SIDES = ((6, YE, Z), F32)
CUBE = ((X, Y, Z), F32)
FOUR = ((VIEWS, X, Y, Z), F32)
ROW = ((8, Z), F32)
GF = 1 << 30
HALO = ((VIEWS, REACH, Y, Z), F32)


def local(estimate, view_images, psf_taps, view_weights):
    XE8 = (X + 2 * REACH) * 8
    z_a, z_b, estimate = call(first_kernel, [ZS, ZS, CUBE], [estimate], limit=2)
    *weights, share = call(
        reach_kernel,
        [
            ((VIEWS, 56, Z), F32), ((VIEWS, YE, Z), F32), ((VIEWS, 8, Z), F32), ((VIEWS, 16, Z), F32),
            ((VIEWS, 4, YE, Z), F32), ((VIEWS, 4, YE, Z), F32), ROW,
        ],
        [psf_taps, view_weights], specs=[SM, SM], limit=2,
    )
    (row,) = call(sums_kernel, [ROW], [estimate, view_images, *weights[:3]], limit=2, flops=GF // 4)
    shapes = [((256, VIEWS * Z), BF16), ((VIEWS, 4 * Y, 4 * YE), BF16), ((VIEWS, X * 8, XE8), BF16)]
    fz, fy, fx = call(setup_kernel, shapes, [psf_taps], specs=[SM], limit=4, flops=4 * GF)
    bz, by, bx = call(
        transpose_kernel,
        [((VIEWS * Z, 256), BF16), ((VIEWS, 4 * YE, 4 * Y), BF16), ((VIEWS, XE8, X * 8), BF16)],
        [fz, fy, fx], limit=4, flops=GF,
    )
    for iteration in range(ITERS):
        final = iteration + 1 == ITERS
        z_a, z_b = swap(z_a, z_b, "gz")
        for axis, bit in EARLY_STEPS if iteration == 0 else NEXT_STEPS:
            row = sum_step(row, axis, bit)
        rides = [] if iteration == 0 else [row]
        y_a, y_b = call(pack_y_kernel, [YR if rides else YS, YS], [estimate, z_a, z_b, *rides], limit=2)
        y_a, y_b = swap(y_a, y_b, "gy")
        own_f, xa_f, xb_f, row = call(pack_x_kernel, [OWN, XS, XS, ROW], [estimate, z_a, z_b, y_a, y_b, row], limit=2)
        xa_f, xb_f = swap(xa_f, xb_f, "gx")
        row = row + xa_f[REACH + 3, 48:56]
        for axis, bit in FIRST_STEPS if iteration == 0 else FINAL_STEPS:
            row = sum_step(row, axis, bit)
        (mid,) = call(
            forward_most_kernel, [MOST], [own_f, xa_f, fz, fy],
            scratch=[((X + REACH, YE, Z), F32), SIDES2], limit=6, flops=5 * GF,
        )
        (halo_b,) = call(forward_halo_kernel, [HALO], [xb_f, fz, fy], scratch=[SIDES], limit=4, flops=2 * GF)
        (blurred,) = call(forward_last_kernel, [FOUR], [mid, halo_b, fx], limit=4, flops=2 * GF)
        mid, halo_b = call(
            backward_kernel, [MOST, HALO], [blurred, view_images, bx], limit=4, flops=2 * GF
        )
        if iteration == 0:
            data = first = row
            (missed,) = call(misfit_kernel, [ROW], [data, blurred, view_images], limit=2, flops=GF // 4)
        else:
            (missed,) = call(centred_kernel, [ROW], [first, missed, blurred, view_images], limit=2, flops=GF // 4)
            last = sum_step(missed, "gz", 3)
            data = jnp.where(lax.broadcasted_iota(jnp.int32, (8, Z), 1) < 8, first, row)
        (xb_b,) = call(
            backward_halo_kernel, [XS], [halo_b, data, share, bz, by],
            scratch=[SIDES], limit=4, flops=2 * GF,
        )
        own_b, xa_b = call(
            backward_most_kernel, [OWNB, XS], [mid, data, share, bz, by],
            scratch=[SIDES2], limit=4, flops=5 * GF,
        )
        x_a, x_b = swap(xa_b, xb_b, "gx")
        if final:
            for axis, bit in LAST_STEPS:
                last = sum_step(last, axis, bit)
        else:
            (row,) = call(
                totals_kernel, [ROW], [own_f, xa_f, xb_f, own_b, xa_b, xb_b, *weights], limit=2, flops=GF
            )
            for axis, bit in BETWEEN_STEPS:
                row = sum_step(row, axis, bit)
        kept, y_a, y_b = call(add_x_kernel, [((X + 6, Y, Z), F32), YS, YS], [own_b, x_a, x_b], scratch=[OWN], limit=4)
        y_a, y_b = swap(y_a, y_b, "gy")
        main, z_a, z_b = call(
            add_y_kernel, [CUBE, ZR, ZS], [kept, y_a, y_b, last if final else row], scratch=[((X + 6, Y, Z), F32)], limit=2
        )
        z_a, z_b = swap(z_a, z_b, "gz")
        if not final:
            estimate, z_a, z_b, row = call(update_kernel, [CUBE, ZS, ZS, ROW], [main, z_a, z_b, estimate, row], limit=2)
        else:
            last = last + z_a[3 * Y :]
            for axis, bit in TAIL_STEPS:
                last = sum_step(last, axis, bit)
            (estimate,) = call(finish_kernel, [CUBE], [main, z_a, z_b, estimate], limit=2)
            (misfits,) = call(report_kernel, [((ITERS, VIEWS), F32)], [first, data, last], limit=2)
    return (estimate, misfits)


EARLY_STEPS = (("gz", 1), ("gx_1", 1))
FIRST_STEPS = (("gz", 3), ("gy", 1), ("gy", 3), ("gx_0", 1), ("gx_1", 3))
BETWEEN_STEPS = (("gx_1", 1),)
NEXT_STEPS = ()
FINAL_STEPS = (("gz", 3), ("gx_0", 1), ("gy", 3), ("gx_1", 3))
LAST_STEPS = (("gy", 3), ("gx_2", 1), ("gy", 1), ("gx_1", 1), ("gx_1", 3))
TAIL_STEPS = (("gx_0", 1),)


def solution(mesh):
    torus = Mesh(
        mesh.devices.reshape(2, 4, 2, mesh.shape["gy"], mesh.shape["gz"]),
        ("gx_0", "gx_1", "gx_2", "gy", "gz"),
    )
    in_specs = (P(GX, "gy", "gz"), P(None, GX, "gy", "gz"), P(), P())
    out_specs = (P(GX, "gy", "gz"), P())
    return jax.shard_map(local, mesh=torus, in_specs=in_specs, out_specs=out_specs, check_vma=False)
```

```python
import jax
import jax.numpy as jnp
from jax import lax
from jax.experimental import pallas as pl
from jax.experimental.pallas import tpu as pltpu
from jax.sharding import Mesh
from jax.sharding import PartitionSpec as P


TAPS = 31
REACH = 15
ITERS = 2
VIEWS = 4
X, Y, Z = 24, 32, 128
YE = 64
F32 = jnp.float32
BF16 = jnp.bfloat16
GX = ("gx_0", "gx_1", "gx_2")
AXES = {"gx": GX, "gy": "gy", "gz": "gz"}


def parity(name):
    if name == "gx":
        return lax.axis_index("gx_2")
    return lax.rem(lax.axis_index(name), 2)


def position(name):
    if name == "gx":
        return (lax.axis_index("gx_0") * 4 + lax.axis_index("gx_1")) * 2 + lax.axis_index("gx_2")
    return lax.axis_index(name)


def lanes(shape):
    return lax.broadcasted_iota(jnp.int32, shape, len(shape) - 1)


def split(value):
    high = value.astype(BF16)
    low = (value - high.astype(F32)).astype(BF16)
    return high, low


def left_exact(matrix, data):
    high, low = split(data)
    return jnp.dot(matrix, high, preferred_element_type=F32) + jnp.dot(matrix, low, preferred_element_type=F32)


def right_exact(data, matrix):
    rows = data.shape[0]
    both = jnp.dot(jnp.concatenate(split(data), axis=0), matrix, preferred_element_type=F32)
    return both[:rows] + both[rows:]


def extended_offset(index, size, width, odd):
    low_first = index < size + width
    local = jnp.where(low_first, index - size, index - size - width)
    upper = low_first == (odd == 0)
    outside = jnp.where(upper, size + local, local - width)
    return jnp.where(index < size, index, outside)


def taps_matrix(taps_ref, view, axis, source, target):
    tap = source - target + REACH
    out = jnp.zeros(tap.shape, F32)
    for t in range(TAPS):
        out = jnp.where(tap == t, taps_ref[view, axis, t].astype(F32) / 256.0, out)
    return out


def select_matrix(rows, columns, match):
    r = lax.broadcasted_iota(jnp.int32, (rows, columns), 0)
    c = lax.broadcasted_iota(jnp.int32, (rows, columns), 1)
    return match(r, c)


def one_hot(rows, columns, match):
    return jnp.where(select_matrix(rows, columns, match), 1.0, 0.0).astype(BF16)


def setup_kernel(taps_ref, fz, fy, fx):
    odd_x, odd_y, odd_z = parity("gx"), parity("gy"), parity("gz")
    XE = X + 2 * REACH

    def one_view(v, carry):
        lane0 = pl.multiple_of(v * Z, Z)
        raw = lax.broadcasted_iota(jnp.int32, (Z + 32, Z), 0)
        tgt = lax.broadcasted_iota(jnp.int32, (Z + 32, Z), 1)
        band = taps_matrix(taps_ref, v, 2, extended_offset(raw, Z, 16, odd_z), tgt)
        band = jnp.concatenate([band, jnp.zeros((Z - 32, Z), F32)], axis=0)
        fz[:, pl.ds(lane0, Z)] = band.astype(BF16)
        tgt = lax.broadcasted_iota(jnp.int32, (Y, YE), 0)
        src = extended_offset(lax.broadcasted_iota(jnp.int32, (Y, YE), 1), Y, 16, odd_y)
        base = taps_matrix(taps_ref, v, 1, src, tgt).astype(BF16)
        spread = jnp.dot(one_hot(4 * Y, Y, lambda r, c: lax.rem(r, Y) == c), base, preferred_element_type=F32).astype(BF16)
        spread = jnp.dot(spread, one_hot(YE, 4 * YE, lambda r, c: lax.rem(c, YE) == r), preferred_element_type=F32)
        spread = jnp.where(select_matrix(4 * Y, 4 * YE, lambda r, c: r // Y == c // YE), spread, 0.0)
        fy[v] = spread.astype(BF16)
        tgt = lax.broadcasted_iota(jnp.int32, (X, XE), 0)
        src = extended_offset(lax.broadcasted_iota(jnp.int32, (X, XE), 1), X, REACH, odd_x)
        base = taps_matrix(taps_ref, v, 0, src, tgt).astype(BF16)
        spread = jnp.dot(one_hot(X * 8, X, lambda r, c: r // 8 == c), base, preferred_element_type=F32).astype(BF16)
        spread = jnp.dot(spread, one_hot(XE, XE * 8, lambda r, c: c // 8 == r), preferred_element_type=F32)
        spread = jnp.where(select_matrix(X * 8, XE * 8, lambda r, c: lax.rem(r, 8) == lax.rem(c, 8)), spread, 0.0)
        fx[v] = spread.astype(BF16)
        return carry

    lax.fori_loop(0, VIEWS, one_view, 0, unroll=2)


def transpose_kernel(fz, fy, fx, bz, by, bx):
    XE = X + 2 * REACH

    def one_view(v, carry):
        lane0 = pl.multiple_of(v * Z, Z)
        bz[pl.ds(lane0, Z), :] = fz[:, pl.ds(lane0, Z)].astype(F32).T.astype(BF16)
        by[v] = fy[v].astype(F32).T.astype(BF16)
        wide = jnp.concatenate([fx[v].astype(F32), jnp.zeros((X * 8, 512 - XE * 8), F32)], axis=1).T
        bx[v] = wide[: XE * 8].astype(BF16)
        return carry

    lax.fori_loop(0, VIEWS, one_view, 0)


def reach_kernel(taps_ref, weights, along_x, along_y, along_z, sides, sent_a, sent_b, share):
    odd_x, odd_y, odd_z = parity("gx"), parity("gy"), parity("gz")
    lane = lanes((8, Z))
    row = lax.broadcasted_iota(jnp.int32, (8, Z), 0)
    base_x = 3 * (lane // 16)
    near_at = extended_offset(jnp.where(row < 3, base_x + row, X + base_x + row - 3), X, REACH, odd_x)
    far_at = jnp.where(row < 3, X + REACH + base_x + row, lane)
    far_at = extended_offset(far_at, X, REACH, odd_x)
    y_at = extended_offset(lane, Y, 16, odd_y)
    z_at = jnp.where(row == 0, lane, Z + lax.rem(lane, 16) + jnp.where(row == 2, 16, 0))
    z_at = extended_offset(z_at, Z, 16, odd_z)

    def down(values):
        return jnp.broadcast_to(values, (Z, Z)).T

    def one_view(v, carry):
        shares, norm = carry

        def reach(axis, name, size, count, *indices):
            outs = [jnp.zeros((8, Z), F32) for _ in indices]
            ats = [position(name) * size + index + REACH for index in indices]
            taps = jnp.zeros((), jnp.int32)
            for t in range(TAPS):
                tap = taps_ref[v, axis, t]
                taps = taps + tap
                value = tap.astype(F32) / 256.0
                outs = [
                    out + jnp.where((at >= t) & (at < count * size + t), value, 0.0) for out, at in zip(outs, ats)
                ]
            return outs, taps.astype(F32) / 256.0

        (near, far), whole_x = reach(0, "gx", X, 16, near_at, far_at)
        (rows_y,), whole_y = reach(1, "gy", Y, 4, y_at)
        (rows_z,), whole_z = reach(2, "gz", Z, 4, z_at)
        weight = weights[v].astype(F32)
        along_x[v] = down(far[3:4])[0:56]
        spread_y = down(rows_y[0:1])[0:YE]
        along_y[v] = spread_y
        along_z[v] = rows_z
        z_side = (rows_z[1:2], rows_z[2:3])
        for k in range(2):
            sides[v, 8 * k : 8 * k + 8] = near * z_side[k]
        for source, first, dst in ((near, 3, sent_a), (far, 0, sent_b)):
            def tile(k, source=source, first=first):
                return lambda i: spread_y * (source[first + i : first + i + 1] * z_side[k])

            def store(i, value, dst=dst):
                dst[v, i] = value

            def store_rest(first, value, dst=dst):
                dst[v, 3, first : first + 8] = value

            pack_sides(tile(0), tile(1), YE, store, store_rest)
            dst[v, 3, 24:32] = jnp.zeros((8, Z), F32)
            dst[v, 3, 56:64] = jnp.zeros((8, Z), F32)
        whole = jnp.full((8, Z), whole_x * whole_y * whole_z, F32)
        return jnp.where(lane == v, weight, shares), norm + weight * whole

    shares, norm = lax.fori_loop(0, VIEWS, one_view, (jnp.zeros((8, Z), F32), jnp.zeros((8, Z), F32)))
    share[...] = shares / norm


def pack_sides(side_a, side_b, rows, store, store_rest):
    lane = lanes((rows, Z))
    quarter = lanes((8, Z)) // 32
    for i in range(3):
        a, b = side_a(i), side_b(i)
        store(i, jnp.where(lane < 80, a, pltpu.roll(b, 80, 1)))
        rest = pltpu.roll(b, Z - 48, 1)
        for half in range(rows // 32):
            packed = rest[32 * half : 32 * half + 8]
            for q in range(1, 4):
                first = 32 * half + 8 * q
                packed = jnp.where(quarter == q, pltpu.roll(rest[first : first + 8], 32 * q, 1), packed)
            store_rest(32 * half + 8 * i, packed)


def unpack_sides(src, i, rows):
    tile = src[REACH + i]
    lane = lanes((rows, Z))
    parts = []
    for half in range(rows // 32):
        packed = src[REACH + 3, 32 * half + 8 * i : 32 * half + 8 * i + 8]
        parts += [packed] + [pltpu.roll(packed, Z - 32 * q, 1) for q in range(1, 4)]
    a = jnp.where(lane < 80, tile, 0.0)
    b = jnp.where(lane < 48, pltpu.roll(tile, Z - 80, 1), pltpu.roll(jnp.concatenate(parts, axis=0), 48, 1))
    return a, jnp.where(lane < 80, b, 0.0)


def pack_z(load, z_a, z_b):
    group = lanes((3 * Y, Z)) // 16
    up = jnp.zeros((3 * Y, Z), F32)
    down = jnp.zeros((3 * Y, Z), F32)
    for g in range(8):
        part = load(g)
        up = jnp.where(group == g, pltpu.roll(part, (16 * g + 16) % Z, 1) if g != 7 else part, up)
        down = jnp.where(group == g, pltpu.roll(part, 16 * g, 1) if g else part, down)
    odd = parity("gz")
    z_a[...] = jnp.where(odd == 0, up, down)
    z_b[...] = jnp.where(odd == 0, down, up)


def blurred_totals(load, along_x, along_y, along_z):
    lane = lanes((8, Z))
    row = lax.broadcasted_iota(jnp.int32, (8, Z), 0)
    out = jnp.zeros((8, Z), F32)
    for v in range(VIEWS):
        acc = jnp.zeros((Y, Z), F32)
        for i in range(X):
            acc = acc + load(i) * along_x[v, i : i + 1, :]
        total = jnp.sum(acc * along_y[v, 0:Y] * along_z[v, 0:1])
        out = jnp.where((lane == 8 + v) & (row == 0), total, out)
    return out


def first_kernel(est, z_a, z_b, kept):
    kept[...] = est[...]
    pack_z(lambda g: est[3 * g : 3 * g + 3].reshape(3 * Y, Z), z_a, z_b)


def sums_kernel(est, views, along_x, along_y, along_z, row_ref):
    lane = lanes((8, Z))
    row = lax.broadcasted_iota(jnp.int32, (8, Z), 0)
    out = blurred_totals(lambda i: est[i], along_x, along_y, along_z)
    for v in range(VIEWS):
        total = jnp.zeros((Y, Z), F32)
        square = jnp.zeros((Y, Z), F32)
        for i in range(X):
            image = views[v, i]
            total = total + image
            square = square + image * image
        out = jnp.where((lane == v) & (row == 0), jnp.sum(total), out)
        out = jnp.where((lane == 4 + v) & (row == 0), jnp.sum(square), out)
    row_ref[...] = out


def pack_y_kernel(est, z_a, z_b, *refs):
    row, y_a, y_b = refs if len(refs) == 3 else (None, *refs)
    odd = parity("gy")
    start_a = pl.multiple_of((1 - odd) * 16, 16)
    start_b = pl.multiple_of(odd * 16, 16)
    for start, out in ((start_a, y_a), (start_b, y_b)):
        out[0:X] = est[:, pl.ds(start, 16), :]
        for i in range(3):
            out[X + i] = z_a[pl.ds(start + i * Y, 16)]
            out[X + 3 + i] = z_b[pl.ds(start + i * Y, 16)]
    if row is not None:
        y_a[X + 6, 0:8] = row[...]
        y_a[X + 6, 8:16] = row[...]


def pack_x_kernel(est, z_a, z_b, y_a, y_b, row, own, x_a, x_b, row_out):
    def copy(i, carry):
        own[i, 0:Y] = est[i]
        return carry

    def beside(i, carry):
        own[i, Y : Y + 16] = y_a[i]
        own[i, Y + 16 : YE] = y_b[i]
        return carry

    lax.fori_loop(0, X, copy, 0, unroll=12)
    lax.fori_loop(0, X + 6, beside, 0, unroll=10)
    for i in range(3):
        own[X + i, 0:Y] = z_a[i * Y : i * Y + Y]
        own[X + 3 + i, 0:Y] = z_b[i * Y : i * Y + Y]
    total = row[...] + y_a[X + 6, 0:8] if y_a.shape[0] > X + 6 else row[...]
    row_out[...] = total
    odd = parity("gx")
    for flag, out, first_row, rows in ((odd, x_a, 0, YE), (1 - odd, x_b, Y, Y)):
        out[0:REACH] = own[pl.ds((1 - flag) * 9, REACH), first_row : first_row + rows]

        def side(first, flag=flag, first_row=first_row, rows=rows):
            def get(i):
                full = own[first + i, first_row : first_row + rows]
                return jnp.where(flag == 0, pltpu.roll(full, Z - 48, 1), full)

            return get

        write_sides(out, side(X), side(X + 3), rows)
    x_a[REACH + 3, 56:64] = total


def write_sides(out, side_a, side_b, rows):
    def store(i, value):
        out[REACH + i] = value

    def store_rest(first, value):
        out[REACH + 3, first : first + 8] = value

    pack_sides(side_a, side_b, rows, store, store_rest)
    for half in range(rows // 32):
        out[REACH + 3, 32 * half + 24 : 32 * half + 32] = jnp.zeros((8, Z), F32)


def pack_far_kernel(est, z_a, z_b, out):
    flag = 1 - parity("gx")
    out[0:REACH] = est[pl.ds((1 - flag) * 9, REACH)]

    def side(src):
        def get(i):
            full = src[i * Y : i * Y + Y]
            return jnp.where(flag == 0, pltpu.roll(full, Z - 48, 1), full)

        return get

    write_sides(out, side(z_a), side(z_b), Y)


def forward_group(src, sides_ref, plane, fz, fy, store):
    mains, sides = [], []
    lane = lanes((YE, Z))
    for k in range(8):
        p = plane + k
        g, spot = side_spot(p)
        mains.append(src[p])
        a = pltpu.roll(sides_ref[spot], lax.rem(Z - 16 * g, Z), 1)
        b = pltpu.roll(sides_ref[spot + 3], lax.rem(Z + 16 - 16 * g, Z), 1)
        sides.append(jnp.where(lane < 16, a, b))
    data = jnp.concatenate([jnp.concatenate(mains, 0), jnp.concatenate(sides, 0)], axis=1)
    wide = right_exact(data, fz[...])
    half = 4 * YE
    for v in range(VIEWS):
        columns = slice(v * Z, (v + 1) * Z)
        out = left_exact(fy[v], jnp.concatenate([wide[:half, columns], wide[half:, columns]], axis=1))
        store(v, jnp.concatenate([out[:, :Z].reshape(4, Y, Z), out[:, Z:].reshape(4, Y, Z)], axis=0))


def side_spot(p):
    beyond = (p >= X).astype(jnp.int32)
    local_plane = p - X * beyond
    g = local_plane // 3
    return g, local_plane - 3 * g + 6 * beyond


def forward_most_kernel(own, x_a, fz, fy, out, src, sides):
    src[0:X] = own[0:X]
    src[X:] = x_a[0:REACH]
    sides[0:6] = own[X:]
    for i in range(3):
        sides[6 + i], sides[9 + i] = unpack_sides(x_a, i, YE)

    def step(j, carry):
        plane = jnp.minimum(j * 8, X + REACH - 8)

        def store(v, value):
            out[v, pl.ds(plane, 8)] = value

        forward_group(src, sides, plane, fz, fy, store)
        return carry

    lax.fori_loop(0, 5, step, 0, unroll=MOST_UNROLL)


def forward_halo_kernel(near, far, fz, fy, out, src, sides):
    for k, half in enumerate((near, far)):
        rows = slice(k * Y, k * Y + Y)
        src[:, rows] = half[0:REACH]
        for i in range(3):
            sides[i, rows], sides[3 + i, rows] = unpack_sides(half, i, Y)

    def step(j, carry):
        plane = jnp.minimum(j * 8, REACH - 8)

        def store(v, value):
            out[v, pl.ds(plane, 8)] = value

        forward_group(src, sides, plane, fz, fy, store)
        return carry

    lax.fori_loop(0, 2, step, 0, unroll=HALO_UNROLL)


def forward_last_kernel(mid, halo_b, fx, out):
    def one_view(v, carry):
        for pair in range(2):
            columns = []
            for tile in (2 * pair, 2 * pair + 1):
                rows = pl.ds(tile * 8, 8)
                columns.append(
                    jnp.concatenate(
                        [
                            mid[v, :, rows].reshape((X + REACH) * 8, Z),
                            halo_b[v, :, rows].reshape(REACH * 8, Z),
                        ],
                        axis=0,
                    )
                )
            got = left_exact(fx[v], jnp.concatenate(columns, axis=1))
            for k, tile in enumerate((2 * pair, 2 * pair + 1)):
                out[v, :, tile * 8 : tile * 8 + 8] = got[:, k * Z : (k + 1) * Z].reshape(X, 8, Z)
        return carry

    lax.fori_loop(0, VIEWS, one_view, 0, unroll=2)


def pick(row, lane, index):
    return jnp.sum(jnp.where(lane == index, row, 0.0), axis=1, keepdims=True)


def view_scales(sums, share):
    lane = lanes((1, Z))
    row = sums[0:1, :]
    return [pick(share[0:1, :], lane, v) * (pick(row, lane, 8 + v) / pick(row, lane, v)) for v in range(VIEWS)]


def backward_group(load, plane, scales, bz, by, store):
    first, second = [], []
    for v in range(VIEWS):
        data = load(v, plane) * scales[v]
        pair = jnp.concatenate([data[0:4].reshape(4 * Y, Z), data[4:8].reshape(4 * Y, Z)], axis=1)
        got = left_exact(by[v], pair)
        first.append(got[:, :Z])
        second.append(got[:, Z:])
    both = jnp.concatenate([jnp.concatenate(first, axis=1), jnp.concatenate(second, axis=1)], axis=0)
    store(right_exact(both, bz[...]))


def store_extended(dst, sides_ref, plane, wide):
    group = lanes((YE, Z)) // 16
    for k in range(8):
        p = plane + k
        g, spot = side_spot(p)
        rows = wide[k * YE : (k + 1) * YE]
        dst[p] = rows[:, :Z]
        side = rows[:, Z:]
        a = pltpu.roll(side, lax.rem(16 * g + Z, Z), 1)
        b = pltpu.roll(side, lax.rem(16 * g + Z - 16, Z), 1)
        sides_ref[spot] = jnp.where(group == g, a, sides_ref[spot])
        sides_ref[spot + 3] = jnp.where(group == g, b, sides_ref[spot + 3])


def backward_kernel(blurred, views, bx, mid, halo_b):
    def one_view(v, carry):
        for pair in range(2):
            tiles = (2 * pair, 2 * pair + 1)
            b = jnp.concatenate([blurred[v, :, t * 8 : t * 8 + 8].reshape(X * 8, Z) for t in tiles], axis=1)
            image = jnp.concatenate([views[v, :, t * 8 : t * 8 + 8].reshape(X * 8, Z) for t in tiles], axis=1)
            got = left_exact(bx[v], image / b)
            for k, t in enumerate(tiles):
                piece = got[:, k * Z : (k + 1) * Z]
                rows = slice(t * 8, t * 8 + 8)
                mid[v, :, rows] = piece[: (X + REACH) * 8].reshape(X + REACH, 8, Z)
                halo_b[v, :, rows] = piece[(X + REACH) * 8 :].reshape(REACH, 8, Z)
        return carry

    lax.fori_loop(0, VIEWS, one_view, 0, unroll=2)


def misfit_kernel(sums, blurred, views, misfit):
    lane = lanes((1, Z))
    row = sums[0:1, :]
    out_lane = lanes((8, Z))
    out_row = lax.broadcasted_iota(jnp.int32, (8, Z), 0)
    misfits = jnp.zeros((8, Z), F32)
    for v in range(VIEWS):
        flux = pick(row, lane, v) / pick(row, lane, 8 + v)

        def plane(i, total, v=v, flux=flux):
            gap = views[v, i] - flux * blurred[v, i]
            return total + gap * gap

        missed = lax.fori_loop(0, X, plane, jnp.zeros((Y, Z), F32), unroll=4)
        misfits = jnp.where((out_lane == 24 + v) & (out_row == 0), jnp.sum(missed), misfits)
    misfit[...] = misfits


def centred_kernel(sums, earlier, blurred, views, out):
    lane = lanes((1, Z))
    row = sums[0:1, :]
    out_lane = lanes((8, Z))
    out_row = lax.broadcasted_iota(jnp.int32, (8, Z), 0)
    total = earlier[...]
    for v in range(VIEWS):
        centre = pick(row, lane, v) / pick(row, lane, 8 + v)

        def plane(i, carry, v=v, centre=centre):
            value = blurred[v, i]
            gap = views[v, i] - centre * value
            return carry[0] + gap * gap, carry[1] + gap * value, carry[2] + value * value

        zero = jnp.zeros((Y, Z), F32)
        for k, part in enumerate(lax.fori_loop(0, X, plane, (zero, zero, zero), unroll=4)):
            total = jnp.where((out_lane == 12 + 4 * k + v) & (out_row == 0), jnp.sum(part), total)
    out[...] = total


def report_kernel(first, sums, last, out):
    def at(row, start):
        return pltpu.roll(row, Z - start, 1) if start else row

    before, now, end = first[...], sums[...], last[...]
    square = at(now, 4)
    shift = now / at(now, 8) - before / at(before, 8)
    missed = at(end, 12) - 2.0 * shift * at(end, 16) + shift * shift * at(end, 20)
    out[0:1] = (at(end, 24) / square)[0:1, 0:VIEWS]
    out[1:2] = (missed / square)[0:1, 0:VIEWS]


def backward_halo_kernel(halo, sums, share, bz, by, near, far, dst, sides):
    sides[...] = jnp.zeros((6, YE, Z), F32)
    scales = view_scales(sums, share)

    def step(j, carry):
        plane = jnp.minimum(j * 8, REACH - 8)
        backward_group(
            lambda v, p: halo[v, pl.ds(p, 8)], plane, scales, bz, by,
            lambda wide: store_extended(dst, sides, plane, wide),
        )
        return carry

    lax.fori_loop(0, 2, step, 0, unroll=HALO_UNROLL)
    for k, half in enumerate((near, far)):
        rows = slice(k * Y, k * Y + Y)
        half[0:REACH] = dst[:, rows]
        write_sides(half, lambda i: sides[i, rows], lambda i: sides[3 + i, rows], Y)


def backward_most_kernel(mid, sums, share, bz, by, own, x_a, sides):
    sides[...] = jnp.zeros((12, YE, Z), F32)
    scales = view_scales(sums, share)

    def step(j, carry):
        plane = jnp.minimum(j * 8, X + REACH - 8)
        backward_group(
            lambda v, p: mid[v, pl.ds(p, 8)], plane, scales, bz, by,
            lambda wide: store_extended(own, sides, plane, wide),
        )
        return carry

    lax.fori_loop(0, 5, step, 0, unroll=MOST_UNROLL)
    own[X + REACH :] = sides[0:6]
    x_a[0:REACH] = own[X : X + REACH]
    write_sides(x_a, lambda i: sides[6 + i], lambda i: sides[9 + i], YE)


def totals_kernel(own_f, xa_f, xn_f, xp_f, own_b, xa_b, xn_b, xp_b, along_x, along_y, along_z, sides, sent_a, sent_b, out):
    def far(p):
        return jnp.concatenate([xn_f[p] * xn_b[p], xp_f[p] * xp_b[p]], axis=0)

    def planes(product_of, count, first, accs):
        def one(p, accs):
            product = product_of(p)
            return tuple(acc + product * along_x[v, pl.ds(first + p, 1), :] for v, acc in enumerate(accs))

        return lax.fori_loop(0, count, one, accs, unroll=3)

    accs = tuple(jnp.zeros((YE, Z), F32) for _ in range(VIEWS))
    accs = planes(lambda p: own_f[p] * own_b[p], X, 0, accs)
    accs = planes(lambda p: xa_f[p] * xa_b[p], REACH, X, accs)
    accs = planes(far, REACH, X + REACH, accs)
    lane = lanes((8, Z))
    row = lax.broadcasted_iota(jnp.int32, (8, Z), 0)
    result = jnp.zeros((8, Z), F32)
    for v in range(VIEWS):
        acc = accs[v] * along_z[v, 0:1]
        for k in range(2):
            for i in range(3):
                product = own_f[X + 3 * k + i] * own_b[X + REACH + 3 * k + i]
                acc = acc + product * sides[v, 8 * k + i : 8 * k + i + 1]
        acc = acc * along_y[v]
        for i in range(4):
            acc = acc + xa_f[REACH + i] * xa_b[REACH + i] * sent_a[v, i] + far(REACH + i) * sent_b[v, i]
        result = jnp.where((lane == 8 + v) & (row == 0), jnp.sum(acc), result)
    out[...] = result


def add_sides(total, src, flag, first_row, rows):
    spot = slice(first_row, first_row + rows)
    for i in range(3):
        for k, side in enumerate(unpack_sides(src, i, rows)):
            at = X + 3 * k + i
            total[at, spot] = total[at, spot] + jnp.where(flag == 0, pltpu.roll(side, 48, 1), side)


def add_x_kernel(own, x_a, x_b, kept, y_a, y_b, total):
    odd = parity("gx")
    start_a = (1 - odd) * 9
    start_b = odd * 9

    def copy(i, carry):
        total[i] = own[i]
        return carry

    def add(m, carry):
        total[start_a + m] = total[start_a + m] + x_a[m]
        return carry

    def add_far(m, carry):
        total[start_b + m, Y:YE] = total[start_b + m, Y:YE] + x_b[m]
        return carry

    def share_out(i, carry):
        kept[i] = total[i, 0:Y]
        y_a[i] = total[i, Y : Y + 16]
        y_b[i] = total[i, Y + 16 : YE]
        return carry

    lax.fori_loop(0, X, copy, 0, unroll=8)
    lax.fori_loop(0, REACH, add, 0, unroll=5)
    lax.fori_loop(0, REACH, add_far, 0, unroll=5)
    total[X:] = own[X + REACH :]
    for flag, src, first_row, rows in ((odd, x_a, 0, YE), (1 - odd, x_b, Y, Y)):
        add_sides(total, src, flag, first_row, rows)
    lax.fori_loop(0, X + 6, share_out, 0, unroll=10)


def add_y_kernel(kept, y_a, y_b, far, row, main, z_a, z_b, total):
    total[...] = kept[...]
    flag = 1 - parity("gx")
    spot = pl.ds((1 - flag) * 9, REACH)
    total[spot] = total[spot] + far[0:REACH]
    add_sides(total, far, flag, 0, Y)
    odd = parity("gy")
    for start, src in (((1 - odd) * 16, y_a), (odd * 16, y_b)):
        spot = pl.ds(pl.multiple_of(start, 16), 16)
        total[:, spot] = total[:, spot] + src[...]
    main[...] = total[0:X]
    for i in range(3):
        z_a[Y * i : Y * i + Y] = total[X + i]
        z_b[Y * i : Y * i + Y] = total[X + 3 + i]
    z_a[3 * Y :] = row[...]


def corrected(main, z_a, z_b, est, g):
    odd = parity("gz")
    lane = lanes((3 * Y, Z))
    a = z_a[0 : 3 * Y]
    b = z_b[...]
    up = jnp.where(odd == 0, a, b)
    down = jnp.where(odd == 0, b, a)
    up = pltpu.roll(up, (112 - 16 * g) % Z, 1) if g != 7 else up
    down = pltpu.roll(down, (Z - 16 * g) % Z, 1) if g else down
    total = main[3 * g : 3 * g + 3].reshape(3 * Y, Z)
    total = total + jnp.where(lane >= 112, up, 0.0) + jnp.where(lane < 16, down, 0.0)
    return est[3 * g : 3 * g + 3].reshape(3 * Y, Z) * total


def update_kernel(main, z_a, z_b, est, row, out, out_a, out_b, row_out):
    for g in range(8):
        out[3 * g : 3 * g + 3] = corrected(main, z_a, z_b, est, g).reshape(3, Y, Z)
    pack_z(lambda g: out[3 * g : 3 * g + 3].reshape(3 * Y, Z), out_a, out_b)
    row_out[...] = row[...] + z_a[3 * Y :]


def finish_kernel(main, z_a, z_b, est, out):
    for g in range(8):
        out[3 * g : 3 * g + 3] = corrected(main, z_a, z_b, est, g).reshape(3, Y, Z)


VM = pl.BlockSpec(memory_space=pltpu.VMEM)
SM = pl.BlockSpec(memory_space=pltpu.SMEM)


def call(kernel, outs, operands, specs=None, scratch=(), limit=16, flops=0):
    shapes = [jax.ShapeDtypeStruct(shape, dtype) for shape, dtype in outs]
    return pl.pallas_call(
        kernel,
        out_shape=shapes,
        in_specs=specs or [VM] * len(operands),
        out_specs=[VM] * len(shapes),
        scratch_shapes=[pltpu.VMEM(shape, dtype) for shape, dtype in scratch],
        compiler_params=pltpu.CompilerParams(vmem_limit_bytes=limit << 20),
        cost_estimate=pl.CostEstimate(flops=max(flops, 1000), bytes_accessed=1000, transcendentals=0),
    )(*operands)


def pairs_of(axis):
    names = AXES[axis]
    count = lax.axis_size(names)
    first = [(i, i ^ 1) for i in range(count)]
    second = [(i, i + 1) for i in range(1, count - 1, 2)] + [(i + 1, i) for i in range(1, count - 1, 2)]
    return names, first, second


def swap(a, b, axis):
    names, first, second = pairs_of(axis)
    b = lax.ppermute(b, names, second)
    a = lax.ppermute(a, names, first)
    return a, b


def swap_far(b):
    names, _, second = pairs_of("gx")
    return lax.ppermute(b, names, second)


def sum_step(row, axis, bit):
    count = lax.axis_size(axis)
    other = lax.ppermute(row, axis, [(i, i ^ bit) for i in range(count)])
    return row + other


MOST_UNROLL = 1
HALO_UNROLL = 1
ZS = ((3 * Y, Z), F32)
ZR = ((3 * Y + 8, Z), F32)
YS = ((X + 6, 16, Z), F32)
YR = ((X + 7, 16, Z), F32)
MOST = ((VIEWS, X + REACH, Y, Z), F32)
OWNB = ((X + REACH + 6, YE, Z), F32)
SIDES2 = ((12, YE, Z), F32)
XS = ((REACH + 4, YE, Z), F32)
XH = ((REACH + 4, Y, Z), F32)
OWN = ((X + 6, YE, Z), F32)
SIDES = ((6, YE, Z), F32)
CUBE = ((X, Y, Z), F32)
FOUR = ((VIEWS, X, Y, Z), F32)
ROW = ((8, Z), F32)
GF = 1 << 30
HALO = ((VIEWS, REACH, Y, Z), F32)


def local(estimate, view_images, psf_taps, view_weights):
    XE8 = (X + 2 * REACH) * 8
    z_a, z_b, estimate = call(first_kernel, [ZS, ZS, CUBE], [estimate], limit=2)
    *weights, share = call(
        reach_kernel,
        [
            ((VIEWS, 56, Z), F32), ((VIEWS, YE, Z), F32), ((VIEWS, 8, Z), F32), ((VIEWS, 16, Z), F32),
            ((VIEWS, 4, YE, Z), F32), ((VIEWS, 4, YE, Z), F32), ROW,
        ],
        [psf_taps, view_weights], specs=[SM, SM], limit=2,
    )
    (row,) = call(sums_kernel, [ROW], [estimate, view_images, *weights[:3]], limit=2, flops=GF // 4)
    shapes = [((256, VIEWS * Z), BF16), ((VIEWS, 4 * Y, 4 * YE), BF16), ((VIEWS, X * 8, XE8), BF16)]
    fz, fy, fx = call(setup_kernel, shapes, [psf_taps], specs=[SM], limit=4, flops=4 * GF)
    bz, by, bx = call(
        transpose_kernel,
        [((VIEWS * Z, 256), BF16), ((VIEWS, 4 * YE, 4 * Y), BF16), ((VIEWS, XE8, X * 8), BF16)],
        [fz, fy, fx], limit=4, flops=GF,
    )
    for iteration in range(ITERS):
        final = iteration + 1 == ITERS
        z_a, z_b = swap(z_a, z_b, "gz")
        for axis, bit in EARLY_STEPS if iteration == 0 else NEXT_STEPS:
            row = sum_step(row, axis, bit)
        rides = [] if iteration == 0 else [row]
        y_a, y_b = call(pack_y_kernel, [YR if rides else YS, YS], [estimate, z_a, z_b, *rides], limit=2)
        y_a, y_b = swap(y_a, y_b, "gy")
        (xn_f,) = call(pack_far_kernel, [XH], [estimate, z_a, z_b], limit=2)
        xn_f = swap_far(xn_f)
        own_f, xa_f, xp_f, row = call(pack_x_kernel, [OWN, XS, XH, ROW], [estimate, z_a, z_b, y_a, y_b, row], limit=2)
        xa_f, xp_f = swap(xa_f, xp_f, "gx")
        row = row + xa_f[REACH + 3, 56:64]
        for axis, bit in FIRST_STEPS if iteration == 0 else FINAL_STEPS:
            row = sum_step(row, axis, bit)
        (mid,) = call(
            forward_most_kernel, [MOST], [own_f, xa_f, fz, fy],
            scratch=[((X + REACH, YE, Z), F32), SIDES2], limit=6, flops=5 * GF,
        )
        (halo_b,) = call(
            forward_halo_kernel, [HALO], [xn_f, xp_f, fz, fy],
            scratch=[((REACH, YE, Z), F32), SIDES], limit=6, flops=2 * GF
        )
        (blurred,) = call(forward_last_kernel, [FOUR], [mid, halo_b, fx], limit=4, flops=2 * GF)
        mid, halo_b = call(
            backward_kernel, [MOST, HALO], [blurred, view_images, bx], limit=4, flops=2 * GF
        )
        if iteration == 0:
            data = first = row
            (missed,) = call(misfit_kernel, [ROW], [data, blurred, view_images], limit=2, flops=GF // 4)
        else:
            (missed,) = call(centred_kernel, [ROW], [first, missed, blurred, view_images], limit=2, flops=GF // 4)
            last = sum_step(missed, "gz", 3)
            data = jnp.where(lax.broadcasted_iota(jnp.int32, (8, Z), 1) < 8, first, row)
        xn_b, xp_b = call(
            backward_halo_kernel, [XH, XH], [halo_b, data, share, bz, by],
            scratch=[((REACH, YE, Z), F32), SIDES], limit=6, flops=2 * GF,
        )
        own_b, xa_b = call(
            backward_most_kernel, [OWNB, XS], [mid, data, share, bz, by],
            scratch=[SIDES2], limit=4, flops=5 * GF,
        )
        x_a, x_b = swap(xa_b, xp_b, "gx")
        far = swap_far(xn_b)
        if final:
            for axis, bit in LAST_STEPS:
                last = sum_step(last, axis, bit)
        else:
            (row,) = call(
                totals_kernel, [ROW], [own_f, xa_f, xn_f, xp_f, own_b, xa_b, xn_b, xp_b, *weights], limit=2, flops=GF
            )
            for axis, bit in BETWEEN_STEPS:
                row = sum_step(row, axis, bit)
        kept, y_a, y_b = call(add_x_kernel, [((X + 6, Y, Z), F32), YS, YS], [own_b, x_a, x_b], scratch=[OWN], limit=4)
        y_a, y_b = swap(y_a, y_b, "gy")
        main, z_a, z_b = call(
            add_y_kernel, [CUBE, ZR, ZS], [kept, y_a, y_b, far, last if final else row], scratch=[((X + 6, Y, Z), F32)], limit=2
        )
        z_a, z_b = swap(z_a, z_b, "gz")
        if not final:
            estimate, z_a, z_b, row = call(update_kernel, [CUBE, ZS, ZS, ROW], [main, z_a, z_b, estimate, row], limit=2)
        else:
            last = last + z_a[3 * Y :]
            for axis, bit in TAIL_STEPS:
                last = sum_step(last, axis, bit)
            (estimate,) = call(finish_kernel, [CUBE], [main, z_a, z_b, estimate], limit=2)
            (misfits,) = call(report_kernel, [((ITERS, VIEWS), F32)], [first, data, last], limit=2)
    return (estimate, misfits)


EARLY_STEPS = (("gz", 1), ("gx_1", 1))
FIRST_STEPS = (("gz", 3), ("gy", 1), ("gy", 3), ("gx_0", 1), ("gx_1", 3))
BETWEEN_STEPS = (("gx_0", 1),)
NEXT_STEPS = ()
FINAL_STEPS = (("gz", 3), ("gy", 3), ("gx_1", 1), ("gx_1", 3))
LAST_STEPS = (("gx_1", 1), ("gx_2", 1), ("gy", 1), ("gx_0", 1), ("gx_1", 3))
TAIL_STEPS = (("gy", 3),)


def solution(mesh):
    torus = Mesh(
        mesh.devices.reshape(2, 4, 2, mesh.shape["gy"], mesh.shape["gz"]),
        ("gx_0", "gx_1", "gx_2", "gy", "gz"),
    )
    in_specs = (P(GX, "gy", "gz"), P(None, GX, "gy", "gz"), P(), P())
    out_specs = (P(GX, "gy", "gz"), P())
    return jax.shard_map(local, mesh=torus, in_specs=in_specs, out_specs=out_specs, check_vma=False)
```

```python
import jax
import jax.numpy as jnp
from jax import lax
from jax.experimental import pallas as pl
from jax.experimental.pallas import tpu as pltpu
from jax.sharding import Mesh
from jax.sharding import PartitionSpec as P


TAPS = 31
REACH = 15
ITERS = 2
VIEWS = 4
X, Y, Z = 24, 32, 128
YE = 64
F32 = jnp.float32
BF16 = jnp.bfloat16
GX = ("gx_0", "gx_1", "gx_2")
AXES = {"gx": GX, "gy": "gy", "gz": "gz"}


def parity(name):
    if name == "gx":
        return lax.axis_index("gx_2")
    return lax.rem(lax.axis_index(name), 2)


def position(name):
    if name == "gx":
        return (lax.axis_index("gx_0") * 4 + lax.axis_index("gx_1")) * 2 + lax.axis_index("gx_2")
    return lax.axis_index(name)


def lanes(shape):
    return lax.broadcasted_iota(jnp.int32, shape, len(shape) - 1)


def split(value):
    high = value.astype(BF16)
    low = (value - high.astype(F32)).astype(BF16)
    return high, low


def left_exact(matrix, data):
    high, low = split(data)
    return jnp.dot(matrix, high, preferred_element_type=F32) + jnp.dot(matrix, low, preferred_element_type=F32)


def right_exact(data, matrix):
    rows = data.shape[0]
    both = jnp.dot(jnp.concatenate(split(data), axis=0), matrix, preferred_element_type=F32)
    return both[:rows] + both[rows:]


def extended_offset(index, size, width, odd):
    low_first = index < size + width
    local = jnp.where(low_first, index - size, index - size - width)
    upper = low_first == (odd == 0)
    outside = jnp.where(upper, size + local, local - width)
    return jnp.where(index < size, index, outside)


def taps_matrix(taps_ref, view, axis, source, target):
    tap = source - target + REACH
    out = jnp.zeros(tap.shape, F32)
    for t in range(TAPS):
        out = jnp.where(tap == t, taps_ref[view, axis, t].astype(F32) / 256.0, out)
    return out


def select_matrix(rows, columns, match):
    r = lax.broadcasted_iota(jnp.int32, (rows, columns), 0)
    c = lax.broadcasted_iota(jnp.int32, (rows, columns), 1)
    return match(r, c)


def one_hot(rows, columns, match):
    return jnp.where(select_matrix(rows, columns, match), 1.0, 0.0).astype(BF16)


def setup_kernel(taps_ref, fz, fy, fx):
    odd_x, odd_y, odd_z = parity("gx"), parity("gy"), parity("gz")
    XE = X + 2 * REACH

    def one_view(v, carry):
        lane0 = pl.multiple_of(v * Z, Z)
        raw = lax.broadcasted_iota(jnp.int32, (Z + 32, Z), 0)
        tgt = lax.broadcasted_iota(jnp.int32, (Z + 32, Z), 1)
        band = taps_matrix(taps_ref, v, 2, extended_offset(raw, Z, 16, odd_z), tgt)
        band = jnp.concatenate([band, jnp.zeros((Z - 32, Z), F32)], axis=0)
        fz[:, pl.ds(lane0, Z)] = band.astype(BF16)
        tgt = lax.broadcasted_iota(jnp.int32, (Y, YE), 0)
        src = extended_offset(lax.broadcasted_iota(jnp.int32, (Y, YE), 1), Y, 16, odd_y)
        base = taps_matrix(taps_ref, v, 1, src, tgt).astype(BF16)
        spread = jnp.dot(one_hot(4 * Y, Y, lambda r, c: lax.rem(r, Y) == c), base, preferred_element_type=F32).astype(BF16)
        spread = jnp.dot(spread, one_hot(YE, 4 * YE, lambda r, c: lax.rem(c, YE) == r), preferred_element_type=F32)
        spread = jnp.where(select_matrix(4 * Y, 4 * YE, lambda r, c: r // Y == c // YE), spread, 0.0)
        fy[v] = spread.astype(BF16)
        tgt = lax.broadcasted_iota(jnp.int32, (X, XE), 0)
        src = extended_offset(lax.broadcasted_iota(jnp.int32, (X, XE), 1), X, REACH, odd_x)
        base = taps_matrix(taps_ref, v, 0, src, tgt).astype(BF16)
        spread = jnp.dot(one_hot(X * 8, X, lambda r, c: r // 8 == c), base, preferred_element_type=F32).astype(BF16)
        spread = jnp.dot(spread, one_hot(XE, XE * 8, lambda r, c: c // 8 == r), preferred_element_type=F32)
        spread = jnp.where(select_matrix(X * 8, XE * 8, lambda r, c: lax.rem(r, 8) == lax.rem(c, 8)), spread, 0.0)
        fx[v] = spread.astype(BF16)
        return carry

    lax.fori_loop(0, VIEWS, one_view, 0, unroll=2)


def transpose_kernel(fz, fy, fx, bz, by, bx):
    XE = X + 2 * REACH

    def one_view(v, carry):
        lane0 = pl.multiple_of(v * Z, Z)
        bz[pl.ds(lane0, Z), :] = fz[:, pl.ds(lane0, Z)].astype(F32).T.astype(BF16)
        by[v] = fy[v].astype(F32).T.astype(BF16)
        wide = jnp.concatenate([fx[v].astype(F32), jnp.zeros((X * 8, 512 - XE * 8), F32)], axis=1).T
        bx[v] = wide[: XE * 8].astype(BF16)
        return carry

    lax.fori_loop(0, VIEWS, one_view, 0)


def reach_kernel(taps_ref, weights, along_x, along_y, along_z, sides, sent_a, sent_b, share):
    odd_x, odd_y, odd_z = parity("gx"), parity("gy"), parity("gz")
    lane = lanes((8, Z))
    row = lax.broadcasted_iota(jnp.int32, (8, Z), 0)
    base_x = 3 * (lane // 16)
    near_at = extended_offset(jnp.where(row < 3, base_x + row, X + base_x + row - 3), X, REACH, odd_x)
    far_at = jnp.where(row < 3, X + REACH + base_x + row, lane)
    far_at = extended_offset(far_at, X, REACH, odd_x)
    y_at = extended_offset(lane, Y, 16, odd_y)
    z_at = jnp.where(row == 0, lane, Z + lax.rem(lane, 16) + jnp.where(row == 2, 16, 0))
    z_at = extended_offset(z_at, Z, 16, odd_z)

    def down(values):
        return jnp.broadcast_to(values, (Z, Z)).T

    def one_view(v, carry):
        shares, norm = carry

        def reach(axis, name, size, count, *indices):
            outs = [jnp.zeros((8, Z), F32) for _ in indices]
            ats = [position(name) * size + index + REACH for index in indices]
            taps = jnp.zeros((), jnp.int32)
            for t in range(TAPS):
                tap = taps_ref[v, axis, t]
                taps = taps + tap
                value = tap.astype(F32) / 256.0
                outs = [
                    out + jnp.where((at >= t) & (at < count * size + t), value, 0.0) for out, at in zip(outs, ats)
                ]
            return outs, taps.astype(F32) / 256.0

        (near, far), whole_x = reach(0, "gx", X, 16, near_at, far_at)
        (rows_y,), whole_y = reach(1, "gy", Y, 4, y_at)
        (rows_z,), whole_z = reach(2, "gz", Z, 4, z_at)
        weight = weights[v].astype(F32)
        along_x[v] = down(far[3:4])[0:56]
        spread_y = down(rows_y[0:1])[0:YE]
        along_y[v] = spread_y
        along_z[v] = rows_z
        z_side = (rows_z[1:2], rows_z[2:3])
        for k in range(2):
            sides[v, 8 * k : 8 * k + 8] = near * z_side[k]
        for source, first, dst in ((near, 3, sent_a), (far, 0, sent_b)):
            def tile(k, source=source, first=first):
                return lambda i: spread_y * (source[first + i : first + i + 1] * z_side[k])

            def store(i, value, dst=dst):
                dst[v, i] = value

            def store_rest(i, value, dst=dst):
                dst[v, 3, 16 * i : 16 * i + 16] = value

            pack_sides(tile(0), tile(1), store, store_rest)
            dst[v, 3, 48:64] = jnp.zeros((16, Z), F32)
        whole = jnp.full((8, Z), whole_x * whole_y * whole_z, F32)
        return jnp.where(lane == v, weight, shares), norm + weight * whole

    shares, norm = lax.fori_loop(0, VIEWS, one_view, (jnp.zeros((8, Z), F32), jnp.zeros((8, Z), F32)))
    share[...] = shares / norm


def pack_sides(side_a, side_b, store, store_rest):
    lane = lanes((YE, Z))
    quarter = lanes((16, Z)) // 32
    for i in range(3):
        a, b = side_a(i), side_b(i)
        store(i, jnp.where(lane < 80, a, pltpu.roll(b, 80, 1)))
        rest = pltpu.roll(b, Z - 48, 1)
        packed = rest[0:16]
        for q in range(1, 4):
            packed = jnp.where(quarter == q, pltpu.roll(rest[16 * q : 16 * q + 16], 32 * q, 1), packed)
        store_rest(i, packed)


def unpack_sides(tile, packed):
    lane = lanes((YE, Z))
    parts = [packed] + [pltpu.roll(packed, Z - 32 * q, 1) for q in range(1, 4)]
    rest = jnp.concatenate(parts, axis=0)
    a = jnp.where(lane < 80, tile, 0.0)
    b = jnp.where(lane < 48, pltpu.roll(tile, Z - 80, 1), pltpu.roll(rest, 48, 1))
    return a, jnp.where(lane < 80, b, 0.0)


def pack_z(load, z_a, z_b):
    group = lanes((3 * Y, Z)) // 16
    up = jnp.zeros((3 * Y, Z), F32)
    down = jnp.zeros((3 * Y, Z), F32)
    for g in range(8):
        part = load(g)
        up = jnp.where(group == g, pltpu.roll(part, (16 * g + 16) % Z, 1) if g != 7 else part, up)
        down = jnp.where(group == g, pltpu.roll(part, 16 * g, 1) if g else part, down)
    odd = parity("gz")
    z_a[...] = jnp.where(odd == 0, up, down)
    z_b[...] = jnp.where(odd == 0, down, up)


def blurred_totals(load, along_x, along_y, along_z):
    lane = lanes((8, Z))
    row = lax.broadcasted_iota(jnp.int32, (8, Z), 0)
    out = jnp.zeros((8, Z), F32)
    for v in range(VIEWS):
        acc = jnp.zeros((Y, Z), F32)
        for i in range(X):
            acc = acc + load(i) * along_x[v, i : i + 1, :]
        total = jnp.sum(acc * along_y[v, 0:Y] * along_z[v, 0:1])
        out = jnp.where((lane == 8 + v) & (row == 0), total, out)
    return out


def first_kernel(est, z_a, z_b, kept):
    kept[...] = est[...]
    pack_z(lambda g: est[3 * g : 3 * g + 3].reshape(3 * Y, Z), z_a, z_b)


def sums_kernel(est, views, along_x, along_y, along_z, row_ref):
    lane = lanes((8, Z))
    row = lax.broadcasted_iota(jnp.int32, (8, Z), 0)
    out = blurred_totals(lambda i: est[i], along_x, along_y, along_z)
    for v in range(VIEWS):
        total = jnp.zeros((Y, Z), F32)
        square = jnp.zeros((Y, Z), F32)
        for i in range(X):
            image = views[v, i]
            total = total + image
            square = square + image * image
        out = jnp.where((lane == v) & (row == 0), jnp.sum(total), out)
        out = jnp.where((lane == 4 + v) & (row == 0), jnp.sum(square), out)
    row_ref[...] = out


def pack_y_kernel(est, z_a, z_b, *refs):
    row, y_a, y_b = refs if len(refs) == 3 else (None, *refs)
    odd = parity("gy")
    start_a = pl.multiple_of((1 - odd) * 16, 16)
    start_b = pl.multiple_of(odd * 16, 16)
    for start, out in ((start_a, y_a), (start_b, y_b)):
        out[0:X] = est[:, pl.ds(start, 16), :]
        for i in range(3):
            out[X + i] = z_a[pl.ds(start + i * Y, 16)]
            out[X + 3 + i] = z_b[pl.ds(start + i * Y, 16)]
    if row is not None:
        y_a[X + 6, 0:8] = row[...]
        y_a[X + 6, 8:16] = row[...]


def pack_x_kernel(est, z_a, z_b, y_a, y_b, row, own, x_a, x_b, row_out):
    def copy(i, carry):
        own[i, 0:Y] = est[i]
        return carry

    def beside(i, carry):
        own[i, Y : Y + 16] = y_a[i]
        own[i, Y + 16 : YE] = y_b[i]
        return carry

    lax.fori_loop(0, X, copy, 0, unroll=12)
    lax.fori_loop(0, X + 6, beside, 0, unroll=10)
    for i in range(3):
        own[X + i, 0:Y] = z_a[i * Y : i * Y + Y]
        own[X + 3 + i, 0:Y] = z_b[i * Y : i * Y + Y]
    total = row[...] + y_a[X + 6, 0:8] if y_a.shape[0] > X + 6 else row[...]
    row_out[...] = total
    odd = parity("gx")
    for flag, out in ((odd, x_a), (1 - odd, x_b)):
        out[0:REACH] = own[pl.ds((1 - flag) * 9, REACH)]

        def side(first):
            def get(i, flag=flag):
                full = own[first + i]
                return jnp.where(flag == 0, pltpu.roll(full, Z - 48, 1), full)

            return get

        def store(i, value, out=out):
            out[REACH + i] = value

        def store_rest(i, value, out=out):
            out[REACH + 3, 16 * i : 16 * i + 16] = value

        pack_sides(side(X), side(X + 3), store, store_rest)
        out[REACH + 3, 48:56] = total
        out[REACH + 3, 56:64] = total


def forward_group(src, sides_ref, plane, fz, fy, store):
    mains, sides = [], []
    lane = lanes((YE, Z))
    for k in range(8):
        p = plane + k
        g, spot = side_spot(p)
        mains.append(src[p])
        a = pltpu.roll(sides_ref[spot], lax.rem(Z - 16 * g, Z), 1)
        b = pltpu.roll(sides_ref[spot + 3], lax.rem(Z + 16 - 16 * g, Z), 1)
        sides.append(jnp.where(lane < 16, a, b))
    data = jnp.concatenate([jnp.concatenate(mains, 0), jnp.concatenate(sides, 0)], axis=1)
    wide = right_exact(data, fz[...])
    half = 4 * YE
    for v in range(VIEWS):
        columns = slice(v * Z, (v + 1) * Z)
        out = left_exact(fy[v], jnp.concatenate([wide[:half, columns], wide[half:, columns]], axis=1))
        store(v, jnp.concatenate([out[:, :Z].reshape(4, Y, Z), out[:, Z:].reshape(4, Y, Z)], axis=0))


def side_spot(p):
    beyond = (p >= X).astype(jnp.int32)
    local_plane = p - X * beyond
    g = local_plane // 3
    return g, local_plane - 3 * g + 6 * beyond


def forward_most_kernel(own, x_a, fz, fy, out, src, sides):
    src[0:X] = own[0:X]
    src[X:] = x_a[0:REACH]
    sides[0:6] = own[X:]
    for i in range(3):
        sides[6 + i], sides[9 + i] = unpack_sides(x_a[REACH + i], x_a[REACH + 3, 16 * i : 16 * i + 16])

    def step(j, carry):
        plane = jnp.minimum(j * 8, X + REACH - 8)

        def store(v, value):
            out[v, pl.ds(plane, 8)] = value

        forward_group(src, sides, plane, fz, fy, store)
        return carry

    lax.fori_loop(0, 5, step, 0, unroll=MOST_UNROLL)


def forward_halo_kernel(src, fz, fy, out, sides):
    for i in range(3):
        sides[i], sides[3 + i] = unpack_sides(src[REACH + i], src[REACH + 3, 16 * i : 16 * i + 16])

    def step(j, carry):
        plane = jnp.minimum(j * 8, REACH - 8)

        def store(v, value):
            out[v, pl.ds(plane, 8)] = value

        forward_group(src, sides, plane, fz, fy, store)
        return carry

    lax.fori_loop(0, 2, step, 0, unroll=2)


def forward_last_kernel(mid, halo_b, fx, out):
    def one_view(v, carry):
        for pair in range(2):
            columns = []
            for tile in (2 * pair, 2 * pair + 1):
                rows = pl.ds(tile * 8, 8)
                columns.append(
                    jnp.concatenate(
                        [
                            mid[v, :, rows].reshape((X + REACH) * 8, Z),
                            halo_b[v, :, rows].reshape(REACH * 8, Z),
                        ],
                        axis=0,
                    )
                )
            got = left_exact(fx[v], jnp.concatenate(columns, axis=1))
            for k, tile in enumerate((2 * pair, 2 * pair + 1)):
                out[v, :, tile * 8 : tile * 8 + 8] = got[:, k * Z : (k + 1) * Z].reshape(X, 8, Z)
        return carry

    lax.fori_loop(0, VIEWS, one_view, 0, unroll=2)


def pick(row, lane, index):
    return jnp.sum(jnp.where(lane == index, row, 0.0), axis=1, keepdims=True)


def view_scales(sums, share):
    lane = lanes((1, Z))
    row = sums[0:1, :]
    return [pick(share[0:1, :], lane, v) * (pick(row, lane, 8 + v) / pick(row, lane, v)) for v in range(VIEWS)]


def backward_group(load, plane, scales, bz, by, store):
    first, second = [], []
    for v in range(VIEWS):
        data = load(v, plane) * scales[v]
        pair = jnp.concatenate([data[0:4].reshape(4 * Y, Z), data[4:8].reshape(4 * Y, Z)], axis=1)
        got = left_exact(by[v], pair)
        first.append(got[:, :Z])
        second.append(got[:, Z:])
    both = jnp.concatenate([jnp.concatenate(first, axis=1), jnp.concatenate(second, axis=1)], axis=0)
    store(right_exact(both, bz[...]))


def store_extended(dst, sides_ref, plane, wide):
    group = lanes((YE, Z)) // 16
    for k in range(8):
        p = plane + k
        g, spot = side_spot(p)
        rows = wide[k * YE : (k + 1) * YE]
        dst[p] = rows[:, :Z]
        side = rows[:, Z:]
        a = pltpu.roll(side, lax.rem(16 * g + Z, Z), 1)
        b = pltpu.roll(side, lax.rem(16 * g + Z - 16, Z), 1)
        sides_ref[spot] = jnp.where(group == g, a, sides_ref[spot])
        sides_ref[spot + 3] = jnp.where(group == g, b, sides_ref[spot + 3])


def backward_kernel(blurred, views, bx, mid, halo_b):
    def one_view(v, carry):
        for pair in range(2):
            tiles = (2 * pair, 2 * pair + 1)
            b = jnp.concatenate([blurred[v, :, t * 8 : t * 8 + 8].reshape(X * 8, Z) for t in tiles], axis=1)
            image = jnp.concatenate([views[v, :, t * 8 : t * 8 + 8].reshape(X * 8, Z) for t in tiles], axis=1)
            got = left_exact(bx[v], image / b)
            for k, t in enumerate(tiles):
                piece = got[:, k * Z : (k + 1) * Z]
                rows = slice(t * 8, t * 8 + 8)
                mid[v, :, rows] = piece[: (X + REACH) * 8].reshape(X + REACH, 8, Z)
                halo_b[v, :, rows] = piece[(X + REACH) * 8 :].reshape(REACH, 8, Z)
        return carry

    lax.fori_loop(0, VIEWS, one_view, 0, unroll=2)


def misfit_kernel(sums, blurred, views, misfit):
    lane = lanes((1, Z))
    row = sums[0:1, :]
    out_lane = lanes((8, Z))
    out_row = lax.broadcasted_iota(jnp.int32, (8, Z), 0)
    misfits = jnp.zeros((8, Z), F32)
    for v in range(VIEWS):
        flux = pick(row, lane, v) / pick(row, lane, 8 + v)

        def plane(i, total, v=v, flux=flux):
            gap = views[v, i] - flux * blurred[v, i]
            return total + gap * gap

        missed = lax.fori_loop(0, X, plane, jnp.zeros((Y, Z), F32), unroll=4)
        misfits = jnp.where((out_lane == 24 + v) & (out_row == 0), jnp.sum(missed), misfits)
    misfit[...] = misfits


def centred_kernel(sums, earlier, blurred, views, out):
    lane = lanes((1, Z))
    row = sums[0:1, :]
    out_lane = lanes((8, Z))
    out_row = lax.broadcasted_iota(jnp.int32, (8, Z), 0)
    total = earlier[...]
    for v in range(VIEWS):
        centre = pick(row, lane, v) / pick(row, lane, 8 + v)

        def plane(i, carry, v=v, centre=centre):
            value = blurred[v, i]
            gap = views[v, i] - centre * value
            return carry[0] + gap * gap, carry[1] + gap * value, carry[2] + value * value

        zero = jnp.zeros((Y, Z), F32)
        for k, part in enumerate(lax.fori_loop(0, X, plane, (zero, zero, zero), unroll=4)):
            total = jnp.where((out_lane == 12 + 4 * k + v) & (out_row == 0), jnp.sum(part), total)
    out[...] = total


def report_kernel(first, sums, last, out):
    def at(row, start):
        return pltpu.roll(row, Z - start, 1) if start else row

    before, now, end = first[...], sums[...], last[...]
    square = at(now, 4)
    shift = now / at(now, 8) - before / at(before, 8)
    missed = at(end, 12) - 2.0 * shift * at(end, 16) + shift * shift * at(end, 20)
    out[0:1] = (at(end, 24) / square)[0:1, 0:VIEWS]
    out[1:2] = (missed / square)[0:1, 0:VIEWS]


def backward_halo_kernel(halo, sums, share, bz, by, dst, sides):
    sides[...] = jnp.zeros((6, YE, Z), F32)
    scales = view_scales(sums, share)

    def step(j, carry):
        plane = jnp.minimum(j * 8, REACH - 8)
        backward_group(
            lambda v, p: halo[v, pl.ds(p, 8)], plane, scales, bz, by,
            lambda wide: store_extended(dst, sides, plane, wide),
        )
        return carry

    lax.fori_loop(0, 2, step, 0, unroll=HALO_UNROLL)
    send_sides(dst, sides, 0)


def send_sides(dst, sides, first):
    def store(i, value):
        dst[REACH + i] = value

    def store_rest(i, value):
        dst[REACH + 3, 16 * i : 16 * i + 16] = value

    pack_sides(lambda i: sides[first + i], lambda i: sides[first + 3 + i], store, store_rest)
    dst[REACH + 3, 48:64] = jnp.zeros((16, Z), F32)


def backward_most_kernel(mid, sums, share, bz, by, own, x_a, sides):
    sides[...] = jnp.zeros((12, YE, Z), F32)
    scales = view_scales(sums, share)

    def step(j, carry):
        plane = jnp.minimum(j * 8, X + REACH - 8)
        backward_group(
            lambda v, p: mid[v, pl.ds(p, 8)], plane, scales, bz, by,
            lambda wide: store_extended(own, sides, plane, wide),
        )
        return carry

    lax.fori_loop(0, 5, step, 0, unroll=MOST_UNROLL)
    own[X + REACH :] = sides[0:6]
    x_a[0:REACH] = own[X : X + REACH]
    send_sides(x_a, sides, 6)


def totals_kernel(own_f, xa_f, xb_f, own_b, xa_b, xb_b, along_x, along_y, along_z, sides, sent_a, sent_b, out):
    def planes(left, right, count, first, accs):
        def one(p, accs):
            product = left[p] * right[p]
            return tuple(acc + product * along_x[v, pl.ds(first + p, 1), :] for v, acc in enumerate(accs))

        return lax.fori_loop(0, count, one, accs, unroll=3)

    accs = tuple(jnp.zeros((YE, Z), F32) for _ in range(VIEWS))
    accs = planes(own_f, own_b, X, 0, accs)
    accs = planes(xa_f, xa_b, REACH, X, accs)
    accs = planes(xb_f, xb_b, REACH, X + REACH, accs)
    lane = lanes((8, Z))
    row = lax.broadcasted_iota(jnp.int32, (8, Z), 0)
    result = jnp.zeros((8, Z), F32)
    for v in range(VIEWS):
        acc = accs[v] * along_z[v, 0:1]
        for k in range(2):
            for i in range(3):
                product = own_f[X + 3 * k + i] * own_b[X + REACH + 3 * k + i]
                acc = acc + product * sides[v, 8 * k + i : 8 * k + i + 1]
        acc = acc * along_y[v]
        for left, right, weight in ((xa_f, xa_b, sent_a), (xb_f, xb_b, sent_b)):
            for i in range(4):
                acc = acc + left[REACH + i] * right[REACH + i] * weight[v, i]
        result = jnp.where((lane == 8 + v) & (row == 0), jnp.sum(acc), result)
    out[...] = result


def add_x_kernel(own, x_a, x_b, kept, y_a, y_b, total):
    odd = parity("gx")
    start_a = (1 - odd) * 9
    start_b = odd * 9

    def copy(i, carry):
        total[i] = own[i]
        return carry

    def add(m, carry):
        total[start_a + m] = total[start_a + m] + x_a[m]
        return carry

    def add_far(m, carry):
        total[start_b + m] = total[start_b + m] + x_b[m]
        return carry

    def share_out(i, carry):
        kept[i] = total[i, 0:Y]
        y_a[i] = total[i, Y : Y + 16]
        y_b[i] = total[i, Y + 16 : YE]
        return carry

    lax.fori_loop(0, X, copy, 0, unroll=8)
    lax.fori_loop(0, REACH, add, 0, unroll=5)
    lax.fori_loop(0, REACH, add_far, 0, unroll=5)
    total[X:] = own[X + REACH :]
    for flag, src in ((odd, x_a), (1 - odd, x_b)):
        for i in range(3):
            sides = unpack_sides(src[REACH + i], src[REACH + 3, 16 * i : 16 * i + 16])
            for k, side in enumerate(sides):
                at = X + 3 * k + i
                total[at] = total[at] + jnp.where(flag == 0, pltpu.roll(side, 48, 1), side)
    lax.fori_loop(0, X + 6, share_out, 0, unroll=10)


def add_y_kernel(kept, y_a, y_b, row, main, z_a, z_b, total):
    total[...] = kept[...]
    odd = parity("gy")
    for start, src in (((1 - odd) * 16, y_a), (odd * 16, y_b)):
        spot = pl.ds(pl.multiple_of(start, 16), 16)
        total[:, spot] = total[:, spot] + src[...]
    main[...] = total[0:X]
    for i in range(3):
        z_a[Y * i : Y * i + Y] = total[X + i]
        z_b[Y * i : Y * i + Y] = total[X + 3 + i]
    z_a[3 * Y :] = row[...]


def corrected(main, z_a, z_b, est, g):
    odd = parity("gz")
    lane = lanes((3 * Y, Z))
    a = z_a[0 : 3 * Y]
    b = z_b[...]
    up = jnp.where(odd == 0, a, b)
    down = jnp.where(odd == 0, b, a)
    up = pltpu.roll(up, (112 - 16 * g) % Z, 1) if g != 7 else up
    down = pltpu.roll(down, (Z - 16 * g) % Z, 1) if g else down
    total = main[3 * g : 3 * g + 3].reshape(3 * Y, Z)
    total = total + jnp.where(lane >= 112, up, 0.0) + jnp.where(lane < 16, down, 0.0)
    return est[3 * g : 3 * g + 3].reshape(3 * Y, Z) * total


def update_kernel(main, z_a, z_b, est, row, out, out_a, out_b, row_out):
    for g in range(8):
        out[3 * g : 3 * g + 3] = corrected(main, z_a, z_b, est, g).reshape(3, Y, Z)
    pack_z(lambda g: out[3 * g : 3 * g + 3].reshape(3 * Y, Z), out_a, out_b)
    row_out[...] = row[...] + z_a[3 * Y :]


def finish_kernel(main, z_a, z_b, est, out):
    for g in range(8):
        out[3 * g : 3 * g + 3] = corrected(main, z_a, z_b, est, g).reshape(3, Y, Z)


VM = pl.BlockSpec(memory_space=pltpu.VMEM)
SM = pl.BlockSpec(memory_space=pltpu.SMEM)


def call(kernel, outs, operands, specs=None, scratch=(), limit=16, flops=0):
    shapes = [jax.ShapeDtypeStruct(shape, dtype) for shape, dtype in outs]
    return pl.pallas_call(
        kernel,
        out_shape=shapes,
        in_specs=specs or [VM] * len(operands),
        out_specs=[VM] * len(shapes),
        scratch_shapes=[pltpu.VMEM(shape, dtype) for shape, dtype in scratch],
        compiler_params=pltpu.CompilerParams(vmem_limit_bytes=limit << 20),
        cost_estimate=pl.CostEstimate(flops=max(flops, 1000), bytes_accessed=1000, transcendentals=0),
    )(*operands)


def swap(a, b, axis):
    names = AXES[axis]
    count = lax.axis_size(names)
    first = [(i, i ^ 1) for i in range(count)]
    second = [(i, i + 1) for i in range(1, count - 1, 2)] + [(i + 1, i) for i in range(1, count - 1, 2)]
    b = lax.ppermute(b, names, second)
    a = lax.ppermute(a, names, first)
    return a, b


def sum_step(row, axis, bit):
    count = lax.axis_size(axis)
    other = lax.ppermute(row, axis, [(i, i ^ bit) for i in range(count)])
    return row + other


MOST_UNROLL = 1
HALO_UNROLL = 1
ZS = ((3 * Y, Z), F32)
ZR = ((3 * Y + 8, Z), F32)
YS = ((X + 6, 16, Z), F32)
YR = ((X + 7, 16, Z), F32)
MOST = ((VIEWS, X + REACH, Y, Z), F32)
OWNB = ((X + REACH + 6, YE, Z), F32)
SIDES2 = ((12, YE, Z), F32)
XS = ((REACH + 4, YE, Z), F32)
OWN = ((X + 6, YE, Z), F32)
SIDES = ((6, YE, Z), F32)
CUBE = ((X, Y, Z), F32)
FOUR = ((VIEWS, X, Y, Z), F32)
ROW = ((8, Z), F32)
GF = 1 << 30
HALO = ((VIEWS, REACH, Y, Z), F32)


def local(estimate, view_images, psf_taps, view_weights):
    XE8 = (X + 2 * REACH) * 8
    z_a, z_b, estimate = call(first_kernel, [ZS, ZS, CUBE], [estimate], limit=2)
    *weights, share = call(
        reach_kernel,
        [
            ((VIEWS, 56, Z), F32), ((VIEWS, YE, Z), F32), ((VIEWS, 8, Z), F32), ((VIEWS, 16, Z), F32),
            ((VIEWS, 4, YE, Z), F32), ((VIEWS, 4, YE, Z), F32), ROW,
        ],
        [psf_taps, view_weights], specs=[SM, SM], limit=2,
    )
    (row,) = call(sums_kernel, [ROW], [estimate, view_images, *weights[:3]], limit=2, flops=GF // 4)
    shapes = [((256, VIEWS * Z), BF16), ((VIEWS, 4 * Y, 4 * YE), BF16), ((VIEWS, X * 8, XE8), BF16)]
    fz, fy, fx = call(setup_kernel, shapes, [psf_taps], specs=[SM], limit=4, flops=4 * GF)
    bz, by, bx = call(
        transpose_kernel,
        [((VIEWS * Z, 256), BF16), ((VIEWS, 4 * YE, 4 * Y), BF16), ((VIEWS, XE8, X * 8), BF16)],
        [fz, fy, fx], limit=4, flops=GF,
    )
    for iteration in range(ITERS):
        final = iteration + 1 == ITERS
        z_a, z_b = swap(z_a, z_b, "gz")
        for axis, bit in EARLY_STEPS if iteration == 0 else NEXT_STEPS:
            row = sum_step(row, axis, bit)
        rides = [] if iteration == 0 else [row]
        y_a, y_b = call(pack_y_kernel, [YR if rides else YS, YS], [estimate, z_a, z_b, *rides], limit=2)
        y_a, y_b = swap(y_a, y_b, "gy")
        own_f, xa_f, xb_f, row = call(pack_x_kernel, [OWN, XS, XS, ROW], [estimate, z_a, z_b, y_a, y_b, row], limit=2)
        xa_f, xb_f = swap(xa_f, xb_f, "gx")
        row = row + xa_f[REACH + 3, 48:56]
        for axis, bit in FIRST_STEPS if iteration == 0 else FINAL_STEPS:
            row = sum_step(row, axis, bit)
        (mid,) = call(
            forward_most_kernel, [MOST], [own_f, xa_f, fz, fy],
            scratch=[((X + REACH, YE, Z), F32), SIDES2], limit=6, flops=5 * GF,
        )
        (halo_b,) = call(forward_halo_kernel, [HALO], [xb_f, fz, fy], scratch=[SIDES], limit=4, flops=2 * GF)
        (blurred,) = call(forward_last_kernel, [FOUR], [mid, halo_b, fx], limit=4, flops=2 * GF)
        mid, halo_b = call(
            backward_kernel, [MOST, HALO], [blurred, view_images, bx], limit=4, flops=2 * GF
        )
        if iteration == 0:
            data = first = row
            (missed,) = call(misfit_kernel, [ROW], [data, blurred, view_images], limit=2, flops=GF // 4)
        else:
            (missed,) = call(centred_kernel, [ROW], [first, missed, blurred, view_images], limit=2, flops=GF // 4)
            last = sum_step(missed, "gz", 3)
            data = jnp.where(lax.broadcasted_iota(jnp.int32, (8, Z), 1) < 8, first, row)
        (xb_b,) = call(
            backward_halo_kernel, [XS], [halo_b, data, share, bz, by],
            scratch=[SIDES], limit=4, flops=2 * GF,
        )
        own_b, xa_b = call(
            backward_most_kernel, [OWNB, XS], [mid, data, share, bz, by],
            scratch=[SIDES2], limit=4, flops=5 * GF,
        )
        x_a, x_b = swap(xa_b, xb_b, "gx")
        if final:
            for axis, bit in LAST_STEPS:
                last = sum_step(last, axis, bit)
        else:
            (row,) = call(
                totals_kernel, [ROW], [own_f, xa_f, xb_f, own_b, xa_b, xb_b, *weights], limit=2, flops=GF
            )
            for axis, bit in BETWEEN_STEPS:
                row = sum_step(row, axis, bit)
        kept, y_a, y_b = call(add_x_kernel, [((X + 6, Y, Z), F32), YS, YS], [own_b, x_a, x_b], scratch=[OWN], limit=4)
        y_a, y_b = swap(y_a, y_b, "gy")
        main, z_a, z_b = call(
            add_y_kernel, [CUBE, ZR, ZS], [kept, y_a, y_b, last if final else row], scratch=[((X + 6, Y, Z), F32)], limit=2
        )
        z_a, z_b = swap(z_a, z_b, "gz")
        if not final:
            estimate, z_a, z_b, row = call(update_kernel, [CUBE, ZS, ZS, ROW], [main, z_a, z_b, estimate, row], limit=2)
        else:
            last = last + z_a[3 * Y :]
            for axis, bit in TAIL_STEPS:
                last = sum_step(last, axis, bit)
            (estimate,) = call(finish_kernel, [CUBE], [main, z_a, z_b, estimate], limit=2)
            (misfits,) = call(report_kernel, [((ITERS, VIEWS), F32)], [first, data, last], limit=2)
    return (estimate, misfits)


EARLY_STEPS = (("gz", 1),)
FIRST_STEPS = (("gz", 3), ("gy", 1), ("gy", 3), ("gx_0", 1), ("gx_1", 1), ("gx_1", 3))
BETWEEN_STEPS = (("gx_1", 1),)
NEXT_STEPS = ()
FINAL_STEPS = (("gz", 3), ("gx_0", 1), ("gy", 3), ("gx_1", 3))
LAST_STEPS = (("gy", 3), ("gx_2", 1), ("gy", 1), ("gx_1", 1), ("gx_1", 3))
TAIL_STEPS = (("gx_0", 1),)


def solution(mesh):
    torus = Mesh(
        mesh.devices.reshape(2, 4, 2, mesh.shape["gy"], mesh.shape["gz"]),
        ("gx_0", "gx_1", "gx_2", "gy", "gz"),
    )
    in_specs = (P(GX, "gy", "gz"), P(None, GX, "gy", "gz"), P(), P())
    out_specs = (P(GX, "gy", "gz"), P())
    return jax.shard_map(local, mesh=torus, in_specs=in_specs, out_specs=out_specs, check_vma=False)
```
